256 devices in a mesh: row: 8 (over x, core), col: 32 (over y, z).
Axes of the slice: x: 4, y: 4, z: 8, core: 2. Of those that a mesh axis runs over, the one named last changes fastest.
Arguments:
- pooled: bfloat16 [16384, 1152], P(('row', 'col')), may hold values from -32 to 32
- hidden: bfloat16 [16384, 4304], P(('row', 'col')), may hold values from -6 to 6
- text: bfloat16 [16384, 1152], P(('row', 'col')), may hold values from -12 to 12
- weight: float32 [1152, 4304], P('col', 'row'), may hold values from -0.09375 to 0.09375
- row_moment: float32 [1152], P('col'), may hold values from 1e-07 to 1e-05
- col_moment: float32 [4304], P('row'), may hold values from 1e-07 to 1e-05
- log_scale: float32 [], replicated, may hold values from 4.2 to 4.8
- bias: float32 [], replicated, may hold values from -16 to -12
Outputs:
- update: float32 [1152, 4304], P('col', 'row')
- new_row: float32 [1152], P('col')
- new_col: float32 [4304], P('row')
- loss: float32 [], replicated
The draws below stay inside these ranges and needn't reach their ends.
All inputs are finite; a program needn't handle non-finite values.
Results may differ from the reference program's by a relative error of at most 0.004.
Values may be sent and summed in bfloat16 or wider, within the bound.
A program may use at most 128 MiB of HBM per device.

```python
import math
import jax
import jax.numpy as jnp
from jax import lax

D = 1152
FF = 4304
TOK_DEV = 64
BATCH = 16384
N_ROW = 8
N_COL = 32


def noise_block(key, shape):
    return jax.random.normal(key, shape, jnp.float32)


def pair_parts(key):
    folded = jax.random.fold_in(key, 4242)
    subkeys = jax.random.split(folded, 6)
    group_count = 16
    centers = noise_block(subkeys[0], (group_count, D))
    members = jax.random.randint(subkeys[1], (BATCH,), 0, group_count)
    onehot = (members[:, None] == jnp.arange(group_count, dtype=jnp.int32)[None, :]).astype(jnp.float32)
    cluster = jnp.dot(onehot, centers, precision=lax.Precision.HIGHEST)
    shared = noise_block(subkeys[2], (BATCH, D))
    strength = jax.random.uniform(subkeys[3], (BATCH, 1), jnp.float32, 0.1, 0.5)
    own_image = noise_block(subkeys[4], (BATCH, D))
    own_text = noise_block(subkeys[5], (BATCH, D))
    cluster_weight = 0.5
    image_side = cluster_weight * cluster + shared + 1.5 * own_image
    text_side = cluster_weight * cluster + strength * shared + 1.5 * own_text
    return (jnp.clip(image_side, -32.0, 32.0), jnp.clip(text_side, -12.0, 12.0))


def draw_pooled(key, part):
    return pair_parts(key)[0].astype(jnp.bfloat16)


def draw_text(key, part):
    return pair_parts(key)[1].astype(jnp.bfloat16)


def block_levels(key, extent, cuts, least, largest):
    loudness, own = 1.0, jax.random.fold_in(key, 6)
    for axis_at, shards_of in cuts:
        heights = jnp.exp(jax.random.uniform(jax.random.fold_in(own, axis_at), (shards_of,), jnp.float32, least / len(cuts), largest / len(cuts)))
        loudness = loudness * jnp.repeat(heights, extent[axis_at] // shards_of).reshape([-1 if axis == axis_at else 1 for axis in range(len(extent))])
    return loudness


def scatter_about(key, shape, spread, bound, cuts=(), kind=jnp.bfloat16):
    array = jax.random.normal(key, shape, jnp.float32) * spread
    if len(cuts) > 0:
        array = block_levels(key, shape, cuts, -0.22, 0.18) * array
    return jnp.clip(array, min=-bound, max=bound).astype(kind)


def setup_inputs(seed: int = 0) -> dict:
    streams_of = jax.random.split(jax.random.key(seed), 9)
    pooled = draw_pooled(jax.random.fold_in(streams_of[8], 71), 0)
    hidden = scatter_about(streams_of[1], (BATCH, FF), 1.0, 6.0, ((0, 256),))
    text = draw_text(jax.random.fold_in(streams_of[8], 71), 0)
    weight = scatter_about(streams_of[3], (D, FF), FF ** -0.5, 0.09375, ((0, 32), (1, 8)), jnp.float32)
    row_moment = jnp.clip(jnp.exp(math.log(9.999999747378752e-06) - 4.6051701 * jax.random.uniform(streams_of[4], (D,), jnp.float32) ** block_levels(streams_of[4], (D,), ((0, 32),), -0.2, 0.2)), 1.0000000116860974e-07, 9.999999747378752e-06)
    col_moment = jnp.clip(jnp.exp(math.log(9.999999747378752e-06) - 4.6051701 * jax.random.uniform(streams_of[5], (FF,), jnp.float32) ** block_levels(streams_of[5], (FF,), ((0, 8),), -0.2, 0.2)), 1.0000000116860974e-07, 9.999999747378752e-06)
    log_scale = jnp.clip(jax.random.uniform(streams_of[6], (), jnp.float32, 4.2, 4.8), 4.2, 4.8)
    bias = jnp.clip(jax.random.uniform(streams_of[7], (), jnp.float32, -16.0, -12.0), -16.0, -12.0)
    return dict(pooled=pooled, hidden=hidden, text=text, weight=weight, row_moment=row_moment, col_moment=col_moment, log_scale=log_scale, bias=bias)


EPSILON = 1e-06
DECAY_RATE = 0.8
CLIP_LEVEL = 1.0
FLOOR_VALUE = 1e-30

def reference(pooled, hidden, text, weight, row_moment, col_moment, log_scale, bias):
    batch_total = TOK_DEV * N_ROW * N_COL
    weight_half = weight.astype(jnp.bfloat16)
    projected = jnp.dot(hidden, weight_half.T, preferred_element_type=jnp.float32)
    mixed_rows = pooled.astype(jnp.float32) + projected
    length = jnp.sqrt(lax.optimization_barrier(jnp.sum(mixed_rows * mixed_rows, axis=1, keepdims=True)) + EPSILON)
    image_unit = mixed_rows / length
    images = image_unit.astype(jnp.bfloat16)
    text_float = text.astype(jnp.float32)
    text_units = (text_float / jnp.sqrt(lax.optimization_barrier(jnp.sum(text_float * text_float, axis=1, keepdims=True)) + EPSILON)).astype(jnp.bfloat16)
    logit_scale = jnp.exp(log_scale.astype(jnp.float32))
    block_rows = batch_total // N_ROW
    image_blocks = images.reshape(N_ROW, block_rows, D)
    text_ids = jnp.arange(batch_total, dtype=jnp.int32)

    def one_block(block_item):
        image_block, block_index = block_item
        image_ids = block_index * block_rows + jnp.arange(block_rows, dtype=jnp.int32)
        logits = logit_scale * jnp.dot(image_block, text_units.T, preferred_element_type=jnp.float32) + bias
        label_sign = jnp.where(image_ids[:, None] == text_ids[None, :], jnp.float32(1.0), jnp.float32(-1.0))
        loss_sum = jnp.sum(jax.nn.softplus(-label_sign * logits))
        grad_logits = (-label_sign * jax.nn.sigmoid(-label_sign * logits) / batch_total).astype(jnp.bfloat16)
        return (loss_sum, logit_scale * jnp.dot(grad_logits, text_units, preferred_element_type=jnp.float32))
    loss_sums, unit_grads = lax.map(one_block, (image_blocks, jnp.arange(N_ROW, dtype=jnp.int32)))
    loss = jnp.sum(loss_sums) / batch_total
    unit_grad = unit_grads.reshape(batch_total, D)
    mixed_grad = ((unit_grad - image_unit * lax.optimization_barrier(jnp.sum(image_unit * unit_grad, axis=1, keepdims=True))) / length).astype(jnp.bfloat16)
    gradient = jnp.dot(mixed_grad.T, hidden, preferred_element_type=jnp.float32)
    squared = gradient * gradient + FLOOR_VALUE
    new_row = DECAY_RATE * row_moment + (1.0 - DECAY_RATE) * lax.optimization_barrier(jnp.mean(squared, axis=1))
    new_col = DECAY_RATE * col_moment + (1.0 - DECAY_RATE) * lax.optimization_barrier(jnp.mean(squared, axis=0))
    second = new_row[:, None] * new_col[None, :]
    raw_update = gradient / jnp.sqrt(second)
    update_rms = jnp.sqrt(jnp.mean(raw_update * raw_update))
    update = raw_update / jnp.maximum(1.0, update_rms / CLIP_LEVEL)
    return (update, new_row, new_col, loss)
```

```python
import functools

import jax
import jax.numpy as jnp
from jax import lax
from jax.sharding import Mesh
from jax.sharding import PartitionSpec as P

D = 1152
FF = 4304
ROW = ("row_0", "row_1")
COL = ("col_0", "col_1")
ROW_COL = ("row_0", "row_1", "col_0", "col_1")


EPSILON = 1e-06
DECAY_RATE = 0.8
CLIP_LEVEL = 1.0
FLOOR_VALUE = 1e-30


def laid_out(pieces, dim):
    dims = list(pieces.shape[1:])
    dims[dim] *= pieces.shape[0]
    return jnp.moveaxis(pieces, 0, dim).reshape(dims)


def sent_to_all(array, axis):
    copies = jnp.broadcast_to(array, (lax.axis_size(axis), *array.shape))
    return lax.all_to_all(copies, axis, split_axis=0, concat_axis=0, tiled=True)


def collect(array, axis, dim):
    return laid_out(sent_to_all(array, axis), dim)


def split_up(array, dim, devices):
    dims = array.shape
    pieces = array.reshape(*dims[:dim], devices, dims[dim] // devices, *dims[dim + 1 :])
    return jnp.moveaxis(pieces, dim, 0)


def sum_at_owner(array, axis, dim):
    pieces = split_up(array.astype(jnp.bfloat16), dim, lax.axis_size(axis))
    arrived = lax.all_to_all(pieces, axis, split_axis=0, concat_axis=0, tiled=True)
    return arrived.astype(jnp.float32).sum(axis=0)


def sum_by_axis(running, axes):
    for axis in axes:
        running = lax.psum_scatter(running, axis, scatter_dimension=0, tiled=True)
    return running


def of_everyone(array, axis):
    everything = sent_to_all(array, axis)
    return jnp.sum(everything, axis=0)


def one_axis_at_a_time(array, axes):
    return functools.reduce(lax.psum, axes, array)


def over_row_index(positions, column, tokens, columns):
    return (positions // tokens * columns + column) * tokens + positions % tokens


def over_col_index(positions, row_place, tokens, columns):
    return row_place * columns * tokens + positions


def pair_tile(images, image_ids, texts, text_ids, logit_scale, bias, batch_total):
    logits = logit_scale * jnp.dot(images, texts.T, preferred_element_type=jnp.float32) + bias
    label_sign = jnp.where(
        image_ids[:, None] == text_ids[None, :], jnp.float32(1.0), jnp.float32(-1.0)
    )
    loss_sum = jnp.sum(jax.nn.softplus(-label_sign * logits))
    grad_logits = (-label_sign * jax.nn.sigmoid(-label_sign * logits) / batch_total).astype(
        jnp.bfloat16
    )
    return (loss_sum, logit_scale * jnp.dot(grad_logits, texts, preferred_element_type=jnp.float32))


def per_device(pooled, hidden, text, weight, row_moment, col_moment, log_scale, bias):
    rows_count = lax.axis_size(ROW)
    cols_count = lax.axis_size(COL)
    row_place = lax.axis_index(ROW)
    col_place = lax.axis_index(COL)
    tokens = pooled.shape[0]
    batch_total = tokens * rows_count * cols_count
    split_hidden = lax.all_to_all(hidden, ROW, split_axis=1, concat_axis=0, tiled=True)
    weight_half = weight.astype(jnp.bfloat16)
    partial_proj = lax.dot_general(
        split_hidden,
        collect(weight_half, COL, 0),
        (((1,), (1,)), ((), ())),
        preferred_element_type=jnp.float32,
    )
    projected = sum_at_owner(partial_proj, ROW, 0)
    mixed_rows = pooled.astype(jnp.float32) + projected
    length = jnp.sqrt(jnp.sum(mixed_rows * mixed_rows, axis=1, keepdims=True) + EPSILON)
    image_unit = mixed_rows / length
    images = image_unit.astype(jnp.bfloat16)
    text_float = text.astype(jnp.float32)
    text_units = (
        text_float / jnp.sqrt(jnp.sum(text_float * text_float, axis=1, keepdims=True) + EPSILON)
    ).astype(jnp.bfloat16)
    logit_scale = jnp.exp(log_scale)
    image_rows = collect(images, ROW, 0)
    image_ids = over_row_index(
        jnp.arange(image_rows.shape[0], dtype=jnp.int32), col_place, tokens, cols_count
    )
    piece = lax.all_gather(text_units, COL, axis=0, tiled=True)
    text_ids = over_col_index(
        jnp.arange(piece.shape[0], dtype=jnp.int32), row_place, tokens, cols_count
    )
    loss_local, unit_part = pair_tile(
        image_rows, image_ids, piece, text_ids, logit_scale, bias, batch_total
    )
    unit_grad = sum_at_owner(unit_part, ROW, 0)
    mixed_grad = (
        (unit_grad - image_unit * jnp.sum(image_unit * unit_grad, axis=1, keepdims=True)) / length
    ).astype(jnp.bfloat16)
    grad_rows = collect(mixed_grad, ROW, 0)
    gradient = sum_at_owner(
        lax.dot_general(
            grad_rows, split_hidden, (((0,), (0,)), ((), ())), preferred_element_type=jnp.float32
        ),
        COL,
        0,
    )
    squared = gradient * gradient + FLOOR_VALUE
    row_sum = of_everyone(jnp.sum(squared, axis=1), ROW)
    col_sum = of_everyone(jnp.sum(squared, axis=0), COL)
    new_row = DECAY_RATE * row_moment + (1.0 - DECAY_RATE) * row_sum / FF
    new_col = DECAY_RATE * col_moment + (1.0 - DECAY_RATE) * col_sum / D
    second = new_row[:, None] * new_col[None, :]
    raw_update = gradient / jnp.sqrt(second)
    loss_total, update_total = lax.psum(
        (loss_local, jnp.sum(raw_update * raw_update)), ROW_COL
    )
    update_rms = jnp.sqrt(update_total / (D * FF))
    update = raw_update / jnp.maximum(1.0, update_rms / CLIP_LEVEL)
    loss = loss_total / batch_total
    return (update, new_row, new_col, loss)


def solution(mesh):
    finer = Mesh(mesh.devices.reshape(4, 2, 4, 8), ("row_0", "row_1", "col_0", "col_1"))
    return jax.shard_map(
        per_device,
        mesh=finer,
        in_specs=(
            P(ROW_COL, None),
            P(ROW_COL, None),
            P(ROW_COL, None),
            P(COL, ROW),
            P(COL),
            P(ROW),
            P(),
            P(),
        ),
        out_specs=(P(COL, ROW), P(COL), P(ROW), P()),
        check_vma=False,
    )
```

```python
import functools

import jax
import jax.numpy as jnp
from jax import lax
from jax.experimental import pallas as pl
from jax.experimental.pallas import tpu as pltpu
from jax.sharding import Mesh
from jax.sharding import PartitionSpec as P

D = 1152
FF = 4304
NX, NC, NY, NZ = 4, 2, 4, 8
TOK = 64
KD = FF // (NX * NC)
KP = 640
ED = D // (NY * NZ)
EP = 48
WLA = 256
TLA = 512
ROW = ("x", "c")
COL = ("y", "z")
ALL = ("x", "c", "y", "z")
BATCH = TOK * NX * NC * NY * NZ

EPSILON = 1e-06
DECAY_RATE = 0.8
CLIP_LEVEL = 1.0
FLOOR_VALUE = 1e-30

MESH = pl.DeviceIdType.MESH
F32 = jnp.float32
BF16 = jnp.bfloat16


def mod(value, size):
    return lax.rem(value + 2 * size, size)


class Copies:
    def __init__(self):
        self.sent = []

    def send(self, src, dst, ssem, rsem, device):
        copy = pltpu.make_async_remote_copy(src, dst, ssem, rsem, device_id=device, device_id_type=MESH)
        copy.start()
        self.sent.append(copy)

    def arrived(self, dst, ssem, rsem, device):
        pltpu.make_async_remote_copy(
            dst, dst, ssem, rsem, device_id=device, device_id_type=MESH
        ).wait_recv()

    def finish(self):
        for copy in self.sent:
            copy.wait_send()


A0, AP, AM, BP, BM, YP, YM, Y2 = 0, 4, 20, 36, 40, 44, 52, 60
N_MSG = 68
OFFSETS = [0, -1, 1, -2, 2, -3, 3, -4]


class PlaneGather:
    def __init__(self, copies, piece, a, b, la, ssem, rsem, y, z):
        self.copies, self.piece, self.a, self.b, self.la = copies, piece, a, b, la
        self.ssem, self.rsem, self.y, self.z = ssem, rsem, y, z

    def _send(self, src, dst, i, device):
        self.copies.send(src, dst, self.ssem.at[i], self.rsem.at[i], device)

    def _wait(self, dst, i, device):
        self.copies.arrived(dst, self.ssem.at[i], self.rsem.at[i], device)

    def own(self):
        self.a[self.z, self.y] = self.piece[:, : self.la]
        self.b[self.y, self.z] = self.piece[:, self.la :]

    def _a(self, zo, dy):
        return self.a.at[mod(self.z + zo, NZ), mod(self.y - dy, NY)]

    def _b(self, yo, zo):
        return self.b.at[mod(self.y + yo, NY), mod(self.z + zo, NZ)]

    def _zdev(self, o):
        return {"z": mod(self.z + o, NZ)}

    def _ydev(self, o):
        return {"y": mod(self.y + o, NY)}

    @staticmethod
    def _has(sign, s, dy):
        if s < NZ // 2:
            return s >= 1
        return s == NZ // 2 and (dy < NY // 2) == (sign > 0)

    def _ring_a(self, s, dy, sign):
        if not self._has(sign, s, dy):
            return
        src = self._a(-sign * (s - 1), dy)
        dst = src
        if s == 1 and dy == 0:
            src = self.piece.at[:, pl.ds(0, self.la)]
        self._send(src, dst, (AP if sign > 0 else AM) + (s - 1) * 4 + dy, self._zdev(sign))

    def _ring_b(self, s, sign):
        if s > (NZ // 2 if sign > 0 else NZ // 2 - 1):
            return
        dst = self._b(0, -sign * (s - 1))
        src = self.piece.at[:, pl.ds(self.la, self.piece.shape[1] - self.la)] if s == 1 else dst
        self._send(src, dst, (BP if sign > 0 else BM) + s - 1, self._zdev(sign))

    def _spread_b(self, j):
        dst = self._b(0, OFFSETS[j])
        src = self.piece.at[:, pl.ds(self.la, self.piece.shape[1] - self.la)] if j == 0 else dst
        self._send(src, dst, YP + j, self._ydev(1))
        self._send(src, dst, YM + j, self._ydev(-1))

    def _near_b(self, j):
        o = OFFSETS[j]
        self._wait(self._b(-1, o), YP + j, self._ydev(-1))
        if j % 2 == 0:
            self._send(self._b(-1, o), self._b(-1, o), Y2 + j, self._ydev(1))
        self._wait(self._b(1, o), YM + j, self._ydev(1))
        if j % 2 == 1:
            self._send(self._b(1, o), self._b(1, o), Y2 + j, self._ydev(-1))

    def far(self, j):
        o = OFFSETS[j]
        yo = -2 if j % 2 == 0 else 2
        self._wait(self._b(yo, o), Y2 + j, self._ydev(-1 if j % 2 == 0 else 1))

    def start(self):
        for dy in range(1, NY):
            self._send(self.piece.at[:, pl.ds(0, self.la)], self._a(0, 0), A0 + dy - 1, self._ydev(dy))
        for sign in (1, -1):
            self._ring_b(1, sign)
            self._ring_a(1, 0, sign)
        self._spread_b(0)

    def step(self, k):
        for s_sign in (1, -1):
            if k <= (NZ // 2 if s_sign > 0 else NZ // 2 - 1):
                self._wait(self._b(0, -s_sign * k), (BP if s_sign > 0 else BM) + k - 1, self._zdev(-s_sign))
                self._ring_b(k + 1, s_sign)
                self._spread_b(OFFSETS.index(-s_sign * k))
        for dy in range(NY):
            if k == 1:
                if dy == 0:
                    continue
                self._wait(self._a(0, dy), A0 + dy - 1, self._ydev(-dy))
                self._ring_a(1, dy, 1)
                self._ring_a(1, dy, -1)
                continue
            s = k - 1
            for sign in (1, -1):
                if self._has(sign, s, dy):
                    self._wait(
                        self._a(-sign * s, dy), (AP if sign > 0 else AM) + (s - 1) * 4 + dy, self._zdev(-sign)
                    )
                    self._ring_a(s + 1, dy, sign)
        for j, o in enumerate(OFFSETS):
            if abs(o) == k - 1:
                self._near_b(j)


def front_kernel(
    hid, wp, text, pooled, scale_ref, bias_ref,
    h_out, mg_out, loss_out,
    wa, wb, wc, ta, tb, tn, part, give, take, share, got, img, unit, length,
    acc, give2, take2, share2, got2,
    w_s, w_r, t_s, t_r, h_s, h_r, p_s, p_r, i_s, i_r, u_s, u_r, m_s, m_r,
):
    x, c = lax.axis_index("x"), lax.axis_index("c")
    y, z = lax.axis_index("y"), lax.axis_index("z")
    me = c * NX + x
    other = 1 - c

    barrier = pltpu.get_barrier_semaphore()
    peers = [{"z": mod(z + 1, NZ)}, {"z": mod(z - 1, NZ)}]
    peers += [{"y": mod(y + dy, NY)} for dy in range(1, NY)]
    peers += [
        {"x": mod(x + dx, NX), "c": lax.rem(c + dc, NC)}
        for dx in range(NX) for dc in range(NC) if dx + dc > 0
    ]
    for peer in peers:
        pl.semaphore_signal(barrier, inc=1, device_id=peer, device_id_type=MESH)
    pl.semaphore_wait(barrier, len(peers))

    copies = Copies()
    w = PlaneGather(copies, wp, wa, wb, WLA, w_s, w_r, y, z)
    t = PlaneGather(copies, tn, ta, tb, TLA, t_s, t_r, y, z)

    w.start()
    row_peers = [(dx, dc) for dx in range(NX) for dc in range(NC) if dx + dc > 0]
    for i, (dx, dc) in enumerate(row_peers):
        xx, cc = mod(x + dx, NX), lax.rem(c + dc, NC)
        copies.send(hid.at[cc * NX + xx], h_out.at[me], h_s.at[i], h_r.at[i], {"x": xx, "c": cc})
    h_out[me] = hid[me]
    w.own()
    tf = text[...].astype(F32)
    tn[...] = (tf / jnp.sqrt(jnp.sum(tf * tf, axis=1, keepdims=True) + EPSILON)).astype(BF16)
    w.step(1)
    w.step(2)
    w.step(3)
    t.own()
    t.start()
    w.step(4)
    w.step(5)
    for j in range(8):
        w.far(j)

    r_id = lax.broadcasted_iota(jnp.int32, (4 * ED, 4 * EP), 0)
    c_id = lax.broadcasted_iota(jnp.int32, (4 * ED, 4 * EP), 1)
    pick = jnp.zeros((4 * ED, 4 * EP), F32)
    for g in range(4):
        hit = (r_id >= ED * g) & (r_id < ED * (g + 1)) & (c_id - r_id == (EP - ED) * g)
        pick = jnp.where(hit, 1.0, pick)
    pick = pick.astype(BF16)
    for g in range(8):
        yy, z0 = g // 2, 4 * (g % 2)
        wc[pl.ds(4 * ED * g, 4 * ED), 0:WLA] = jnp.dot(
            pick, wa[z0 : z0 + 4, yy].reshape(4 * EP, WLA), preferred_element_type=F32
        ).astype(BF16)
        wc[pl.ds(4 * ED * g, 4 * ED), WLA:KP] = jnp.dot(
            pick, wb[yy, z0 : z0 + 4].reshape(4 * EP, KP - WLA), preferred_element_type=F32
        ).astype(BF16)

    for i, (dx, dc) in enumerate(row_peers):
        xx, cc = mod(x - dx, NX), lax.rem(c + dc, NC)
        copies.arrived(h_out.at[cc * NX + xx], h_s.at[i], h_r.at[i], {"x": xx, "c": cc})

    def project(half):
        rows = h_out[pl.ds(half * NX, NX)].reshape(NX * TOK, KP)
        for n in range(3):
            part[pl.ds(half * NX, NX), :, 384 * n : 384 * (n + 1)] = lax.dot_general(
                rows, wc[384 * n : 384 * (n + 1), :], (((1,), (1,)), ((), ())), preferred_element_type=F32
            ).reshape(NX, TOK, 384)

    def reduce_rows(val, gv, tk, sh, gt, ss, rs, between):
        gv[...] = val[pl.ds(other * NX, NX)].astype(BF16)
        between()
        copies.send(gv, tk, ss.at[0], rs.at[0], {"c": other})
        yield
        copies.arrived(tk, ss.at[0], rs.at[0], {"c": other})
        for dx in (2, 1, 3):
            xx = mod(x + dx, NX)
            sh[dx - 1] = (val[c * NX + xx] + tk[xx].astype(F32)).astype(BF16)
        for dx in (2, 1, 3):
            copies.send(sh.at[dx - 1], gt.at[dx - 1], ss.at[dx], rs.at[dx], {"x": mod(x + dx, NX)})
        yield
        total = val[me] + tk[x].astype(F32)
        for dx in (1, 3, 2):
            copies.arrived(gt.at[dx - 1], ss.at[dx], rs.at[dx], {"x": mod(x - dx, NX)})
        for dx in (1, 2, 3):
            total = total + gt[dx - 1].astype(F32)
        yield total

    def share_rows(buf, ss, rs):
        copies.send(buf.at[me], buf.at[me], ss.at[4], rs.at[4], {"c": other})
        for dx in (2, 1, 3):
            copies.send(buf.at[me], buf.at[me], ss.at[dx], rs.at[dx], {"x": mod(x + dx, NX)})
        for dx in (1, 3, 2):
            got_at = buf.at[c * NX + mod(x - dx, NX)]
            copies.arrived(got_at, ss.at[dx], rs.at[dx], {"x": mod(x - dx, NX)})
            copies.send(got_at, got_at, ss.at[4 + dx], rs.at[4 + dx], {"c": other})
        for dx in range(NX):
            copies.arrived(
                buf.at[other * NX + mod(x - dx, NX)], ss.at[4 + dx], rs.at[4 + dx], {"c": other}
            )

    project(other)
    red = reduce_rows(part, give, take, share, got, p_s, p_r, lambda: None)
    next(red)
    project(c)
    t.step(1)
    next(red)
    t.step(2)
    mixed = pooled[...].astype(F32) + next(red)
    ln = jnp.sqrt(jnp.sum(mixed * mixed, axis=1, keepdims=True) + EPSILON)
    length[...] = jnp.broadcast_to(ln, length.shape)
    un = mixed / ln
    unit[...] = un
    img[me] = un.astype(BF16)
    share_rows(img, i_s, i_r)
    t.step(3)
    t.step(4)
    t.step(5)
    for j in range(8):
        t.far(j)

    scale = scale_ref[0]
    bias = bias_ref[0]
    acc[...] = jnp.zeros_like(acc)
    loss_out[...] = jnp.zeros_like(loss_out)
    tile = 256
    col = lax.broadcasted_iota(jnp.int32, (tile, 4 * TOK), 1)
    row = lax.broadcasted_iota(jnp.int32, (tile, 4 * TOK), 0)
    n_tile = NX * NC * TOK // tile
    per = tile // TOK

    def pair(step, carry):
        g = step // n_tile
        h = lax.rem(step, n_tile)
        images = img[pl.ds(h * per, per)].reshape(tile, D)
        t_a = ta[g].reshape(NY * TOK, TLA)
        t_b = tb[:, g].reshape(NY * TOK, D - TLA)
        dims = (((1,), (1,)), ((), ()))
        logits = lax.dot_general(images[:, :TLA], t_a, dims, preferred_element_type=F32)
        logits += lax.dot_general(images[:, TLA:], t_b, dims, preferred_element_type=F32)
        logits = scale * logits + bias
        delta = TOK * (me - h * per - y) + jnp.where(g == z, 0, 1 << 20)
        same = (row - col == delta) & (col >= TOK * y) & (col < TOK * y + TOK)
        m = jnp.where(same, -logits, logits)
        e = jnp.exp(-jnp.abs(m))
        loss_out[...] += jnp.sum(
            (jnp.maximum(m, 0.0) + jnp.log1p(e)).reshape(tile // 8, 8, NY * TOK), axis=0
        )
        sig = jnp.where(m >= 0.0, 1.0, e) / (1.0 + e)
        pg = (jnp.where(same, -sig, sig) * (1.0 / BATCH)).astype(BF16)
        acc[pl.ds(h * per, per), :, :TLA] += jnp.dot(pg, t_a, preferred_element_type=F32).reshape(per, TOK, TLA)
        acc[pl.ds(h * per, per), :, TLA:] += jnp.dot(pg, t_b, preferred_element_type=F32).reshape(per, TOK, D - TLA)
        return carry

    lax.fori_loop(0, NZ * n_tile, pair, 0)

    red = reduce_rows(acc, give2, take2, share2, got2, u_s, u_r, lambda: None)
    next(red)
    next(red)
    ug = scale * next(red)
    un = unit[...]
    ln = length[:, 0:1]
    mg_out[me] = ((ug - un * jnp.sum(un * ug, axis=1, keepdims=True)) / ln).astype(BF16)
    share_rows(mg_out, m_s, m_r)
    copies.finish()


def front(hid, wp, text, pooled, scale, bias):
    vmem = pl.BlockSpec(memory_space=pltpu.VMEM)
    smem = pl.BlockSpec(memory_space=pltpu.SMEM)
    n_row = NX * NC
    dma = pltpu.SemaphoreType.DMA
    return pl.pallas_call(
        front_kernel,
        out_shape=(
            jax.ShapeDtypeStruct((n_row, TOK, KP), BF16),
            jax.ShapeDtypeStruct((n_row, TOK, D), BF16),
            jax.ShapeDtypeStruct((8, NY * TOK), F32),
        ),
        in_specs=[vmem, vmem, vmem, vmem, smem, smem],
        out_specs=(vmem, vmem, vmem),
        scratch_shapes=[
            pltpu.VMEM((NZ, NY, EP, WLA), BF16),
            pltpu.VMEM((NY, NZ, EP, KP - WLA), BF16),
            pltpu.VMEM((D, KP), BF16),
            pltpu.VMEM((NZ, NY, TOK, TLA), BF16),
            pltpu.VMEM((NY, NZ, TOK, D - TLA), BF16),
            pltpu.VMEM((TOK, D), BF16),
            pltpu.VMEM((n_row, TOK, D), F32),
            pltpu.VMEM((NX, TOK, D), BF16),
            pltpu.VMEM((NX, TOK, D), BF16),
            pltpu.VMEM((NX - 1, TOK, D), BF16),
            pltpu.VMEM((NX - 1, TOK, D), BF16),
            pltpu.VMEM((n_row, TOK, D), BF16),
            pltpu.VMEM((TOK, D), F32),
            pltpu.VMEM((TOK, 128), F32),
            pltpu.VMEM((n_row, TOK, D), F32),
            pltpu.VMEM((NX, TOK, D), BF16),
            pltpu.VMEM((NX, TOK, D), BF16),
            pltpu.VMEM((NX - 1, TOK, D), BF16),
            pltpu.VMEM((NX - 1, TOK, D), BF16),
            dma((N_MSG,)), dma((N_MSG,)), dma((N_MSG,)), dma((N_MSG,)),
            dma((8,)), dma((8,)), dma((4,)), dma((4,)), dma((8,)), dma((8,)),
            dma((4,)), dma((4,)), dma((8,)), dma((8,)),
        ],
        compiler_params=pltpu.CompilerParams(
            collective_id=0, has_side_effects=True, vmem_limit_bytes=60 * 1024 * 1024
        ),
        name="front",
    )(hid, wp, text, pooled, scale, bias)


def split_up(array, dim, devices):
    dims = array.shape
    pieces = array.reshape(*dims[:dim], devices, dims[dim] // devices, *dims[dim + 1 :])
    return jnp.moveaxis(pieces, dim, 0)


def sum_at_owner(array, axis, dim):
    pieces = split_up(array.astype(BF16), dim, lax.axis_size(axis))
    arrived = lax.all_to_all(pieces, axis, split_axis=0, concat_axis=0, tiled=True)
    return arrived.astype(F32).sum(axis=0)


def of_everyone(array, axis):
    copies = jnp.broadcast_to(array, (lax.axis_size(axis), *array.shape))
    return jnp.sum(lax.all_to_all(copies, axis, split_axis=0, concat_axis=0, tiled=True), axis=0)


def per_device(pooled, hidden, text, weight, row_moment, col_moment, log_scale, bias):
    hid = hidden.reshape(TOK, NX, NC, KD).transpose(2, 1, 0, 3).reshape(NX * NC, TOK, KD)
    hid = jnp.pad(hid, ((0, 0), (0, 0), (0, KP - KD)))
    wp = jnp.pad(weight.astype(BF16), ((0, EP - ED), (0, KP - KD)))
    h_all, mg_all, loss_tile = front(
        hid, wp, text, pooled, jnp.exp(log_scale).reshape(1), bias.reshape(1)
    )
    loss_local = jnp.sum(loss_tile)
    full = lax.dot_general(
        mg_all.reshape(-1, D), h_all.reshape(-1, KP)[:, :KD], (((0,), (0,)), ((), ())), preferred_element_type=F32
    )
    gradient = sum_at_owner(full, COL, 0)
    squared = gradient * gradient + FLOOR_VALUE
    row_sum = of_everyone(jnp.sum(squared, axis=1), ROW)
    col_sum = of_everyone(jnp.sum(squared, axis=0), COL)
    new_row = DECAY_RATE * row_moment + (1.0 - DECAY_RATE) * row_sum / FF
    new_col = DECAY_RATE * col_moment + (1.0 - DECAY_RATE) * col_sum / D
    second = new_row[:, None] * new_col[None, :]
    raw_update = gradient / jnp.sqrt(second)
    loss_total, update_total = lax.psum((loss_local, jnp.sum(raw_update * raw_update)), ALL)
    update_rms = jnp.sqrt(update_total / (D * FF))
    update = raw_update / jnp.maximum(1.0, update_rms / CLIP_LEVEL)
    return (update, new_row, new_col, loss_total / BATCH)


def solution(mesh):
    finer = Mesh(mesh.devices.reshape(NX, NC, NY, NZ), ALL)
    return jax.shard_map(
        per_device,
        mesh=finer,
        in_specs=(
            P(ALL, None), P(ALL, None), P(ALL, None), P(COL, ROW), P(COL), P(ROW), P(), P(),
        ),
        out_specs=(P(COL, ROW), P(COL), P(ROW), P()),
        check_vma=False,
    )
```

```python
import functools

import jax
import jax.numpy as jnp
from jax import lax
from jax.experimental import pallas as pl
from jax.experimental.pallas import tpu as pltpu
from jax.sharding import Mesh
from jax.sharding import PartitionSpec as P

D = 1152
FF = 4304
NX, NC, NY, NZ = 4, 2, 4, 8
TOK = 64
KD = FF // (NX * NC)
KP = 640
ED = D // (NY * NZ)
EP = 48
WLA = 256
TLA = 512
EG = 40
GLA = 512
ROW = ("x", "c")
COL = ("y", "z")
ALL = ("x", "c", "y", "z")
BATCH = TOK * NX * NC * NY * NZ

EPSILON = 1e-06
DECAY_RATE = 0.8
CLIP_LEVEL = 1.0
FLOOR_VALUE = 1e-30

MESH = pl.DeviceIdType.MESH
F32 = jnp.float32
BF16 = jnp.bfloat16


def mod(value, size):
    return lax.rem(value + 2 * size, size)


class Copies:
    def __init__(self):
        self.sent = []

    def send(self, src, dst, ssem, rsem, device):
        copy = pltpu.make_async_remote_copy(src, dst, ssem, rsem, device_id=device, device_id_type=MESH)
        copy.start()
        self.sent.append(copy)

    def arrived(self, dst, ssem, rsem, device):
        pltpu.make_async_remote_copy(
            dst, dst, ssem, rsem, device_id=device, device_id_type=MESH
        ).wait_recv()

    def finish(self):
        for copy in self.sent:
            copy.wait_send()


A0, AP, AM, BP, BM, YP, YM, Y2 = 0, 4, 20, 36, 40, 44, 52, 60
N_MSG = 68
OFFSETS = [0, -1, 1, -2, 2, -3, 3, -4]


class PlaneGather:
    def __init__(self, copies, piece, a, b, la, ssem, rsem, y, z):
        self.copies, self.piece, self.a, self.b, self.la = copies, piece, a, b, la
        self.ssem, self.rsem, self.y, self.z = ssem, rsem, y, z

    def _send(self, src, dst, i, device):
        self.copies.send(src, dst, self.ssem.at[i], self.rsem.at[i], device)

    def _wait(self, dst, i, device):
        self.copies.arrived(dst, self.ssem.at[i], self.rsem.at[i], device)

    def own(self):
        self.a[self.z, self.y] = self.piece[:, : self.la]
        self.b[self.y, self.z] = self.piece[:, self.la :]

    def _a(self, zo, dy):
        return self.a.at[mod(self.z + zo, NZ), mod(self.y - dy, NY)]

    def _b(self, yo, zo):
        return self.b.at[mod(self.y + yo, NY), mod(self.z + zo, NZ)]

    def _zdev(self, o):
        return {"z": mod(self.z + o, NZ)}

    def _ydev(self, o):
        return {"y": mod(self.y + o, NY)}

    @staticmethod
    def _has(sign, s, dy):
        if s < NZ // 2:
            return s >= 1
        return s == NZ // 2 and (dy < NY // 2) == (sign > 0)

    def _ring_a(self, s, dy, sign):
        if not self._has(sign, s, dy):
            return
        src = self._a(-sign * (s - 1), dy)
        dst = src
        if s == 1 and dy == 0:
            src = self.piece.at[:, pl.ds(0, self.la)]
        self._send(src, dst, (AP if sign > 0 else AM) + (s - 1) * 4 + dy, self._zdev(sign))

    def _ring_b(self, s, sign):
        if s > (NZ // 2 if sign > 0 else NZ // 2 - 1):
            return
        dst = self._b(0, -sign * (s - 1))
        src = self.piece.at[:, pl.ds(self.la, self.piece.shape[1] - self.la)] if s == 1 else dst
        self._send(src, dst, (BP if sign > 0 else BM) + s - 1, self._zdev(sign))

    def _spread_b(self, j):
        dst = self._b(0, OFFSETS[j])
        src = self.piece.at[:, pl.ds(self.la, self.piece.shape[1] - self.la)] if j == 0 else dst
        self._send(src, dst, YP + j, self._ydev(1))
        self._send(src, dst, YM + j, self._ydev(-1))

    def _near_b(self, j):
        o = OFFSETS[j]
        self._wait(self._b(-1, o), YP + j, self._ydev(-1))
        if j % 2 == 0:
            self._send(self._b(-1, o), self._b(-1, o), Y2 + j, self._ydev(1))
        self._wait(self._b(1, o), YM + j, self._ydev(1))
        if j % 2 == 1:
            self._send(self._b(1, o), self._b(1, o), Y2 + j, self._ydev(-1))

    def far(self, j):
        o = OFFSETS[j]
        yo = -2 if j % 2 == 0 else 2
        self._wait(self._b(yo, o), Y2 + j, self._ydev(-1 if j % 2 == 0 else 1))

    def start(self):
        for dy in range(1, NY):
            self._send(self.piece.at[:, pl.ds(0, self.la)], self._a(0, 0), A0 + dy - 1, self._ydev(dy))
        for sign in (1, -1):
            self._ring_b(1, sign)
            self._ring_a(1, 0, sign)
        self._spread_b(0)

    def step(self, k):
        for s_sign in (1, -1):
            if k <= (NZ // 2 if s_sign > 0 else NZ // 2 - 1):
                self._wait(self._b(0, -s_sign * k), (BP if s_sign > 0 else BM) + k - 1, self._zdev(-s_sign))
                self._ring_b(k + 1, s_sign)
                self._spread_b(OFFSETS.index(-s_sign * k))
        for dy in range(NY):
            if k == 1:
                if dy == 0:
                    continue
                self._wait(self._a(0, dy), A0 + dy - 1, self._ydev(-dy))
                self._ring_a(1, dy, 1)
                self._ring_a(1, dy, -1)
                continue
            s = k - 1
            for sign in (1, -1):
                if self._has(sign, s, dy):
                    self._wait(
                        self._a(-sign * s, dy), (AP if sign > 0 else AM) + (s - 1) * 4 + dy, self._zdev(-sign)
                    )
                    self._ring_a(s + 1, dy, sign)
        for j, o in enumerate(OFFSETS):
            if abs(o) == k - 1:
                self._near_b(j)


def whole_kernel(
    hid, wp, text, pooled, row_moment, col_moment, scale_ref, bias_ref,
    update_out, row_out, col_out, total_out,
    h_out, mg_out, loss_out,
    wa, wb, wc, ta, tb, tn, part, give, take, share, got, img, unit, length,
    acc, give2, take2, share2, got2,
    grad, far_p, far_m, near_p, near_m, relay_p, relay_m,
    r_far_p, r_far_m, r_near_p, r_near_m, r_relay_p, r_relay_m,
    z_give, z_take, b_give, b_take, yb_give, yb_take,
    row_give, row_take, cy_give, cy_take, cz_give, cz_take,
    s_give, s_take, sy_give, sy_take, sz_give, sz_take,
    w_s, w_r, t_s, t_r, h_s, h_r, p_s, p_r, i_s, i_r, u_s, u_r, m_s, m_r,
    g_s, g_r, z_s, z_r, b_s, b_r, yb_s, yb_r, st_s, st_r,
):
    x, c = lax.axis_index("x"), lax.axis_index("c")
    y, z = lax.axis_index("y"), lax.axis_index("z")
    me = c * NX + x
    other = 1 - c

    barrier = pltpu.get_barrier_semaphore()
    peers = [{"z": mod(z + dz, NZ)} for dz in range(1, NZ)]
    peers += [{"y": mod(y + dy, NY)} for dy in range(1, NY)]
    peers += [
        {"x": mod(x + dx, NX), "c": lax.rem(c + dc, NC)}
        for dx in range(NX) for dc in range(NC) if dx + dc > 0
    ]
    for peer in peers:
        pl.semaphore_signal(barrier, inc=1, device_id=peer, device_id_type=MESH)
    pl.semaphore_wait(barrier, len(peers))

    copies = Copies()
    w = PlaneGather(copies, wp, wa, wb, WLA, w_s, w_r, y, z)
    t = PlaneGather(copies, tn, ta, tb, TLA, t_s, t_r, y, z)

    w.start()
    row_peers = [(dx, dc) for dx in range(NX) for dc in range(NC) if dx + dc > 0]
    for i, (dx, dc) in enumerate(row_peers):
        xx, cc = mod(x + dx, NX), lax.rem(c + dc, NC)
        copies.send(hid.at[cc * NX + xx], h_out.at[me], h_s.at[i], h_r.at[i], {"x": xx, "c": cc})
    h_out[me] = hid[me]
    w.own()
    tf = text[...].astype(F32)
    tn[...] = (tf / jnp.sqrt(jnp.sum(tf * tf, axis=1, keepdims=True) + EPSILON)).astype(BF16)
    w.step(1)
    w.step(2)
    w.step(3)
    t.own()
    t.start()
    w.step(4)
    w.step(5)
    for j in range(8):
        w.far(j)

    r_id = lax.broadcasted_iota(jnp.int32, (4 * ED, 4 * EP), 0)
    c_id = lax.broadcasted_iota(jnp.int32, (4 * ED, 4 * EP), 1)
    pick = jnp.zeros((4 * ED, 4 * EP), F32)
    for g in range(4):
        hit = (r_id >= ED * g) & (r_id < ED * (g + 1)) & (c_id - r_id == (EP - ED) * g)
        pick = jnp.where(hit, 1.0, pick)
    pick = pick.astype(BF16)
    for g in range(8):
        yy, z0 = g // 2, 4 * (g % 2)
        wc[pl.ds(4 * ED * g, 4 * ED), 0:WLA] = jnp.dot(
            pick, wa[z0 : z0 + 4, yy].reshape(4 * EP, WLA), preferred_element_type=F32
        ).astype(BF16)
        wc[pl.ds(4 * ED * g, 4 * ED), WLA:KP] = jnp.dot(
            pick, wb[yy, z0 : z0 + 4].reshape(4 * EP, KP - WLA), preferred_element_type=F32
        ).astype(BF16)

    for i, (dx, dc) in enumerate(row_peers):
        xx, cc = mod(x - dx, NX), lax.rem(c + dc, NC)
        copies.arrived(h_out.at[cc * NX + xx], h_s.at[i], h_r.at[i], {"x": xx, "c": cc})

    def project(half):
        rows = h_out[pl.ds(half * NX, NX)].reshape(NX * TOK, KP)
        for n in range(3):
            part[pl.ds(half * NX, NX), :, 384 * n : 384 * (n + 1)] = lax.dot_general(
                rows, wc[384 * n : 384 * (n + 1), :], (((1,), (1,)), ((), ())), preferred_element_type=F32
            ).reshape(NX, TOK, 384)

    def reduce_rows(val, gv, tk, sh, gt, ss, rs, between):
        gv[...] = val[pl.ds(other * NX, NX)].astype(BF16)
        between()
        copies.send(gv, tk, ss.at[0], rs.at[0], {"c": other})
        yield
        copies.arrived(tk, ss.at[0], rs.at[0], {"c": other})
        for dx in (2, 1, 3):
            xx = mod(x + dx, NX)
            sh[dx - 1] = (val[c * NX + xx] + tk[xx].astype(F32)).astype(BF16)
        for dx in (2, 1, 3):
            copies.send(sh.at[dx - 1], gt.at[dx - 1], ss.at[dx], rs.at[dx], {"x": mod(x + dx, NX)})
        yield
        total = val[me] + tk[x].astype(F32)
        for dx in (1, 3, 2):
            copies.arrived(gt.at[dx - 1], ss.at[dx], rs.at[dx], {"x": mod(x - dx, NX)})
        for dx in (1, 2, 3):
            total = total + gt[dx - 1].astype(F32)
        yield total

    def share_rows(buf, ss, rs):
        copies.send(buf.at[me], buf.at[me], ss.at[4], rs.at[4], {"c": other})
        for dx in (2, 1, 3):
            copies.send(buf.at[me], buf.at[me], ss.at[dx], rs.at[dx], {"x": mod(x + dx, NX)})
        for dx in (1, 3, 2):
            got_at = buf.at[c * NX + mod(x - dx, NX)]
            copies.arrived(got_at, ss.at[dx], rs.at[dx], {"x": mod(x - dx, NX)})
            copies.send(got_at, got_at, ss.at[4 + dx], rs.at[4 + dx], {"c": other})
        for dx in range(NX):
            copies.arrived(
                buf.at[other * NX + mod(x - dx, NX)], ss.at[4 + dx], rs.at[4 + dx], {"c": other}
            )

    project(other)
    red = reduce_rows(part, give, take, share, got, p_s, p_r, lambda: None)
    next(red)
    project(c)
    t.step(1)
    next(red)
    t.step(2)
    mixed = pooled[...].astype(F32) + next(red)
    ln = jnp.sqrt(jnp.sum(mixed * mixed, axis=1, keepdims=True) + EPSILON)
    length[...] = jnp.broadcast_to(ln, length.shape)
    un = mixed / ln
    unit[...] = un
    img[me] = un.astype(BF16)
    share_rows(img, i_s, i_r)
    t.step(3)
    t.step(4)
    t.step(5)
    for j in range(8):
        t.far(j)

    scale = scale_ref[0]
    bias = bias_ref[0]
    acc[...] = jnp.zeros_like(acc)
    loss_out[...] = jnp.zeros_like(loss_out)
    tile = 256
    col = lax.broadcasted_iota(jnp.int32, (tile, 4 * TOK), 1)
    row = lax.broadcasted_iota(jnp.int32, (tile, 4 * TOK), 0)
    n_tile = NX * NC * TOK // tile
    per = tile // TOK

    def pair(step, carry):
        g = step // n_tile
        h = lax.rem(step, n_tile)
        images = img[pl.ds(h * per, per)].reshape(tile, D)
        t_a = ta[g].reshape(NY * TOK, TLA)
        t_b = tb[:, g].reshape(NY * TOK, D - TLA)
        dims = (((1,), (1,)), ((), ()))
        logits = lax.dot_general(images[:, :TLA], t_a, dims, preferred_element_type=F32)
        logits += lax.dot_general(images[:, TLA:], t_b, dims, preferred_element_type=F32)
        logits = scale * logits + bias
        delta = TOK * (me - h * per - y) + jnp.where(g == z, 0, 1 << 20)
        same = (row - col == delta) & (col >= TOK * y) & (col < TOK * y + TOK)
        m = jnp.where(same, -logits, logits)
        e = jnp.exp(-jnp.abs(m))
        loss_out[...] += jnp.sum(
            (jnp.maximum(m, 0.0) + jnp.log1p(e)).reshape(tile // 8, 8, NY * TOK), axis=0
        )
        sig = jnp.where(m >= 0.0, 1.0, e) / (1.0 + e)
        pg = (jnp.where(same, -sig, sig) * (1.0 / BATCH)).astype(BF16)
        acc[pl.ds(h * per, per), :, :TLA] += jnp.dot(pg, t_a, preferred_element_type=F32).reshape(per, TOK, TLA)
        acc[pl.ds(h * per, per), :, TLA:] += jnp.dot(pg, t_b, preferred_element_type=F32).reshape(per, TOK, D - TLA)
        return carry

    lax.fori_loop(0, NZ * n_tile, pair, 0)

    red = reduce_rows(acc, give2, take2, share2, got2, u_s, u_r, lambda: None)
    next(red)
    next(red)
    ug = scale * next(red)
    un = unit[...]
    ln = length[:, 0:1]
    mg_out[me] = ((ug - un * jnp.sum(un * ug, axis=1, keepdims=True)) / ln).astype(BF16)
    share_rows(mg_out, m_s, m_r)

    zi = lax.broadcasted_iota(jnp.int32, (NZ, EG, 384), 0)
    ji = lax.broadcasted_iota(jnp.int32, (NZ, EG, 384), 1)
    li = lax.broadcasted_iota(jnp.int32, (NZ, EG, 384), 2)
    h_all = h_out[...].reshape(NX * NC * TOK, KP)

    def gradient_of(yy):
        choose = jnp.where((ji < ED) & (li == 32 * yy + ED * zi + ji), 1.0, 0.0)
        choose = choose.reshape(NZ * EG, 384).astype(BF16)
        mg = mg_out[:, :, pl.ds(pl.multiple_of(256 * yy, 128), 384)].reshape(NX * NC * TOK, 384)
        mg_t = lax.dot_general(choose, mg, (((1,), (1,)), ((), ())), preferred_element_type=F32).astype(BF16)
        grad[yy] = jnp.dot(mg_t, h_all, preferred_element_type=F32).reshape(NZ, EG, KP)
        b_give[:, yy] = grad[yy, :, :, GLA:].astype(BF16)

    half = NZ // 2
    y_far, y_up, y_down = mod(y + 2, NY), mod(y + 1, NY), mod(y - 1, NY)
    up, down = {"y": y_up}, {"y": y_down}
    gradient_of(y_far)
    far_p[...] = grad[y_far, :half, :, :GLA].astype(BF16)
    far_m[...] = grad[y_far, half:, :, :GLA].astype(BF16)
    copies.send(far_p, r_far_p, g_s.at[0], g_r.at[0], up)
    copies.send(far_m, r_far_m, g_s.at[1], g_r.at[1], down)
    gradient_of(y_up)
    near_p[...] = grad[y_up, half:, :, :GLA].astype(BF16)
    copies.send(near_p, r_near_p, g_s.at[2], g_r.at[2], up)
    gradient_of(y_down)
    near_m[...] = grad[y_down, :half, :, :GLA].astype(BF16)
    copies.send(near_m, r_near_m, g_s.at[3], g_r.at[3], down)
    gradient_of(y)
    copies.arrived(r_far_p, g_s.at[0], g_r.at[0], down)
    relay_p[...] = (grad[y_up, :half, :, :GLA] + r_far_p[...].astype(F32)).astype(BF16)
    copies.send(relay_p, r_relay_p, g_s.at[4], g_r.at[4], up)
    copies.arrived(r_far_m, g_s.at[1], g_r.at[1], up)
    relay_m[...] = (grad[y_down, half:, :, :GLA] + r_far_m[...].astype(F32)).astype(BF16)
    copies.send(relay_m, r_relay_m, g_s.at[5], g_r.at[5], down)
    z_order = (4, 3, 5, 2, 6, 1, 7)
    z_near = (1, 7, 2, 6, 3, 5, 4)
    for dz in z_order:
        zz = mod(z + dz, NZ)
        copies.send(b_give.at[zz], b_take.at[dz - 1], b_s.at[dz - 1], b_r.at[dz - 1], {"z": zz})
    copies.arrived(r_near_p, g_s.at[2], g_r.at[2], down)
    copies.arrived(r_near_m, g_s.at[3], g_r.at[3], up)
    copies.arrived(r_relay_p, g_s.at[4], g_r.at[4], down)
    copies.arrived(r_relay_m, g_s.at[5], g_r.at[5], up)
    grad[y, :half, :, :GLA] += r_relay_p[...].astype(F32) + r_near_m[...].astype(F32)
    grad[y, half:, :, :GLA] += r_near_p[...].astype(F32) + r_relay_m[...].astype(F32)
    z_give[...] = grad[y, :, :, :GLA].astype(z_give.dtype)
    for dz in z_order:
        zz = mod(z + dz, NZ)
        copies.send(z_give.at[zz], z_take.at[dz - 1], z_s.at[dz - 1], z_r.at[dz - 1], {"z": zz})
    part_b = grad[:, pl.ds(z, 1), :, GLA:].reshape(NY, EG, KP - GLA)
    for dz in z_near:
        copies.arrived(b_take.at[dz - 1], b_s.at[dz - 1], b_r.at[dz - 1], {"z": mod(z - dz, NZ)})
        part_b = part_b + b_take[dz - 1].astype(F32)
    yb_give[...] = part_b
    for dy in (2, 1, 3):
        yy = mod(y + dy, NY)
        copies.send(yb_give.at[yy], yb_take.at[dy - 1], yb_s.at[dy - 1], yb_r.at[dy - 1], {"y": yy})
    right = yb_give[y]
    for dy in (1, 3, 2):
        copies.arrived(yb_take.at[dy - 1], yb_s.at[dy - 1], yb_r.at[dy - 1], {"y": mod(y - dy, NY)})
        right = right + yb_take[dy - 1]
    left = grad[y, pl.ds(z, 1), :, :GLA].reshape(EG, GLA)
    for dz in z_near:
        copies.arrived(z_take.at[dz - 1], z_s.at[dz - 1], z_r.at[dz - 1], {"z": mod(z - dz, NZ)})
        left = left + z_take[dz - 1].astype(F32)
    grad[y, pl.ds(z, 1), :, :GLA] = left.reshape(1, EG, GLA)
    grad[y, pl.ds(z, 1), :, GLA:] = right.reshape(1, EG, KP - GLA)

    g = grad[y, pl.ds(z, 1)].reshape(EG, KP)
    e_id = lax.broadcasted_iota(jnp.int32, (EG, KP), 0)
    k_id = lax.broadcasted_iota(jnp.int32, (EG, KP), 1)
    squared = jnp.where((e_id < ED) & (k_id < KD), g * g + FLOOR_VALUE, 0.0)

    def exchange(give_ref, take_ref, base, value, kind):
        give_ref[...] = value
        sizes = {"row": row_peers, "y": range(1, NY), "z": range(1, NZ)}[kind]
        for i, d in enumerate(sizes):
            if kind == "row":
                device = {"x": mod(x + d[0], NX), "c": lax.rem(c + d[1], NC)}
            else:
                device = {kind: mod((y if kind == "y" else z) + d, NY if kind == "y" else NZ)}
            copies.send(give_ref, take_ref.at[i], st_s.at[base + i], st_r.at[base + i], device)

    def collected(take_ref, base, value, kind):
        sizes = {"row": row_peers, "y": range(1, NY), "z": range(1, NZ)}[kind]
        for i, d in enumerate(sizes):
            if kind == "row":
                device = {"x": mod(x - d[0], NX), "c": lax.rem(c + d[1], NC)}
            else:
                device = {kind: mod((y if kind == "y" else z) - d, NY if kind == "y" else NZ)}
            copies.arrived(take_ref.at[i], st_s.at[base + i], st_r.at[base + i], device)
            value = value + take_ref[i]
        return value

    cols = jnp.sum(squared, axis=0, keepdims=True)
    rows = jnp.broadcast_to(jnp.sum(squared, axis=1, keepdims=True), (EG, 128))
    exchange(cy_give, cy_take, 7, cols, "y")
    exchange(row_give, row_take, 0, rows, "row")
    cols = collected(cy_take, 7, cols, "y")
    exchange(cz_give, cz_take, 10, cols, "z")
    rows = collected(row_take, 0, rows, "row")
    new_row = DECAY_RATE * row_moment[...] + (1.0 - DECAY_RATE) * rows / FF
    row_out[...] = new_row
    new_row = jnp.where(e_id[:, 0:128] < ED, new_row, 1.0)[:, 0:1]
    cols = collected(cz_take, 10, cols, "z")
    new_col = DECAY_RATE * col_moment[...] + (1.0 - DECAY_RATE) * cols / D
    col_out[...] = new_col
    new_col = jnp.where(k_id[0:1] < KD, new_col, 1.0)
    raw = g / jnp.sqrt(new_row * new_col)
    raw_sum = jnp.sum(jnp.sum(raw * raw, axis=0, keepdims=True), axis=1, keepdims=True)
    loss_sum = jnp.sum(jnp.sum(loss_out[...], axis=0, keepdims=True), axis=1, keepdims=True)
    lane = k_id[0:1, 0:128]
    both = jnp.where(lane == 0, raw_sum, jnp.where(lane == 1, loss_sum, 0.0))
    exchange(s_give, s_take, 17, both, "row")
    both = collected(s_take, 17, both, "row")
    exchange(sy_give, sy_take, 24, both, "y")
    both = collected(sy_take, 24, both, "y")
    exchange(sz_give, sz_take, 27, both, "z")
    both = collected(sz_take, 27, both, "z")
    total_out[...] = both / BATCH
    rms = jnp.sqrt(both[:, 0:1] / (D * FF))
    upd = raw / jnp.maximum(1.0, rms / CLIP_LEVEL)
    update_out[...] = upd[:ED, :KD]
    copies.finish()


def step_kernel(hid, wp, text, pooled, row_moment, col_moment, scale, bias):
    vmem = pl.BlockSpec(memory_space=pltpu.VMEM)
    smem = pl.BlockSpec(memory_space=pltpu.SMEM)
    n_row = NX * NC
    dma = pltpu.SemaphoreType.DMA
    return pl.pallas_call(
        whole_kernel,
        out_shape=(
            jax.ShapeDtypeStruct((ED, KD), F32),
            jax.ShapeDtypeStruct((EG, 128), F32),
            jax.ShapeDtypeStruct((1, KP), F32),
            jax.ShapeDtypeStruct((1, 128), F32),
        ),
        in_specs=[vmem] * 6 + [smem] * 2,
        out_specs=(vmem,) * 4,
        scratch_shapes=[
            pltpu.VMEM((n_row, TOK, KP), BF16),
            pltpu.VMEM((n_row, TOK, D), BF16),
            pltpu.VMEM((8, NY * TOK), F32),
            pltpu.VMEM((NZ, NY, EP, WLA), BF16),
            pltpu.VMEM((NY, NZ, EP, KP - WLA), BF16),
            pltpu.VMEM((D, KP), BF16),
            pltpu.VMEM((NZ, NY, TOK, TLA), BF16),
            pltpu.VMEM((NY, NZ, TOK, D - TLA), BF16),
            pltpu.VMEM((TOK, D), BF16),
            pltpu.VMEM((n_row, TOK, D), F32),
            pltpu.VMEM((NX, TOK, D), BF16),
            pltpu.VMEM((NX, TOK, D), BF16),
            pltpu.VMEM((NX - 1, TOK, D), BF16),
            pltpu.VMEM((NX - 1, TOK, D), BF16),
            pltpu.VMEM((n_row, TOK, D), BF16),
            pltpu.VMEM((TOK, D), F32),
            pltpu.VMEM((TOK, 128), F32),
            pltpu.VMEM((n_row, TOK, D), F32),
            pltpu.VMEM((NX, TOK, D), BF16),
            pltpu.VMEM((NX, TOK, D), BF16),
            pltpu.VMEM((NX - 1, TOK, D), BF16),
            pltpu.VMEM((NX - 1, TOK, D), BF16),
            pltpu.VMEM((NY, NZ, EG, KP), F32),
            *[pltpu.VMEM((NZ // 2, EG, GLA), BF16)] * 12,
            pltpu.VMEM((NZ, EG, GLA), BF16),
            pltpu.VMEM((NZ - 1, EG, GLA), BF16),
            pltpu.VMEM((NZ, NY, EG, KP - GLA), BF16),
            pltpu.VMEM((NZ - 1, NY, EG, KP - GLA), BF16),
            pltpu.VMEM((NY, EG, KP - GLA), F32),
            pltpu.VMEM((NY - 1, EG, KP - GLA), F32),
            pltpu.VMEM((EG, 128), F32),
            pltpu.VMEM((n_row - 1, EG, 128), F32),
            pltpu.VMEM((1, KP), F32),
            pltpu.VMEM((NY - 1, 1, KP), F32),
            pltpu.VMEM((1, KP), F32),
            pltpu.VMEM((NZ - 1, 1, KP), F32),
            pltpu.VMEM((1, 128), F32),
            pltpu.VMEM((n_row - 1, 1, 128), F32),
            pltpu.VMEM((1, 128), F32),
            pltpu.VMEM((NY - 1, 1, 128), F32),
            pltpu.VMEM((1, 128), F32),
            pltpu.VMEM((NZ - 1, 1, 128), F32),
            dma((N_MSG,)), dma((N_MSG,)), dma((N_MSG,)), dma((N_MSG,)),
            dma((8,)), dma((8,)), dma((4,)), dma((4,)), dma((8,)), dma((8,)),
            dma((4,)), dma((4,)), dma((8,)), dma((8,)),
            dma((6,)), dma((6,)), dma((7,)), dma((7,)), dma((7,)), dma((7,)),
            dma((3,)), dma((3,)), dma((34,)), dma((34,)),
        ],
        compiler_params=pltpu.CompilerParams(
            collective_id=0, has_side_effects=True, vmem_limit_bytes=60 * 1024 * 1024
        ),
        name="step",
    )(hid, wp, text, pooled, row_moment, col_moment, scale, bias)


def per_device(pooled, hidden, text, weight, row_moment, col_moment, log_scale, bias):
    hid = hidden.reshape(TOK, NX, NC, KD).transpose(2, 1, 0, 3).reshape(NX * NC, TOK, KD)
    hid = jnp.pad(hid, ((0, 0), (0, 0), (0, KP - KD)))
    wp = jnp.pad(weight.astype(BF16), ((0, EP - ED), (0, KP - KD)))
    row_tile = jnp.broadcast_to(jnp.pad(row_moment, (0, EG - ED))[:, None], (EG, 128))
    col_tile = jnp.pad(col_moment, (0, KP - KD)).reshape(1, KP)
    update, new_row, new_col, total = step_kernel(
        hid, wp, text, pooled, row_tile, col_tile, jnp.exp(log_scale).reshape(1), bias.reshape(1)
    )
    return (update, new_row[:ED, 0], new_col[0, :KD], total[0, 1])


def solution(mesh):
    finer = Mesh(mesh.devices.reshape(NX, NC, NY, NZ), ALL)
    return jax.shard_map(
        per_device,
        mesh=finer,
        in_specs=(
            P(ALL, None), P(ALL, None), P(ALL, None), P(COL, ROW), P(COL), P(ROW), P(), P(),
        ),
        out_specs=(P(COL, ROW), P(COL), P(ROW), P()),
        check_vma=False,
    )
```

```python
import functools

import jax
import jax.numpy as jnp
from jax import lax
from jax.experimental import pallas as pl
from jax.experimental.pallas import tpu as pltpu
from jax.sharding import Mesh
from jax.sharding import PartitionSpec as P

D = 1152
FF = 4304
NX, NC, NY, NZ = 4, 2, 4, 8
TOK = 64
KD = FF // (NX * NC)
KP = 640
ED = D // (NY * NZ)
EP = 48
WLA = 256
TLA = 512
EG = 40
GLA = 512
ROW = ("x", "c")
COL = ("y", "z")
ALL = ("x", "c", "y", "z")
BATCH = TOK * NX * NC * NY * NZ

EPSILON = 1e-06
DECAY_RATE = 0.8
CLIP_LEVEL = 1.0
FLOOR_VALUE = 1e-30

MESH = pl.DeviceIdType.MESH
F32 = jnp.float32
BF16 = jnp.bfloat16


def mod(value, size):
    return lax.rem(value + 2 * size, size)


class Copies:
    def __init__(self):
        self.sent = []

    def send(self, src, dst, ssem, rsem, device):
        pltpu.make_async_remote_copy(src, dst, ssem, rsem, device_id=device, device_id_type=MESH).start()
        self.sent.append((src, dst, ssem, rsem, device))

    def arrived(self, dst, ssem, rsem, device):
        pltpu.make_async_remote_copy(
            dst, dst, ssem, rsem, device_id=device, device_id_type=MESH
        ).wait_recv()

    def finish(self):
        for src, dst, ssem, rsem, device in self.sent:
            pltpu.make_async_remote_copy(
                src, dst, ssem, rsem, device_id=device, device_id_type=MESH
            ).wait_send()


A0, AP, AM, BP, BM, YP, YM, Y2 = 0, 4, 20, 36, 40, 44, 52, 60
N_MSG = 68
OFFSETS = [0, -1, 1, -2, 2, -3, 3, -4]


class PlaneGather:
    def __init__(self, copies, piece, a, b, la, ssem, rsem, y, z):
        self.copies, self.piece, self.a, self.b, self.la = copies, piece, a, b, la
        self.ssem, self.rsem, self.y, self.z = ssem, rsem, y, z
        self.ys = {o: mod(y + o, NY) for o in range(1 - NY, NY)}
        self.zs = {o: mod(z + o, NZ) for o in range(-(NZ // 2), NZ // 2 + 1)}
        self.sems = [(ssem.at[i], rsem.at[i]) for i in range(N_MSG)]
        self.a_at = {(o, dy): a.at[self.zs[o], self.ys[-dy]] for o in self.zs for dy in range(NY)}
        self.b_at = {(yo, o): b.at[self.ys[yo], self.zs[o]] for o in self.zs for yo in range(-2, 3)}

    def _send(self, src, dst, i, device):
        self.copies.send(src, dst, *self.sems[i], device)

    def _wait(self, dst, i, device):
        sems = self.sems[i] if isinstance(i, int) else (self.ssem.at[i], self.rsem.at[i])
        self.copies.arrived(dst, *sems, device)

    def own(self):
        self.a[self.z, self.y] = self.piece[:, : self.la]
        self.b[self.y, self.z] = self.piece[:, self.la :]

    def _a(self, zo, dy):
        return self.a_at[zo, dy]

    def _b(self, yo, zo):
        return self.b_at[yo, zo]

    def _zdev(self, o):
        return {"z": self.zs[o]}

    def _ydev(self, o):
        return {"y": self.ys[o]}

    @staticmethod
    def _has(sign, s, dy):
        if s < NZ // 2:
            return s >= 1
        return s == NZ // 2 and (dy < NY // 2) == (sign > 0)

    def _ring_a(self, s, dy, sign):
        if not self._has(sign, s, dy):
            return
        src = self._a(-sign * (s - 1), dy)
        dst = src
        if s == 1 and dy == 0:
            src = self.piece.at[:, pl.ds(0, self.la)]
        self._send(src, dst, (AP if sign > 0 else AM) + (s - 1) * 4 + dy, self._zdev(sign))

    def _ring_b(self, s, sign):
        if s > (NZ // 2 if sign > 0 else NZ // 2 - 1):
            return
        dst = self._b(0, -sign * (s - 1))
        src = self.piece.at[:, pl.ds(self.la, self.piece.shape[1] - self.la)] if s == 1 else dst
        self._send(src, dst, (BP if sign > 0 else BM) + s - 1, self._zdev(sign))

    def _spread_b(self, j):
        dst = self._b(0, OFFSETS[j])
        src = self.piece.at[:, pl.ds(self.la, self.piece.shape[1] - self.la)] if j == 0 else dst
        self._send(src, dst, YP + j, self._ydev(1))
        self._send(src, dst, YM + j, self._ydev(-1))

    def _near_b(self, j):
        o = OFFSETS[j]
        self._wait(self._b(-1, o), YP + j, self._ydev(-1))
        if j % 2 == 0:
            self._send(self._b(-1, o), self._b(-1, o), Y2 + j, self._ydev(1))
        self._wait(self._b(1, o), YM + j, self._ydev(1))
        if j % 2 == 1:
            self._send(self._b(1, o), self._b(1, o), Y2 + j, self._ydev(-1))

    def far(self, j):
        o = OFFSETS[j]
        yo = -2 if j % 2 == 0 else 2
        self._wait(self._b(yo, o), Y2 + j, self._ydev(-1 if j % 2 == 0 else 1))

    def far_at(self, j):
        if isinstance(j, int):
            return self.far(j)
        hop = (j + 1) // 2
        zz = mod(self.z + hop * (1 - 2 * lax.rem(j, 2)), NZ)
        self._wait(self.b.at[self.ys[2], zz], Y2 + j, self._ydev(1))

    def start(self):
        for dy in range(1, NY):
            self._send(self.piece.at[:, pl.ds(0, self.la)], self._a(0, 0), A0 + dy - 1, self._ydev(dy))
        for sign in (1, -1):
            self._ring_b(1, sign)
            self._ring_a(1, 0, sign)
        self._spread_b(0)

    def step(self, k):
        for s_sign in (1, -1):
            if k <= (NZ // 2 if s_sign > 0 else NZ // 2 - 1):
                self._wait(self._b(0, -s_sign * k), (BP if s_sign > 0 else BM) + k - 1, self._zdev(-s_sign))
                self._ring_b(k + 1, s_sign)
                self._spread_b(OFFSETS.index(-s_sign * k))
        for dy in range(NY):
            if k == 1:
                if dy == 0:
                    continue
                self._wait(self._a(0, dy), A0 + dy - 1, self._ydev(-dy))
                self._ring_a(1, dy, 1)
                self._ring_a(1, dy, -1)
                continue
            s = k - 1
            for sign in (1, -1):
                if self._has(sign, s, dy):
                    self._wait(
                        self._a(-sign * s, dy), (AP if sign > 0 else AM) + (s - 1) * 4 + dy, self._zdev(-sign)
                    )
                    self._ring_a(s + 1, dy, sign)
        for j, o in enumerate(OFFSETS):
            if abs(o) == k - 1:
                self._near_b(j)


def whole_kernel(
    hidden, weight, text, pooled, row_moment, col_moment, scale_ref, bias_ref,
    update_out, small_out,
    hid, wp, logit_a, logit_b, pg_a, pg_b,
    h_out, mg_out, loss_out,
    wa, wb, wc, ta, tb, tn, part, give, take, share, got, img, unit, length,
    acc, give2, take2, share2, got2,
    grad, far_p, far_m, near_p, near_m, relay_p, relay_m,
    r_far_p, r_far_m, r_near_p, r_near_m, r_relay_p, r_relay_m,
    z_give, z_take, b_give, b_take, yb_give, yb_take,
    row_give, row_take, cy_give, cy_take, cz_give, cz_take,
    s_give, s_take, l_give, l_take, sy_give, sy_take, sz_give, sz_take,
    w_s, w_r, t_s, t_r, h_s, h_r, p_s, p_r, i_s, i_r, u_s, u_r, m_s, m_r,
    g_s, g_r, z_s, z_r, b_s, b_r, yb_s, yb_r, st_s, st_r,
):
    x, c = lax.axis_index("x"), lax.axis_index("c")
    y, z = lax.axis_index("y"), lax.axis_index("z")
    me = c * NX + x
    other = 1 - c

    with jax.named_scope("prep"):
        wp[...] = jnp.zeros_like(wp)
        wp[:ED, :KD] = weight[...].astype(BF16)
        hid[...] = jnp.zeros_like(hid)
        for r in range(NX * NC):
            hid[(r % NC) * NX + r // NC, :, :KD] = hidden[:, KD * r : KD * (r + 1)]
    with jax.named_scope("barrier"):
        barrier = pltpu.get_barrier_semaphore()
        peers = [{"z": mod(z + dz, NZ)} for dz in range(1, NZ)]
        peers += [{"y": mod(y + dy, NY)} for dy in range(1, NY)]
        peers += [
            {"x": mod(x + dx, NX), "c": lax.rem(c + dc, NC)}
            for dx in range(NX) for dc in range(NC) if dx + dc > 0
        ]
        for peer in peers:
            pl.semaphore_signal(barrier, inc=1, device_id=peer, device_id_type=MESH)
        pl.semaphore_wait(barrier, len(peers))

    copies = Copies()
    w = PlaneGather(copies, wp, wa, wb, WLA, w_s, w_r, y, z)
    t = PlaneGather(copies, tn, ta, tb, TLA, t_s, t_r, y, z)

    with jax.named_scope("wstart"):
        w.start()
        row_peers = [(dx, dc) for dx in range(NX) for dc in range(NC) if dx + dc > 0]
        for i, (dx, dc) in enumerate(row_peers):
            xx, cc = mod(x + dx, NX), lax.rem(c + dc, NC)
            copies.send(hid.at[cc * NX + xx], h_out.at[me], h_s.at[i], h_r.at[i], {"x": xx, "c": cc})
        h_out[me] = hid[me]
        w.own()
        tf = text[...].astype(F32)
        tn[...] = (tf / jnp.sqrt(jnp.sum(tf * tf, axis=1, keepdims=True) + EPSILON)).astype(BF16)
    with jax.named_scope("w123"):
        w.step(1)
        w.step(2)
        w.step(3)
    with jax.named_scope("tstart"):
        t.own()
        t.start()
    with jax.named_scope("w45far"):
        w.step(4)
        w.step(5)
        for j in range(8):
            w.far(j)

    with jax.named_scope("compact"):
        r_id = lax.broadcasted_iota(jnp.int32, (4 * ED, 4 * EP), 0)
        c_id = lax.broadcasted_iota(jnp.int32, (4 * ED, 4 * EP), 1)
        pick = jnp.zeros((4 * ED, 4 * EP), F32)
        for g in range(4):
            hit = (r_id >= ED * g) & (r_id < ED * (g + 1)) & (c_id - r_id == (EP - ED) * g)
            pick = jnp.where(hit, 1.0, pick)
        pick = pick.astype(BF16)
        for g in range(8):
            yy, z0 = g // 2, 4 * (g % 2)
            wc[pl.ds(4 * ED * g, 4 * ED), 0:WLA] = jnp.dot(
                pick, wa[z0 : z0 + 4, yy].reshape(4 * EP, WLA), preferred_element_type=F32
            ).astype(BF16)
            wc[pl.ds(4 * ED * g, 4 * ED), WLA:KP] = jnp.dot(
                pick, wb[yy, z0 : z0 + 4].reshape(4 * EP, KP - WLA), preferred_element_type=F32
            ).astype(BF16)

    with jax.named_scope("hwait"):
        for i, (dx, dc) in enumerate(row_peers):
            xx, cc = mod(x - dx, NX), lax.rem(c + dc, NC)
            copies.arrived(h_out.at[cc * NX + xx], h_s.at[i], h_r.at[i], {"x": xx, "c": cc})

    def project(half):
        rows = h_out[pl.ds(half * NX, NX)].reshape(NX * TOK, KP)
        for n in range(3):
            part[pl.ds(half * NX, NX), :, 384 * n : 384 * (n + 1)] = lax.dot_general(
                rows, wc[384 * n : 384 * (n + 1), :], (((1,), (1,)), ((), ())), preferred_element_type=F32
            ).reshape(NX, TOK, 384)

    def reduce_rows(val, gv, tk, sh, gt, ss, rs):
        gv[...] = val[pl.ds(other * NX, NX)].astype(gv.dtype)
        copies.send(gv, tk, ss.at[0], rs.at[0], {"c": other})
        yield
        copies.arrived(tk, ss.at[0], rs.at[0], {"c": other})
        for dx in (2, 1, 3):
            xx = mod(x + dx, NX)
            sh[dx - 1] = (val[c * NX + xx] + tk[xx].astype(F32)).astype(BF16)
        for dx in (2, 1, 3):
            copies.send(sh.at[dx - 1], gt.at[dx - 1], ss.at[dx], rs.at[dx], {"x": mod(x + dx, NX)})
        yield
        total = val[me] + tk[x].astype(F32)
        for dx in (1, 3, 2):
            copies.arrived(gt.at[dx - 1], ss.at[dx], rs.at[dx], {"x": mod(x - dx, NX)})
        for dx in (1, 2, 3):
            total = total + gt[dx - 1].astype(F32)
        yield total

    def share_rows(buf, ss, rs, between=lambda: None):
        copies.send(buf.at[me], buf.at[me], ss.at[4], rs.at[4], {"c": other})
        for dx in (2, 1, 3):
            copies.send(buf.at[me], buf.at[me], ss.at[dx], rs.at[dx], {"x": mod(x + dx, NX)})
        between()
        for dx in (1, 3, 2):
            got_at = buf.at[c * NX + mod(x - dx, NX)]
            copies.arrived(got_at, ss.at[dx], rs.at[dx], {"x": mod(x - dx, NX)})
            copies.send(got_at, got_at, ss.at[4 + dx], rs.at[4 + dx], {"c": other})
        for dx in range(NX):
            copies.arrived(
                buf.at[other * NX + mod(x - dx, NX)], ss.at[4 + dx], rs.at[4 + dx], {"c": other}
            )

    with jax.named_scope("proj1"):
        project(other)
    with jax.named_scope("red1a"):
        red = reduce_rows(part, give, take, share, got, p_s, p_r)
        next(red)
    with jax.named_scope("proj2"):
        project(c)
    with jax.named_scope("t1"):
        t.step(1)
    with jax.named_scope("red1b"):
        next(red)
    with jax.named_scope("t2"):
        t.step(2)
    with jax.named_scope("red1c_norm"):
        mixed = pooled[...].astype(F32) + next(red)
        ln = jnp.sqrt(jnp.sum(mixed * mixed, axis=1, keepdims=True) + EPSILON)
        length[...] = jnp.broadcast_to(ln, length.shape)
        un = mixed / ln
        unit[...] = un
        img[me] = un.astype(BF16)
    with jax.named_scope("imgshare"):
        share_rows(img, i_s, i_r, lambda: t.step(3))
    with jax.named_scope("pairs"):
        scale = scale_ref[0]
        bias = bias_ref[0]
        acc[...] = jnp.zeros_like(acc)
        loss_out[...] = jnp.zeros_like(loss_out)
        tile = NX * TOK
        t_dims = (((1,), (1,)), ((), ()))

        def texts(g):
            return ta[g].reshape(NY * TOK, TLA), tb[:, g].reshape(NY * TOK, D - TLA)

        def logits_of(g, h, out):
            t_a, t_b = texts(g)
            images = img[h * NX : (h + 1) * NX].reshape(tile, D)
            out[...] = lax.dot_general(
                images[:, :TLA], t_a, t_dims, preferred_element_type=F32
            ) + lax.dot_general(images[:, TLA:], t_b, t_dims, preferred_element_type=F32)

        def elementwise(h, src, out, own):
            m = scale * src[...] + bias
            if own:
                col = lax.broadcasted_iota(jnp.int32, (tile, NY * TOK), 1)
                row = lax.broadcasted_iota(jnp.int32, (tile, NY * TOK), 0)
                same = (row - col == TOK * (me - h * NX - y)) & (col >= TOK * y) & (col < TOK * y + TOK)
                m = jnp.where(same, -m, m)
            e = jnp.exp(-jnp.abs(m))
            d = 1.0 + e
            r = 1.0 / d
            soft = jnp.maximum(m, 0.0) + (jnp.log(d) + (e - (d - 1.0)) * r)
            loss_out[...] += jnp.sum(soft.reshape(tile // 8, 8, NY * TOK), axis=0)
            sig = jnp.where(m >= 0.0, r, e * r)
            if own:
                sig = jnp.where(same, -sig, sig)
            out[...] = sig.astype(BF16)

        def to_images(g, h, src):
            t_a, t_b = texts(g)
            pg = src[...]
            rows = slice(h * NX, (h + 1) * NX)
            acc[rows, :, :TLA] += jnp.dot(pg, t_a, preferred_element_type=F32).reshape(NX, TOK, TLA)
            acc[rows, :, TLA:] += jnp.dot(pg, t_b, preferred_element_type=F32).reshape(NX, TOK, D - TLA)

        def group(j):
            hop = (j + 1) // 2
            return mod(z + hop * (1 - 2 * lax.rem(j, 2)), NZ)

        def body(j, carry):
            @pl.when(j == 3)
            def _():
                t.step(4)

            @pl.when(j == 5)
            def _():
                t.step(5)

            t.far_at(j)
            now, last = group(j), group(j - 1)
            logits_of(now, 0, logit_a)
            elementwise(1, logit_b, pg_b, False)
            to_images(last, 0, pg_a)
            logits_of(now, 1, logit_b)
            elementwise(0, logit_a, pg_a, False)
            to_images(last, 1, pg_b)
            return carry

        t.far_at(1)
        first, final = mod(z + OFFSETS[1], NZ), mod(z + OFFSETS[7], NZ)
        logits_of(first, 0, logit_a)
        logits_of(first, 1, logit_b)
        elementwise(0, logit_a, pg_a, False)
        lax.fori_loop(2, NZ, body, 0)
        t.far_at(0)
        logits_of(z, 0, logit_a)
        elementwise(1, logit_b, pg_b, False)
        to_images(final, 0, pg_a)
        logits_of(z, 1, logit_b)
        elementwise(0, logit_a, pg_a, True)
        to_images(final, 1, pg_b)
        elementwise(1, logit_b, pg_b, True)
        to_images(z, 0, pg_a)
        to_images(z, 1, pg_b)

    with jax.named_scope("red2"):
        red = reduce_rows(acc, give2, take2, share2, got2, u_s, u_r)
        next(red)
        next(red)
        ug = (scale * (1.0 / BATCH)) * next(red)
        un = unit[...]
        ln = length[:, 0:1]
        mg_out[me] = ((ug - un * jnp.sum(un * ug, axis=1, keepdims=True)) / ln).astype(BF16)
    with jax.named_scope("mgshare"):
        share_rows(mg_out, m_s, m_r)

    def exchange(give_ref, take_ref, base, value, kind):
        give_ref[...] = value
        sizes = {"row": row_peers, "y": range(1, NY), "z": range(1, NZ)}[kind]
        for i, d in enumerate(sizes):
            if kind == "row":
                device = {"x": mod(x + d[0], NX), "c": lax.rem(c + d[1], NC)}
            else:
                device = {kind: mod((y if kind == "y" else z) + d, NY if kind == "y" else NZ)}
            copies.send(give_ref, take_ref.at[i], st_s.at[base + i], st_r.at[base + i], device)

    def collected(take_ref, base, value, kind):
        sizes = {"row": row_peers, "y": range(1, NY), "z": range(1, NZ)}[kind]
        for i, d in enumerate(sizes):
            if kind == "row":
                device = {"x": mod(x - d[0], NX), "c": lax.rem(c + d[1], NC)}
            else:
                device = {kind: mod((y if kind == "y" else z) - d, NY if kind == "y" else NZ)}
            copies.arrived(take_ref.at[i], st_s.at[base + i], st_r.at[base + i], device)
            value = value + take_ref[i]
        return value

    zi = lax.broadcasted_iota(jnp.int32, (NZ, EG, 384), 0)
    ji = lax.broadcasted_iota(jnp.int32, (NZ, EG, 384), 1)
    li = lax.broadcasted_iota(jnp.int32, (NZ, EG, 384), 2)
    h_all = h_out[...].reshape(NX * NC * TOK, KP)

    def gradient_of(yy):
        choose = jnp.where((ji < ED) & (li == 32 * yy + ED * zi + ji), 1.0, 0.0)
        choose = choose.reshape(NZ * EG, 384).astype(BF16)
        mg = mg_out[:, :, pl.ds(pl.multiple_of(256 * yy, 128), 384)].reshape(NX * NC * TOK, 384)
        mg_t = lax.dot_general(choose, mg, (((1,), (1,)), ((), ())), preferred_element_type=F32).astype(BF16)
        grad[yy] = jnp.dot(mg_t, h_all, preferred_element_type=F32).reshape(NZ, EG, KP)
        b_give[:, yy] = grad[yy, :, :, GLA:].astype(BF16)

    with jax.named_scope("loss1"):
        loss_sum = jnp.sum(jnp.sum(loss_out[...], axis=0, keepdims=True), axis=1, keepdims=True)
        loss_sum = jnp.broadcast_to(loss_sum, (1, 128))
        exchange(l_give, l_take, 34, loss_sum, "row")
    with jax.named_scope("g_far"):
        half = NZ // 2
        y_far, y_up, y_down = mod(y + 2, NY), mod(y + 1, NY), mod(y - 1, NY)
        up, down = {"y": y_up}, {"y": y_down}
        gradient_of(y_far)
        far_p[...] = grad[y_far, :half, :, :GLA].astype(BF16)
        far_m[...] = grad[y_far, half:, :, :GLA].astype(BF16)
        copies.send(far_p, r_far_p, g_s.at[0], g_r.at[0], up)
        copies.send(far_m, r_far_m, g_s.at[1], g_r.at[1], down)
    with jax.named_scope("g_rest"):
        gradient_of(y_up)
        near_p[...] = grad[y_up, half:, :, :GLA].astype(BF16)
        copies.send(near_p, r_near_p, g_s.at[2], g_r.at[2], up)
        gradient_of(y_down)
        near_m[...] = grad[y_down, :half, :, :GLA].astype(BF16)
        copies.send(near_m, r_near_m, g_s.at[3], g_r.at[3], down)
        gradient_of(y)
    with jax.named_scope("g_relay"):
        copies.arrived(r_far_p, g_s.at[0], g_r.at[0], down)
        relay_p[...] = (grad[y_up, :half, :, :GLA] + r_far_p[...].astype(F32)).astype(BF16)
        copies.send(relay_p, r_relay_p, g_s.at[4], g_r.at[4], up)
        copies.arrived(r_far_m, g_s.at[1], g_r.at[1], up)
        relay_m[...] = (grad[y_down, half:, :, :GLA] + r_far_m[...].astype(F32)).astype(BF16)
        copies.send(relay_m, r_relay_m, g_s.at[5], g_r.at[5], down)
        z_order = (4, 3, 5, 2, 6, 1, 7)
        z_near = (1, 7, 2, 6, 3, 5, 4)
        for dz in z_order:
            zz = mod(z + dz, NZ)
            copies.send(b_give.at[zz], b_take.at[dz - 1], b_s.at[dz - 1], b_r.at[dz - 1], {"z": zz})
    with jax.named_scope("loss2"):
        loss_sum = collected(l_take, 34, loss_sum, "row")
        exchange(sy_give, sy_take, 24, loss_sum, "y")
    with jax.named_scope("g_ysum"):
        copies.arrived(r_near_p, g_s.at[2], g_r.at[2], down)
        copies.arrived(r_near_m, g_s.at[3], g_r.at[3], up)
        copies.arrived(r_relay_p, g_s.at[4], g_r.at[4], down)
        copies.arrived(r_relay_m, g_s.at[5], g_r.at[5], up)
        grad[y, :half, :, :GLA] += r_relay_p[...].astype(F32) + r_near_m[...].astype(F32)
        grad[y, half:, :, :GLA] += r_near_p[...].astype(F32) + r_relay_m[...].astype(F32)
        z_give[...] = grad[y, :, :, :GLA].astype(z_give.dtype)
        for dz in z_order:
            zz = mod(z + dz, NZ)
            copies.send(z_give.at[zz], z_take.at[dz - 1], z_s.at[dz - 1], z_r.at[dz - 1], {"z": zz})
    with jax.named_scope("g_bz"):
        part_b = grad[:, pl.ds(z, 1), :, GLA:].reshape(NY, EG, KP - GLA)
        for dz in z_near:
            copies.arrived(b_take.at[dz - 1], b_s.at[dz - 1], b_r.at[dz - 1], {"z": mod(z - dz, NZ)})
            part_b = part_b + b_take[dz - 1].astype(F32)
        yb_give[...] = part_b
        for dy in (2, 1, 3):
            yy = mod(y + dy, NY)
            copies.send(yb_give.at[yy], yb_take.at[dy - 1], yb_s.at[dy - 1], yb_r.at[dy - 1], {"y": yy})
    with jax.named_scope("g_by"):
        right = yb_give[y]
        for dy in (1, 3, 2):
            copies.arrived(yb_take.at[dy - 1], yb_s.at[dy - 1], yb_r.at[dy - 1], {"y": mod(y - dy, NY)})
            right = right + yb_take[dy - 1]
    with jax.named_scope("loss3"):
        loss_sum = collected(sy_take, 24, loss_sum, "y")
        exchange(sz_give, sz_take, 27, loss_sum, "z")
    with jax.named_scope("g_z"):
        left = grad[y, pl.ds(z, 1), :, :GLA].reshape(EG, GLA)
        for dz in z_near:
            copies.arrived(z_take.at[dz - 1], z_s.at[dz - 1], z_r.at[dz - 1], {"z": mod(z - dz, NZ)})
            left = left + z_take[dz - 1].astype(F32)
        grad[y, pl.ds(z, 1), :, :GLA] = left.reshape(1, EG, GLA)
        grad[y, pl.ds(z, 1), :, GLA:] = right.reshape(1, EG, KP - GLA)

    g = grad[y, pl.ds(z, 1)].reshape(EG, KP)
    e_id = lax.broadcasted_iota(jnp.int32, (EG, KP), 0)
    k_id = lax.broadcasted_iota(jnp.int32, (EG, KP), 1)
    squared = jnp.where((e_id < ED) & (k_id < KD), g * g + FLOOR_VALUE, 0.0)

    with jax.named_scope("st_row"):
        e_col = e_id[:, 0:128]
        l_col = k_id[:, 0:128]
        rows = jnp.broadcast_to(jnp.sum(squared, axis=1, keepdims=True), (EG, 128))
        exchange(row_give, row_take, 0, rows, "row")
        cols = jnp.sum(squared, axis=0, keepdims=True)
        rows = collected(row_take, 0, rows, "row")
        row_line = jnp.sum(jnp.where(e_col == l_col, rows, 0.0), axis=0, keepdims=True)[:, :ED]
        row_line = DECAY_RATE * row_moment[...].reshape(1, ED) + (1.0 - DECAY_RATE) * row_line / FF
        new_row = jnp.sum(
            jnp.where(
                e_id[:, :ED] == k_id[:, :ED], jnp.broadcast_to(row_line, (EG, ED)), 0.0
            ), axis=1, keepdims=True
        )
        new_row = jnp.where(e_col[:, 0:1] < ED, new_row, 1.0)
        ratio = jnp.sum(g * g / new_row, axis=0, keepdims=True)
    with jax.named_scope("st_col"):
        cols2 = jnp.concatenate([cols, ratio], axis=1)
        exchange(cy_give, cy_take, 7, cols2, "y")
        cols2 = collected(cy_take, 7, cols2, "y")
        exchange(cz_give, cz_take, 10, cols2, "z")
        cols2 = collected(cz_take, 10, cols2, "z")
    with jax.named_scope("st_tot"):
        cols, ratio = cols2[:, :KP], cols2[:, KP:]
        col_line = DECAY_RATE * col_moment[...].reshape(1, KD) + (1.0 - DECAY_RATE) * cols[:, :KD] / D
        raw_sum = jnp.sum(ratio[:, :KD] / col_line, axis=1, keepdims=True)
        exchange(s_give, s_take, 17, jnp.broadcast_to(raw_sum, (1, 128)), "row")
        raw = g[:ED, :KD] / jnp.sqrt(new_row[:ED] * col_line)
        loss_sum = collected(sz_take, 27, loss_sum, "z")
        small_out[...] = jnp.zeros_like(small_out)
        small_out[0:1, :KD] = col_line
        small_out[1:2, :ED] = row_line
        small_out[2:3, 0:128] = loss_sum * (1.0 / BATCH)
        both = collected(s_take, 17, jnp.broadcast_to(raw_sum, (1, 128)), "row")
    with jax.named_scope("upd"):
        rms = jnp.sqrt(both[:, 0:1] / (D * FF))
        update_out[...] = raw / jnp.maximum(1.0, rms / CLIP_LEVEL)
    with jax.named_scope("finish"):
        copies.finish()


def step_kernel(hidden, weight, text, pooled, row_moment, col_moment, scale, bias):
    vmem = pl.BlockSpec(memory_space=pltpu.VMEM)
    smem = pl.BlockSpec(memory_space=pltpu.SMEM)
    n_row = NX * NC
    dma = pltpu.SemaphoreType.DMA
    return pl.pallas_call(
        whole_kernel,
        out_shape=(
            jax.ShapeDtypeStruct((ED, KD), F32),
            jax.ShapeDtypeStruct((8, KP), F32),
        ),
        in_specs=[vmem] * 6 + [smem] * 2,
        out_specs=(vmem,) * 2,
        scratch_shapes=[
            pltpu.VMEM((n_row, TOK, KP), BF16),
            pltpu.VMEM((EP, KP), BF16),
            pltpu.VMEM((NX * TOK, NY * TOK), F32),
            pltpu.VMEM((NX * TOK, NY * TOK), F32),
            pltpu.VMEM((NX * TOK, NY * TOK), BF16),
            pltpu.VMEM((NX * TOK, NY * TOK), BF16),
            pltpu.VMEM((n_row, TOK, KP), BF16),
            pltpu.VMEM((n_row, TOK, D), BF16),
            pltpu.VMEM((8, NY * TOK), F32),
            pltpu.VMEM((NZ, NY, EP, WLA), BF16),
            pltpu.VMEM((NY, NZ, EP, KP - WLA), BF16),
            pltpu.VMEM((D, KP), BF16),
            pltpu.VMEM((NZ, NY, TOK, TLA), BF16),
            pltpu.VMEM((NY, NZ, TOK, D - TLA), BF16),
            pltpu.VMEM((TOK, D), BF16),
            pltpu.VMEM((n_row, TOK, D), F32),
            pltpu.VMEM((NX, TOK, D), F32),
            pltpu.VMEM((NX, TOK, D), F32),
            pltpu.VMEM((NX - 1, TOK, D), BF16),
            pltpu.VMEM((NX - 1, TOK, D), BF16),
            pltpu.VMEM((n_row, TOK, D), BF16),
            pltpu.VMEM((TOK, D), F32),
            pltpu.VMEM((TOK, 128), F32),
            pltpu.VMEM((n_row, TOK, D), F32),
            pltpu.VMEM((NX, TOK, D), BF16),
            pltpu.VMEM((NX, TOK, D), BF16),
            pltpu.VMEM((NX - 1, TOK, D), BF16),
            pltpu.VMEM((NX - 1, TOK, D), BF16),
            pltpu.VMEM((NY, NZ, EG, KP), F32),
            *[pltpu.VMEM((NZ // 2, EG, GLA), BF16)] * 12,
            pltpu.VMEM((NZ, EG, GLA), BF16),
            pltpu.VMEM((NZ - 1, EG, GLA), BF16),
            pltpu.VMEM((NZ, NY, EG, KP - GLA), BF16),
            pltpu.VMEM((NZ - 1, NY, EG, KP - GLA), BF16),
            pltpu.VMEM((NY, EG, KP - GLA), F32),
            pltpu.VMEM((NY - 1, EG, KP - GLA), F32),
            pltpu.VMEM((EG, 128), F32),
            pltpu.VMEM((n_row - 1, EG, 128), F32),
            pltpu.VMEM((1, 2 * KP), F32),
            pltpu.VMEM((NY - 1, 1, 2 * KP), F32),
            pltpu.VMEM((1, 2 * KP), F32),
            pltpu.VMEM((NZ - 1, 1, 2 * KP), F32),
            pltpu.VMEM((1, 128), F32),
            pltpu.VMEM((n_row - 1, 1, 128), F32),
            pltpu.VMEM((1, 128), F32),
            pltpu.VMEM((n_row - 1, 1, 128), F32),
            pltpu.VMEM((1, 128), F32),
            pltpu.VMEM((NY - 1, 1, 128), F32),
            pltpu.VMEM((1, 128), F32),
            pltpu.VMEM((NZ - 1, 1, 128), F32),
            dma((N_MSG,)), dma((N_MSG,)), dma((N_MSG,)), dma((N_MSG,)),
            dma((8,)), dma((8,)), dma((4,)), dma((4,)), dma((8,)), dma((8,)),
            dma((4,)), dma((4,)), dma((8,)), dma((8,)),
            dma((6,)), dma((6,)), dma((7,)), dma((7,)), dma((7,)), dma((7,)),
            dma((3,)), dma((3,)), dma((41,)), dma((41,)),
        ],
        compiler_params=pltpu.CompilerParams(
            collective_id=0, has_side_effects=True, vmem_limit_bytes=60 * 1024 * 1024
        ),
        name="step",
    )(hidden, weight, text, pooled, row_moment, col_moment, scale, bias)


def per_device(pooled, hidden, text, weight, row_moment, col_moment, log_scale, bias):
    update, small = step_kernel(
        hidden, weight, text, pooled, row_moment, col_moment, jnp.exp(log_scale).reshape(1), bias.reshape(1)
    )
    return (update, small[1, :ED], small[0, :KD], small[2, 0])


def solution(mesh):
    finer = Mesh(mesh.devices.reshape(NX, NC, NY, NZ), ALL)
    return jax.shard_map(
        per_device,
        mesh=finer,
        in_specs=(
            P(ALL, None), P(ALL, None), P(ALL, None), P(COL, ROW), P(COL), P(ROW), P(), P(),
        ),
        out_specs=(P(COL, ROW), P(COL), P(ROW), P()),
        check_vma=False,
    )
```

```python
import functools

import jax
import jax.numpy as jnp
from jax import lax
from jax.experimental import pallas as pl
from jax.experimental.pallas import tpu as pltpu
from jax.sharding import Mesh
from jax.sharding import PartitionSpec as P

D = 1152
FF = 4304
NX, NC, NY, NZ = 4, 2, 4, 8
TOK = 64
KD = FF // (NX * NC)
KP = 640
ED = D // (NY * NZ)
EP = 48
WLA = 256
TLA = 512
EG = 40
GLA = 384
GLB = 512
ROW = ("x", "c")
COL = ("y", "z")
ALL = ("x", "c", "y", "z")
BATCH = TOK * NX * NC * NY * NZ

EPSILON = 1e-06
DECAY_RATE = 0.8
CLIP_LEVEL = 1.0
FLOOR_VALUE = 1e-30

MESH = pl.DeviceIdType.MESH
F32 = jnp.float32
BF16 = jnp.bfloat16


def mod(value, size):
    return lax.rem(value + 2 * size, size)


def send(src, dst, ssem, rsem, device):
    pltpu.make_async_remote_copy(src, dst, ssem, rsem, device_id=device, device_id_type=MESH).start()


def arrived(dst, ssem, rsem, device):
    pltpu.make_async_remote_copy(dst, dst, ssem, rsem, device_id=device, device_id_type=MESH).wait_recv()


def all_sent(ref, ssem, rsem, device):
    pltpu.make_async_remote_copy(ref, ref, ssem, rsem, device_id=device, device_id_type=MESH).wait_send()


A0, AP, AM, BP, BM, YP, YM, Y2 = 0, 4, 20, 36, 40, 44, 52, 60
N_MSG = 68
EXCHANGES = (0, 7, 10, 17, 24, 27, 34)
A_MSG = range(A0, BP)
OFFSETS = [0, -1, 1, -2, 2, -3, 3, -4]


class PlaneGather:
    def __init__(self, piece, a, b, la, rows, ssem, rsem, y, z):
        self.piece, self.a, self.b, self.la, self.rows = piece, a, b, la, pl.ds(0, rows)
        self.piece_a = piece.at[self.rows, pl.ds(0, la)]
        self.piece_b = piece.at[self.rows, pl.ds(la, piece.shape[1] - la)]
        self.ssem, self.rsem, self.y, self.z = ssem, rsem, y, z
        self.ys = {o: mod(y + o, NY) for o in range(1 - NY, NY)}
        self.zs = {o: mod(z + o, NZ) for o in range(-(NZ // 2), NZ // 2 + 1)}
        self.sems = [(ssem.at[0 if i in A_MSG else 1], rsem.at[i]) for i in range(N_MSG)]
        self.a_at = {(o, dy): a.at[self.zs[o] * NY + self.ys[-dy], self.rows] for o in self.zs for dy in range(NY)}
        self.b_at = {(yo, o): b.at[self.ys[yo] * NZ + self.zs[o], self.rows] for o in self.zs for yo in range(-2, 3)}

    def _send(self, src, dst, i, device):
        send(src, dst, *self.sems[i], device)

    def _wait(self, dst, i, device):
        sems = self.sems[i] if isinstance(i, int) else (self.ssem.at[1], self.rsem.at[i])
        arrived(dst, *sems, device)

    def own(self):
        self.a[self.z * NY + self.y] = self.piece[:, : self.la]
        self.b[self.y * NZ + self.z] = self.piece[:, self.la :]

    def finish(self):
        n = pl.ds(0, NY * NZ - 1)
        all_sent(self.a.at[n, self.rows], *self.sems[A0], self._zdev(1))
        all_sent(self.b.at[n, self.rows], *self.sems[BP], self._zdev(1))

    def _a(self, zo, dy):
        return self.a_at[zo, dy]

    def _b(self, yo, zo):
        return self.b_at[yo, zo]

    def _zdev(self, o):
        return {"z": self.zs[o]}

    def _ydev(self, o):
        return {"y": self.ys[o]}

    @staticmethod
    def _has(sign, s, dy):
        if s < NZ // 2:
            return s >= 1
        return s == NZ // 2 and (dy < NY // 2) == (sign > 0)

    def _ring_a(self, s, dy, sign):
        if not self._has(sign, s, dy):
            return
        src = self._a(-sign * (s - 1), dy)
        dst = src
        if s == 1 and dy == 0:
            src = self.piece_a
        self._send(src, dst, (AP if sign > 0 else AM) + (s - 1) * 4 + dy, self._zdev(sign))

    def _ring_b(self, s, sign):
        if s > (NZ // 2 if sign > 0 else NZ // 2 - 1):
            return
        dst = self._b(0, -sign * (s - 1))
        src = self.piece_b if s == 1 else dst
        self._send(src, dst, (BP if sign > 0 else BM) + s - 1, self._zdev(sign))

    def _spread_b(self, j):
        dst = self._b(0, OFFSETS[j])
        src = self.piece_b if j == 0 else dst
        self._send(src, dst, YP + j, self._ydev(1))
        self._send(src, dst, YM + j, self._ydev(-1))

    def _near_b(self, j):
        o = OFFSETS[j]
        self._wait(self._b(-1, o), YP + j, self._ydev(-1))
        if j % 2 == 0:
            self._send(self._b(-1, o), self._b(-1, o), Y2 + j, self._ydev(1))
        self._wait(self._b(1, o), YM + j, self._ydev(1))
        if j % 2 == 1:
            self._send(self._b(1, o), self._b(1, o), Y2 + j, self._ydev(-1))

    def far(self, j):
        o = OFFSETS[j]
        yo = -2 if j % 2 == 0 else 2
        self._wait(self._b(yo, o), Y2 + j, self._ydev(-1 if j % 2 == 0 else 1))

    def far_at(self, j):
        if isinstance(j, int):
            return self.far(j)
        hop = (j + 1) // 2
        zz = mod(self.z + hop * (1 - 2 * lax.rem(j, 2)), NZ)
        self._wait(self.b.at[self.ys[2] * NZ + zz, self.rows], Y2 + j, self._ydev(1))

    def start(self):
        for dy in range(1, NY):
            self._send(self.piece_a, self._a(0, 0), A0 + dy - 1, self._ydev(dy))
        for sign in (1, -1):
            self._ring_b(1, sign)
            self._ring_a(1, 0, sign)
        self._spread_b(0)

    def step(self, k):
        for s_sign in (1, -1):
            if k <= (NZ // 2 if s_sign > 0 else NZ // 2 - 1):
                self._wait(self._b(0, -s_sign * k), (BP if s_sign > 0 else BM) + k - 1, self._zdev(-s_sign))
                self._ring_b(k + 1, s_sign)
                self._spread_b(OFFSETS.index(-s_sign * k))
        for dy in range(NY):
            if k == 1:
                if dy == 0:
                    continue
                self._wait(self._a(0, dy), A0 + dy - 1, self._ydev(-dy))
                self._ring_a(1, dy, 1)
                self._ring_a(1, dy, -1)
                continue
            s = k - 1
            for sign in (1, -1):
                if self._has(sign, s, dy):
                    self._wait(
                        self._a(-sign * s, dy), (AP if sign > 0 else AM) + (s - 1) * 4 + dy, self._zdev(-sign)
                    )
                    self._ring_a(s + 1, dy, sign)
        for j, o in enumerate(OFFSETS):
            if abs(o) == k - 1:
                self._near_b(j)


def whole_kernel(
    hidden, weight, text, pooled, row_moment, col_moment, scale_ref, bias_ref,
    update_out, small_out,
    hid, wp, logit_a, logit_b, pg_a, pg_b,
    h_out, mg_out, loss_out,
    wa, wb, wc, ta, tb, tn, part, give, take, share, got, img, unit, length,
    acc, give2, take2, share2, got2,
    grad, far_p, far_m, near_p, near_m, relay_p, relay_m,
    r_far_p, r_far_m, r_near_p, r_near_m, r_relay_p, r_relay_m,
    z_give, z_take, tail, b_give, b_take, yb_give, yb_take,
    row_give, row_take, cy_give, cy_take, cz_give, cz_take,
    s_give, s_take, l_give, l_take, sy_give, sy_take, sz_give, sz_take,
    w_s, w_r, t_s, t_r, h_s, h_r, p_s, p_r, i_s, i_r, u_s, u_r, m_s, m_r,
    g_s, g_r, z_s, z_r, b_s, b_r, yb_s, yb_r, st_s, st_r,
):
    x, c = lax.axis_index("x"), lax.axis_index("c")
    y, z = lax.axis_index("y"), lax.axis_index("z")
    me = c * NX + x
    other = 1 - c

    with jax.named_scope("prep"):
        wp[...] = jnp.zeros_like(wp)
        wp[:ED, :KD] = weight[...].astype(BF16)
        hid[...] = jnp.zeros_like(hid)
        wa[...] = jnp.zeros_like(wa)
        wb[...] = jnp.zeros_like(wb)
        for r in range(NX * NC):
            hid[(r % NC) * NX + r // NC, :, :KD] = hidden[:, KD * r : KD * (r + 1)]
    with jax.named_scope("barrier"):
        barrier = pltpu.get_barrier_semaphore()
        peers = [{"z": mod(z + dz, NZ)} for dz in range(1, NZ)]
        peers += [{"y": mod(y + dy, NY)} for dy in range(1, NY)]
        peers += [
            {"x": mod(x + dx, NX), "c": lax.rem(c + dc, NC)}
            for dx in range(NX) for dc in range(NC) if dx + dc > 0
        ]
        for peer in peers:
            pl.semaphore_signal(barrier, inc=1, device_id=peer, device_id_type=MESH)
        pl.semaphore_wait(barrier, len(peers))

    w = PlaneGather(wp, wa, wb, WLA, EG, w_s, w_r, y, z)
    t = PlaneGather(tn, ta, tb, TLA, TOK, t_s, t_r, y, z)

    with jax.named_scope("wstart"):
        w.start()
        row_peers = [(dx, dc) for dx in range(NX) for dc in range(NC) if dx + dc > 0]
        for i, (dx, dc) in enumerate(row_peers):
            xx, cc = mod(x + dx, NX), lax.rem(c + dc, NC)
            send(hid.at[cc * NX + xx], h_out.at[me], h_s.at[0], h_r.at[i], {"x": xx, "c": cc})
        h_out[me] = hid[me]
        w.own()
        tf = text[...].astype(F32)
        tn[...] = (tf / jnp.sqrt(jnp.sum(tf * tf, axis=1, keepdims=True) + EPSILON)).astype(BF16)
    with jax.named_scope("w123"):
        w.step(1)
        w.step(2)
        w.step(3)
    with jax.named_scope("tstart"):
        t.own()
        t.start()
    with jax.named_scope("w45far"):
        w.step(4)
        w.step(5)
        for j in range(8):
            w.far(j)

    with jax.named_scope("compact"):
        r_id = lax.broadcasted_iota(jnp.int32, (4 * ED, 4 * EP), 0)
        c_id = lax.broadcasted_iota(jnp.int32, (4 * ED, 4 * EP), 1)
        pick = jnp.zeros((4 * ED, 4 * EP), F32)
        for g in range(4):
            hit = (r_id >= ED * g) & (r_id < ED * (g + 1)) & (c_id - r_id == (EP - ED) * g)
            pick = jnp.where(hit, 1.0, pick)
        pick = pick.astype(BF16)
        for g in range(8):
            yy, z0 = g // 2, 4 * (g % 2)
            wc[pl.ds(4 * ED * g, 4 * ED), 0:WLA] = jnp.dot(
                pick, jnp.concatenate([wa[(z0 + k) * NY + yy] for k in range(4)], axis=0), preferred_element_type=F32
            ).astype(BF16)
            wc[pl.ds(4 * ED * g, 4 * ED), WLA:KP] = jnp.dot(
                pick, wb[yy * NZ + z0 : yy * NZ + z0 + 4].reshape(4 * EP, KP - WLA), preferred_element_type=F32
            ).astype(BF16)

    with jax.named_scope("hwait"):
        for i, (dx, dc) in enumerate(row_peers):
            xx, cc = mod(x - dx, NX), lax.rem(c + dc, NC)
            arrived(h_out.at[cc * NX + xx], h_s.at[0], h_r.at[i], {"x": xx, "c": cc})

    def project(half):
        rows = h_out[pl.ds(half * NX, NX)].reshape(NX * TOK, KP)
        for n in range(3):
            part[pl.ds(half * NX, NX), :, 384 * n : 384 * (n + 1)] = lax.dot_general(
                rows, wc[384 * n : 384 * (n + 1), :], (((1,), (1,)), ((), ())), preferred_element_type=F32
            ).reshape(NX, TOK, 384)

    def reduce_rows(val, gv, tk, sh, gt, ss, rs):
        for dx in (2, 1, 3, 0):
            xx = mod(x + dx, NX)
            gv[xx] = val[other * NX + xx].astype(gv.dtype)
            send(gv.at[xx], tk.at[xx], ss.at[0], rs.at[dx], {"c": other})
        yield
        for dx in (2, 1, 3):
            xx = mod(x + dx, NX)
            arrived(tk.at[xx], ss.at[0], rs.at[dx], {"c": other})
            sh[dx - 1] = (val[c * NX + xx] + tk[xx].astype(F32)).astype(BF16)
            send(sh.at[dx - 1], gt.at[dx - 1], ss.at[1], rs.at[NX - 1 + dx], {"x": xx})
        yield
        arrived(tk.at[x], ss.at[0], rs.at[0], {"c": other})
        total = val[me] + tk[x].astype(F32)
        for dx in (1, 3, 2):
            arrived(gt.at[dx - 1], ss.at[1], rs.at[NX - 1 + dx], {"x": mod(x - dx, NX)})
        for dx in (1, 2, 3):
            total = total + gt[dx - 1].astype(F32)
        all_sent(gv, ss.at[0], rs.at[0], {"c": other})
        all_sent(sh, ss.at[1], rs.at[NX], {"x": mod(x + 1, NX)})
        yield total

    def share_rows(buf, ss, rs, between=lambda: None):
        for dx in (2, 1, 3):
            send(buf.at[me], buf.at[me], ss.at[0], rs.at[dx], {"x": mod(x + dx, NX)})
        send(buf.at[me], buf.at[me], ss.at[0], rs.at[4], {"c": other})
        between()
        for dx in (1, 3, 2):
            got_at = buf.at[c * NX + mod(x - dx, NX)]
            arrived(got_at, ss.at[0], rs.at[dx], {"x": mod(x - dx, NX)})
            send(got_at, got_at, ss.at[0], rs.at[4 + dx], {"c": other})
        for dx in (0, 1, 3, 2):
            arrived(buf.at[other * NX + mod(x - dx, NX)], ss.at[0], rs.at[4 + dx], {"c": other})
        all_sent(buf.at[pl.ds(0, 7)], ss.at[0], rs.at[1], {"c": other})

    with jax.named_scope("proj1"):
        project(other)
    with jax.named_scope("red1a"):
        red = reduce_rows(part, give, take, share, got, p_s, p_r)
        next(red)
    with jax.named_scope("proj2"):
        project(c)
    with jax.named_scope("t1"):
        t.step(1)
    with jax.named_scope("red1b"):
        next(red)
    with jax.named_scope("t2"):
        t.step(2)
    with jax.named_scope("red1c_norm"):
        mixed = pooled[...].astype(F32) + next(red)
        ln = jnp.sqrt(jnp.sum(mixed * mixed, axis=1, keepdims=True) + EPSILON)
        length[...] = jnp.broadcast_to(ln, length.shape)
        un = mixed / ln
        unit[...] = un
        img[me] = un.astype(BF16)
    with jax.named_scope("imgshare"):
        share_rows(img, i_s, i_r, lambda: t.step(3))
    with jax.named_scope("pairs"):
        scale = scale_ref[0]
        bias = bias_ref[0]
        acc[...] = jnp.zeros_like(acc)
        loss_out[...] = jnp.zeros_like(loss_out)
        tile = NX * TOK
        t_dims = (((1,), (1,)), ((), ()))

        halves = (other, c)

        def texts(g):
            t_b = jnp.concatenate([tb[yy * NZ + g] for yy in range(NY)], axis=0)
            return ta[pl.ds(g * NY, NY)].reshape(NY * TOK, TLA), t_b

        def logits_of(g, h, out):
            t_a, t_b = texts(g)
            images = img[pl.ds(halves[h] * NX, NX)].reshape(tile, D)
            out[...] = lax.dot_general(
                images[:, :TLA], t_a, t_dims, preferred_element_type=F32
            ) + lax.dot_general(images[:, TLA:], t_b, t_dims, preferred_element_type=F32)

        def elementwise(src, out, own):
            m = scale * src[...] + bias
            if own:
                col = lax.broadcasted_iota(jnp.int32, (tile, NY * TOK), 1)
                row = lax.broadcasted_iota(jnp.int32, (tile, NY * TOK), 0)
                same = (row - col == TOK * (x - y)) & (col >= TOK * y) & (col < TOK * y + TOK)
                m = jnp.where(same, -m, m)
            e = jnp.exp(-jnp.abs(m))
            d = 1.0 + e
            r = 1.0 / d
            soft = jnp.maximum(m, 0.0) + (jnp.log(d) + (e - (d - 1.0)) * r)
            loss_out[...] += jnp.sum(soft.reshape(tile // 8, 8, NY * TOK), axis=0)
            sig = jnp.where(m >= 0.0, r, e * r)
            if own:
                sig = jnp.where(same, -sig, sig)
            out[...] = sig.astype(BF16)

        def to_images(g, h, src):
            t_a, t_b = texts(g)
            pg = src[...]
            rows = pl.ds(halves[h] * NX, NX)
            acc[rows, :, :TLA] += jnp.dot(pg, t_a, preferred_element_type=F32).reshape(NX, TOK, TLA)
            acc[rows, :, TLA:] += jnp.dot(pg, t_b, preferred_element_type=F32).reshape(NX, TOK, D - TLA)

        def group(j):
            hop = (j + 1) // 2
            return mod(z + hop * (1 - 2 * lax.rem(j, 2)), NZ)

        def body(j, carry):
            @pl.when(j == 3)
            def _():
                t.step(4)

            @pl.when(j == 5)
            def _():
                t.step(5)

            t.far_at(j)
            now, last = group(j), group(j - 1)
            logits_of(now, 0, logit_a)
            elementwise(logit_b, pg_b, False)
            to_images(last, 0, pg_a)
            logits_of(now, 1, logit_b)
            elementwise(logit_a, pg_a, False)
            to_images(last, 1, pg_b)
            return carry

        t.far_at(1)
        first, final = mod(z + OFFSETS[1], NZ), mod(z + OFFSETS[7], NZ)
        logits_of(first, 0, logit_a)
        logits_of(first, 1, logit_b)
        elementwise(logit_a, pg_a, False)
        lax.fori_loop(2, NZ, body, 0)
        t.far_at(0)
        logits_of(z, 0, logit_a)
        elementwise(logit_b, pg_b, False)
        to_images(final, 0, pg_a)
        logits_of(z, 1, logit_b)
        elementwise(logit_a, pg_a, False)
        to_images(final, 1, pg_b)
        to_images(z, 0, pg_a)
    with jax.named_scope("red2"):
        red = reduce_rows(acc, give2, take2, share2, got2, u_s, u_r)
        next(red)
        elementwise(logit_b, pg_b, True)
        to_images(z, 1, pg_b)
        next(red)
        ug = (scale * (1.0 / BATCH)) * next(red)
        un = unit[...]
        ln = length[:, 0:1]
        mg_out[me] = ((ug - un * jnp.sum(un * ug, axis=1, keepdims=True)) / ln).astype(BF16)
    with jax.named_scope("mgshare"):
        share_rows(mg_out, m_s, m_r)

    def exchange(give_ref, take_ref, base, value, kind):
        give_ref[...] = value
        slot = EXCHANGES.index(base)
        sizes = {"row": row_peers, "y": range(1, NY), "z": range(1, NZ)}[kind]
        for i, d in enumerate(sizes):
            if kind == "row":
                device = {"x": mod(x + d[0], NX), "c": lax.rem(c + d[1], NC)}
            else:
                device = {kind: mod((y if kind == "y" else z) + d, NY if kind == "y" else NZ)}
            send(give_ref, take_ref.at[i], st_s.at[slot], st_r.at[base + i], device)

    def collected(take_ref, base, value, kind):
        slot = EXCHANGES.index(base)
        sizes = {"row": row_peers, "y": range(1, NY), "z": range(1, NZ)}[kind]
        for i, d in enumerate(sizes):
            if kind == "row":
                device = {"x": mod(x - d[0], NX), "c": lax.rem(c + d[1], NC)}
            else:
                device = {kind: mod((y if kind == "y" else z) - d, NY if kind == "y" else NZ)}
            arrived(take_ref.at[i], st_s.at[slot], st_r.at[base + i], device)
            value = value + take_ref[i]
        all_sent(take_ref, st_s.at[slot], st_r.at[base], device)
        return value

    zi = lax.broadcasted_iota(jnp.int32, (NZ, EG, 384), 0)
    ji = lax.broadcasted_iota(jnp.int32, (NZ, EG, 384), 1)
    li = lax.broadcasted_iota(jnp.int32, (NZ, EG, 384), 2)
    h_all = h_out[...].reshape(NX * NC * TOK, KP)

    def gradient_of(dy):
        yy = mod(y + dy, NY)
        choose = jnp.where((ji < ED) & (li == 32 * yy + ED * zi + ji), 1.0, 0.0)
        choose = choose.reshape(NZ * EG, 384).astype(BF16)
        mg = mg_out[:, :, pl.ds(pl.multiple_of(256 * yy, 128), 384)].reshape(NX * NC * TOK, 384)
        mg_t = lax.dot_general(choose, mg, (((1,), (1,)), ((), ())), preferred_element_type=F32).astype(BF16)
        grad[yy] = jnp.dot(mg_t, h_all, preferred_element_type=F32).reshape(NZ, EG, KP)
        b_give[:, dy] = grad[yy, :, :, GLA:GLB].astype(BF16)
        tail[:, :, 32 * dy : 32 * dy + 32] = grad[yy, :, :, GLB : GLB + 32]

    with jax.named_scope("loss1"):
        loss_sum = jnp.sum(jnp.sum(loss_out[...], axis=0, keepdims=True), axis=1, keepdims=True)
        loss_sum = jnp.broadcast_to(loss_sum, (1, 128))
        exchange(l_give, l_take, 34, loss_sum, "row")
    with jax.named_scope("g_far"):
        half = NZ // 2
        y_far, y_up, y_down = mod(y + 2, NY), mod(y + 1, NY), mod(y - 1, NY)
        up, down = {"y": y_up}, {"y": y_down}
        gradient_of(2)
        far_p[...] = grad[y_far, :half, :, :GLA].astype(BF16)
        far_m[...] = grad[y_far, half:, :, :GLA].astype(BF16)
        send(far_p, r_far_p, g_s.at[0], g_r.at[0], up)
        send(far_m, r_far_m, g_s.at[1], g_r.at[1], down)
    with jax.named_scope("g_rest"):
        gradient_of(1)
        near_p[...] = grad[y_up, half:, :, :GLA].astype(BF16)
        send(near_p, r_near_p, g_s.at[2], g_r.at[2], up)
        gradient_of(3)
        near_m[...] = grad[y_down, :half, :, :GLA].astype(BF16)
        send(near_m, r_near_m, g_s.at[3], g_r.at[3], down)
        gradient_of(0)
        b_give[:, NY] = tail[...].astype(BF16)
        z_order = (4, 3, 5, 2, 6, 1, 7)
        z_near = (1, 7, 2, 6, 3, 5, 4)
        for dz in z_order:
            zz = mod(z + dz, NZ)
            send(b_give.at[zz], b_take.at[dz - 1], b_s.at[0], b_r.at[dz - 1], {"z": zz})
    with jax.named_scope("g_relay"):
        arrived(r_far_p, g_s.at[0], g_r.at[0], down)
        relay_p[...] = (grad[y_up, :half, :, :GLA] + r_far_p[...].astype(F32)).astype(BF16)
        send(relay_p, r_relay_p, g_s.at[4], g_r.at[4], up)
        arrived(r_far_m, g_s.at[1], g_r.at[1], up)
        relay_m[...] = (grad[y_down, half:, :, :GLA] + r_far_m[...].astype(F32)).astype(BF16)
        send(relay_m, r_relay_m, g_s.at[5], g_r.at[5], down)
    with jax.named_scope("loss2"):
        loss_sum = collected(l_take, 34, loss_sum, "row")
        exchange(sy_give, sy_take, 24, loss_sum, "y")
    with jax.named_scope("g_ysum"):
        arrived(r_near_p, g_s.at[2], g_r.at[2], down)
        arrived(r_near_m, g_s.at[3], g_r.at[3], up)
        arrived(r_relay_p, g_s.at[4], g_r.at[4], down)
        arrived(r_relay_m, g_s.at[5], g_r.at[5], up)
        grad[y, :half, :, :GLA] += r_relay_p[...].astype(F32) + r_near_m[...].astype(F32)
        grad[y, half:, :, :GLA] += r_near_p[...].astype(F32) + r_relay_m[...].astype(F32)
        z_give[...] = grad[y, :, :, :GLA].astype(z_give.dtype)
        for dz in z_order:
            zz = mod(z + dz, NZ)
            send(z_give.at[zz], z_take.at[dz - 1], z_s.at[0], z_r.at[dz - 1], {"z": zz})
    with jax.named_scope("g_bz"):
        for dy in range(NY):
            yb_give[dy, 0] = grad[mod(y + dy, NY), pl.ds(z, 1), :, GLA:GLB].reshape(EG, GLB - GLA)
        last = tail[pl.ds(z, 1)].reshape(EG, 128)
        for dz in z_near:
            arrived(b_take.at[dz - 1], b_s.at[0], b_r.at[dz - 1], {"z": mod(z - dz, NZ)})
        for dz in z_near:
            yb_give[:, 0] += b_take[dz - 1, :NY].astype(F32)
            last = last + b_take[dz - 1, NY].astype(F32)
        for dy in range(NY):
            yb_give[dy, 1] = last
        for dy in (2, 1, 3):
            yy = mod(y + dy, NY)
            send(yb_give.at[dy], yb_take.at[dy - 1], yb_s.at[0], yb_r.at[dy - 1], {"y": yy})
    with jax.named_scope("g_by"):
        right = yb_give[0, 0]
        last = last[:, 0:32]
        for dy in (1, 3, 2):
            arrived(yb_take.at[dy - 1], yb_s.at[0], yb_r.at[dy - 1], {"y": mod(y - dy, NY)})
            right = right + yb_take[dy - 1, 0]
            last = last + yb_take[dy - 1, 1][:, 32 * dy : 32 * dy + 32]
    with jax.named_scope("loss3"):
        loss_sum = collected(sy_take, 24, loss_sum, "y")
        exchange(sz_give, sz_take, 27, loss_sum, "z")
    with jax.named_scope("g_z"):
        left = grad[y, pl.ds(z, 1), :, :GLA].reshape(EG, GLA)
        for dz in z_near:
            arrived(z_take.at[dz - 1], z_s.at[0], z_r.at[dz - 1], {"z": mod(z - dz, NZ)})
            left = left + z_take[dz - 1].astype(F32)
        grad[y, pl.ds(z, 1), :, :GLA] = left.reshape(1, EG, GLA)
        grad[y, pl.ds(z, 1), :, GLA:GLB] = right.reshape(1, EG, GLB - GLA)
        grad[y, pl.ds(z, 1), :, GLB : GLB + 32] = last.reshape(1, EG, 32)

    g = grad[y, pl.ds(z, 1)].reshape(EG, KP)
    e_id = lax.broadcasted_iota(jnp.int32, (EG, KP), 0)
    k_id = lax.broadcasted_iota(jnp.int32, (EG, KP), 1)
    squared = jnp.where((e_id < ED) & (k_id < KD), g * g + FLOOR_VALUE, 0.0)

    with jax.named_scope("st_row"):
        e_col = e_id[:, 0:128]
        l_col = k_id[:, 0:128]
        rows = jnp.broadcast_to(jnp.sum(squared, axis=1, keepdims=True), (EG, 128))
        exchange(row_give, row_take, 0, rows, "row")
        cols = jnp.sum(squared, axis=0, keepdims=True)
        rows = collected(row_take, 0, rows, "row")
        row_line = jnp.sum(jnp.where(e_col == l_col, rows, 0.0), axis=0, keepdims=True)[:, :ED]
        row_line = DECAY_RATE * row_moment[...].reshape(1, ED) + (1.0 - DECAY_RATE) * row_line / FF
        new_row = jnp.sum(
            jnp.where(
                e_id[:, :ED] == k_id[:, :ED], jnp.broadcast_to(row_line, (EG, ED)), 0.0
            ), axis=1, keepdims=True
        )
        new_row = jnp.where(e_col[:, 0:1] < ED, new_row, 1.0)
        ratio = jnp.sum(g * g / new_row, axis=0, keepdims=True)
    with jax.named_scope("st_col"):
        cols2 = jnp.concatenate([cols, ratio], axis=1)
        exchange(cy_give, cy_take, 7, cols2, "y")
        cols2 = collected(cy_take, 7, cols2, "y")
        exchange(cz_give, cz_take, 10, cols2, "z")
        cols2 = collected(cz_take, 10, cols2, "z")
    with jax.named_scope("st_tot"):
        cols, ratio = cols2[:, :KP], cols2[:, KP:]
        col_line = DECAY_RATE * col_moment[...].reshape(1, KD) + (1.0 - DECAY_RATE) * cols[:, :KD] / D
        raw_sum = jnp.sum(ratio[:, :KD] / col_line, axis=1, keepdims=True)
        exchange(s_give, s_take, 17, jnp.broadcast_to(raw_sum, (1, 128)), "row")
        raw = g[:ED, :KD] / jnp.sqrt(new_row[:ED] * col_line)
        loss_sum = collected(sz_take, 27, loss_sum, "z")
        small_out[...] = jnp.zeros_like(small_out)
        small_out[0:1, :KD] = col_line
        small_out[1:2, :ED] = row_line
        small_out[2:3, 0:128] = loss_sum * (1.0 / BATCH)
        both = collected(s_take, 17, jnp.broadcast_to(raw_sum, (1, 128)), "row")
    with jax.named_scope("upd"):
        rms = jnp.sqrt(both[:, 0:1] / (D * FF))
        update_out[...] = raw / jnp.maximum(1.0, rms / CLIP_LEVEL)
    with jax.named_scope("finish"):
        w.finish()
        t.finish()
        all_sent(h_out.at[pl.ds(0, 7)], h_s.at[0], h_r.at[0], {"c": other})
        for k, (ref, device) in enumerate(
            ((far_p, up), (far_m, down), (near_p, up), (near_m, down), (relay_p, up), (relay_m, down))
        ):
            all_sent(ref, g_s.at[k], g_r.at[k], device)
        all_sent(z_take, z_s.at[0], z_r.at[0], {"z": mod(z + 1, NZ)})
        all_sent(b_take, b_s.at[0], b_r.at[0], {"z": mod(z + 1, NZ)})
        all_sent(yb_take, yb_s.at[0], yb_r.at[0], up)


def step_kernel(hidden, weight, text, pooled, row_moment, col_moment, scale, bias):
    vmem = pl.BlockSpec(memory_space=pltpu.VMEM)
    smem = pl.BlockSpec(memory_space=pltpu.SMEM)
    n_row = NX * NC
    dma = pltpu.SemaphoreType.DMA
    return pl.pallas_call(
        whole_kernel,
        out_shape=(
            jax.ShapeDtypeStruct((ED, KD), F32),
            jax.ShapeDtypeStruct((8, KP), F32),
        ),
        in_specs=[vmem] * 6 + [smem] * 2,
        out_specs=(vmem,) * 2,
        scratch_shapes=[
            pltpu.VMEM((n_row, TOK, KP), BF16),
            pltpu.VMEM((EP, KP), BF16),
            pltpu.VMEM((NX * TOK, NY * TOK), F32),
            pltpu.VMEM((NX * TOK, NY * TOK), F32),
            pltpu.VMEM((NX * TOK, NY * TOK), BF16),
            pltpu.VMEM((NX * TOK, NY * TOK), BF16),
            pltpu.VMEM((n_row, TOK, KP), BF16),
            pltpu.VMEM((n_row, TOK, D), BF16),
            pltpu.VMEM((8, NY * TOK), F32),
            pltpu.VMEM((NZ * NY, EP, WLA), BF16),
            pltpu.VMEM((NY * NZ, EP, KP - WLA), BF16),
            pltpu.VMEM((D, KP), BF16),
            pltpu.VMEM((NZ * NY, TOK, TLA), BF16),
            pltpu.VMEM((NY * NZ, TOK, D - TLA), BF16),
            pltpu.VMEM((TOK, D), BF16),
            pltpu.VMEM((n_row, TOK, D), F32),
            pltpu.VMEM((NX, TOK, D), F32),
            pltpu.VMEM((NX, TOK, D), F32),
            pltpu.VMEM((NX - 1, TOK, D), BF16),
            pltpu.VMEM((NX - 1, TOK, D), BF16),
            pltpu.VMEM((n_row, TOK, D), BF16),
            pltpu.VMEM((TOK, D), F32),
            pltpu.VMEM((TOK, 128), F32),
            pltpu.VMEM((n_row, TOK, D), F32),
            pltpu.VMEM((NX, TOK, D), BF16),
            pltpu.VMEM((NX, TOK, D), BF16),
            pltpu.VMEM((NX - 1, TOK, D), BF16),
            pltpu.VMEM((NX - 1, TOK, D), BF16),
            pltpu.VMEM((NY, NZ, EG, KP), F32),
            *[pltpu.VMEM((NZ // 2, EG, GLA), BF16)] * 12,
            pltpu.VMEM((NZ, EG, GLA), BF16),
            pltpu.VMEM((NZ - 1, EG, GLA), BF16),
            pltpu.VMEM((NZ, EG, 128), F32),
            pltpu.VMEM((NZ, NY + 1, EG, 128), BF16),
            pltpu.VMEM((NZ - 1, NY + 1, EG, 128), BF16),
            pltpu.VMEM((NY, 2, EG, 128), F32),
            pltpu.VMEM((NY - 1, 2, EG, 128), F32),
            pltpu.VMEM((EG, 128), F32),
            pltpu.VMEM((n_row - 1, EG, 128), F32),
            pltpu.VMEM((1, 2 * KP), F32),
            pltpu.VMEM((NY - 1, 1, 2 * KP), F32),
            pltpu.VMEM((1, 2 * KP), F32),
            pltpu.VMEM((NZ - 1, 1, 2 * KP), F32),
            pltpu.VMEM((1, 128), F32),
            pltpu.VMEM((n_row - 1, 1, 128), F32),
            pltpu.VMEM((1, 128), F32),
            pltpu.VMEM((n_row - 1, 1, 128), F32),
            pltpu.VMEM((1, 128), F32),
            pltpu.VMEM((NY - 1, 1, 128), F32),
            pltpu.VMEM((1, 128), F32),
            pltpu.VMEM((NZ - 1, 1, 128), F32),
            dma((2,)), dma((N_MSG,)), dma((2,)), dma((N_MSG,)),
            dma((1,)), dma((7,)), dma((2,)), dma((7,)), dma((1,)), dma((8,)),
            dma((2,)), dma((7,)), dma((1,)), dma((8,)),
            dma((6,)), dma((6,)), dma((1,)), dma((7,)), dma((1,)), dma((7,)),
            dma((1,)), dma((3,)), dma((7,)), dma((41,)),
        ],
        compiler_params=pltpu.CompilerParams(
            collective_id=0, has_side_effects=True, vmem_limit_bytes=60 * 1024 * 1024
        ),
        name="step",
    )(hidden, weight, text, pooled, row_moment, col_moment, scale, bias)


def out_kernel(update_in, small, update, new_row, new_col, loss):
    update[...] = update_in[...]
    new_row[...] = small[1:2, :ED].reshape(ED)
    new_col[...] = small[0:1, :KD].reshape(KD)
    loss[0] = small[2, 0]


def per_device(pooled, hidden, text, weight, row_moment, col_moment, log_scale, bias):
    update, small = step_kernel(
        hidden, weight, text, pooled, row_moment, col_moment, jnp.exp(log_scale).reshape(1), bias.reshape(1)
    )
    vmem = pl.BlockSpec(memory_space=pltpu.VMEM)
    update, new_row, new_col, loss = pl.pallas_call(
        out_kernel,
        out_shape=(
            jax.ShapeDtypeStruct((ED, KD), F32),
            jax.ShapeDtypeStruct((ED,), F32),
            jax.ShapeDtypeStruct((KD,), F32),
            jax.ShapeDtypeStruct((1,), F32),
        ),
        in_specs=[vmem] * 2,
        out_specs=(vmem, vmem, vmem, pl.BlockSpec(memory_space=pltpu.SMEM)),
        name="out",
    )(update, small)
    return (update, new_row, new_col, loss.reshape(()))


def solution(mesh):
    finer = Mesh(mesh.devices.reshape(NX, NC, NY, NZ), ALL)
    return jax.shard_map(
        per_device,
        mesh=finer,
        in_specs=(
            P(ALL, None), P(ALL, None), P(ALL, None), P(COL, ROW), P(COL), P(ROW), P(), P(),
        ),
        out_specs=(P(COL, ROW), P(COL), P(ROW), P()),
        check_vma=False,
    )
```

```python
import functools

import jax
import jax.numpy as jnp
from jax import lax
from jax.experimental import pallas as pl
from jax.experimental.pallas import tpu as pltpu
from jax.sharding import Mesh
from jax.sharding import PartitionSpec as P

D = 1152
FF = 4304
NX, NC, NY, NZ = 4, 2, 4, 8
TOK = 64
KD = FF // (NX * NC)
KP = 640
ED = D // (NY * NZ)
EP = 48
WLA = 256
TLA = 512
EG = 40
GLA = 384
GLB = 512
ROW = ("x", "c")
COL = ("y", "z")
ALL = ("x", "c", "y", "z")
BATCH = TOK * NX * NC * NY * NZ

EPSILON = 1e-06
DECAY_RATE = 0.8
CLIP_LEVEL = 1.0
FLOOR_VALUE = 1e-30

MESH = pl.DeviceIdType.MESH
F32 = jnp.float32
BF16 = jnp.bfloat16


def mod(value, size):
    return lax.rem(value + 2 * size, size)


def send(src, dst, ssem, rsem, device):
    pltpu.make_async_remote_copy(src, dst, ssem, rsem, device_id=device, device_id_type=MESH).start()


def arrived(dst, ssem, rsem, device):
    pltpu.make_async_remote_copy(dst, dst, ssem, rsem, device_id=device, device_id_type=MESH).wait_recv()


def all_sent(ref, ssem, rsem, device):
    pltpu.make_async_remote_copy(ref, ref, ssem, rsem, device_id=device, device_id_type=MESH).wait_send()


A0, AP, AM, BP, BM, YP, YM, Y2 = 0, 4, 20, 36, 40, 44, 52, 60
N_MSG = 68
EXCHANGES = (0, 7, 10, 17, 24, 27, 34)
A_MSG = range(A0, BP)
OFFSETS = [0, -1, 1, -2, 2, -3, 3, -4]


class PlaneGather:
    def __init__(self, piece, a, b, la, rows, direct, ssem, rsem, y, z):
        self.direct = direct
        self.piece, self.a, self.b, self.la, self.rows = piece, a, b, la, pl.ds(0, rows)
        self.piece_a = piece.at[self.rows, pl.ds(0, la)]
        self.piece_b = piece.at[self.rows, pl.ds(la, piece.shape[1] - la)]
        self.ssem, self.rsem, self.y, self.z = ssem, rsem, y, z
        self.ys = {o: mod(y + o, NY) for o in range(1 - NY, NY)}
        self.zs = {o: mod(z + o, NZ) for o in range(-(NZ // 2), NZ // 2 + 1)}
        self.sems = [(ssem.at[0 if i in A_MSG else 1], rsem.at[i]) for i in range(N_MSG)]
        self.a_at = {(o, dy): a.at[self.zs[o] * NY + self.ys[-dy], self.rows] for o in self.zs for dy in range(NY)}
        self.b_at = {(yo, o): b.at[self.ys[yo] * NZ + self.zs[o], self.rows] for o in self.zs for yo in range(-2, 3)}

    def _send(self, src, dst, i, device):
        send(src, dst, *self.sems[i], device)

    def _wait(self, dst, i, device):
        sems = self.sems[i] if isinstance(i, int) else (self.ssem.at[1], self.rsem.at[i])
        arrived(dst, *sems, device)

    def own(self):
        self.a[self.z * NY + self.y] = self.piece[:, : self.la]
        self.b[self.y * NZ + self.z] = self.piece[:, self.la :]

    def finish(self):
        n = pl.ds(0, NY * NZ - 1)
        all_sent(self.a.at[n, self.rows], *self.sems[A0], self._zdev(1))
        all_sent(self.b.at[n, self.rows], *self.sems[BP], self._zdev(1))

    def _a(self, zo, dy):
        return self.a_at[zo, dy]

    def _b(self, yo, zo):
        return self.b_at[yo, zo]

    def _zdev(self, o):
        return {"z": self.zs[o]}

    def _ydev(self, o):
        return {"y": self.ys[o]}

    @staticmethod
    def _has(sign, s, dy):
        if s < NZ // 2:
            return s >= 1
        return s == NZ // 2 and (dy < NY // 2) == (sign > 0)

    def _ring_a(self, s, dy, sign):
        if not self._has(sign, s, dy):
            return
        src = self._a(-sign * (s - 1), dy)
        dst = src
        if s == 1 and dy == 0:
            src = self.piece_a
        self._send(src, dst, (AP if sign > 0 else AM) + (s - 1) * 4 + dy, self._zdev(sign))

    def _ring_b(self, s, sign):
        if s > (NZ // 2 if sign > 0 else NZ // 2 - 1):
            return
        dst = self._b(0, -sign * (s - 1))
        src = self.piece_b if s == 1 else dst
        self._send(src, dst, (BP if sign > 0 else BM) + s - 1, self._zdev(sign))

    def _spread_b(self, j):
        dst = self._b(0, OFFSETS[j])
        src = self.piece_b if j == 0 else dst
        self._send(src, dst, YP + j, self._ydev(1))
        self._send(src, dst, YM + j, self._ydev(-1))

    def _near_b(self, j):
        o = OFFSETS[j]
        self._wait(self._b(-1, o), YP + j, self._ydev(-1))
        if j % 2 == 0:
            self._send(self._b(-1, o), self._b(-1, o), Y2 + j, self._ydev(1))
        self._wait(self._b(1, o), YM + j, self._ydev(1))
        if j % 2 == 1:
            self._send(self._b(1, o), self._b(1, o), Y2 + j, self._ydev(-1))

    def far(self, j):
        o = OFFSETS[j]
        yo = -2 if j % 2 == 0 else 2
        self._wait(self._b(yo, o), Y2 + j, self._ydev(-1 if j % 2 == 0 else 1))

    def far_at(self, j):
        if isinstance(j, int):
            return self.far(j)
        hop = (j + 1) // 2
        zz = mod(self.z + hop * (1 - 2 * lax.rem(j, 2)), NZ)
        self._wait(self.b.at[self.ys[2] * NZ + zz, self.rows], Y2 + j, self._ydev(1))

    def start(self):
        for dy in range(1, NY):
            self._send(self.piece_a, self._a(0, 0), A0 + dy - 1, self._ydev(dy))
        if self.direct:
            for s, sign in ((4, 1), (3, -1), (3, 1), (2, -1), (2, 1), (1, -1), (1, 1)):
                self._send(self.piece_b, self._b(0, 0), (BP if sign > 0 else BM) + s - 1, self._zdev(sign * s))
        for sign in (1, -1):
            if not self.direct:
                self._ring_b(1, sign)
            self._ring_a(1, 0, sign)
        self._spread_b(0)

    def step(self, k):
        for s_sign in (1, -1):
            if k <= (NZ // 2 if s_sign > 0 else NZ // 2 - 1):
                self._wait(self._b(0, -s_sign * k), (BP if s_sign > 0 else BM) + k - 1, self._zdev(-s_sign))
                if not self.direct:
                    self._ring_b(k + 1, s_sign)
                self._spread_b(OFFSETS.index(-s_sign * k))
        for dy in range(NY):
            if k == 1:
                if dy == 0:
                    continue
                self._wait(self._a(0, dy), A0 + dy - 1, self._ydev(-dy))
                self._ring_a(1, dy, 1)
                self._ring_a(1, dy, -1)
                continue
            s = k - 1
            for sign in (1, -1):
                if self._has(sign, s, dy):
                    self._wait(
                        self._a(-sign * s, dy), (AP if sign > 0 else AM) + (s - 1) * 4 + dy, self._zdev(-sign)
                    )
                    self._ring_a(s + 1, dy, sign)
        for j, o in enumerate(OFFSETS):
            if abs(o) == k - 1:
                self._near_b(j)


def whole_kernel(
    hidden_in, weight_in, text_in, pooled_in, row_in, col_in, scale_ref, bias_ref,
    update_out, small_out,
    hidden, weight, text, pooled, row_moment, col_moment, in_s,
    hid, wp, logit_a, logit_b, pg_a, pg_b,
    h_out, mg_out, loss_out,
    wa, wb, wc, ta, tb, tn, part, give, take, share, got, img, unit, length,
    acc, give2, take2, share2, got2,
    grad, far_p, far_m, near_p, near_m, relay_p, relay_m,
    r_far_p, r_far_m, r_near_p, r_near_m, r_relay_p, r_relay_m,
    z_give, z_take, tail, b_give, b_take, yb_give, yb_take,
    row_give, row_take, cy_give, cy_take, cz_give, cz_take,
    s_give, s_take, l_give, l_take, sy_give, sy_take, sz_give, sz_take,
    w_s, w_r, t_s, t_r, h_s, h_r, p_s, p_r, i_s, i_r, u_s, u_r, m_s, m_r,
    g_s, g_r, z_s, z_r, b_s, b_r, yb_s, yb_r, st_s, st_r,
):
    x, c = lax.axis_index("x"), lax.axis_index("c")
    y, z = lax.axis_index("y"), lax.axis_index("z")
    me = c * NX + x
    other = 1 - c

    loads = [
        pltpu.make_async_copy(src, dst, in_s.at[i])
        for i, (src, dst) in enumerate(
            (
                (weight_in, weight), (hidden_in, hidden), (text_in, text), (pooled_in, pooled),
                (row_in, row_moment), (col_in, col_moment),
            )
        )
    ]
    for load in loads:
        load.start()
    wa[...] = jnp.zeros_like(wa)
    wb[...] = jnp.zeros_like(wb)
    with jax.named_scope("signal"):
        barrier = pltpu.get_barrier_semaphore()
        peers = [{"z": mod(z + dz, NZ)} for dz in range(1, NZ)]
        peers += [{"y": mod(y + dy, NY)} for dy in range(1, NY)]
        peers += [
            {"x": mod(x + dx, NX), "c": lax.rem(c + dc, NC)}
            for dx in range(NX) for dc in range(NC) if dx + dc > 0
        ]
        for peer in peers:
            pl.semaphore_signal(barrier, inc=1, device_id=peer, device_id_type=MESH)

    with jax.named_scope("prep"):
        for load in loads:
            load.wait()
        wp[...] = jnp.zeros_like(wp)
        wp[:ED, :KD] = weight[...].astype(BF16)
        hid[...] = jnp.zeros_like(hid)
        for r in range(NX * NC):
            hid[(r % NC) * NX + r // NC, :, :KD] = hidden[:, KD * r : KD * (r + 1)]
    with jax.named_scope("barrier"):
        pl.semaphore_wait(barrier, len(peers))
    w = PlaneGather(wp, wa, wb, WLA, EG, False, w_s, w_r, y, z)
    t = PlaneGather(tn, ta, tb, TLA, TOK, False, t_s, t_r, y, z)

    with jax.named_scope("wstart"):
        w.start()
        row_peers = [(dx, dc) for dx in range(NX) for dc in range(NC) if dx + dc > 0]
        for i, (dx, dc) in enumerate(row_peers):
            xx, cc = mod(x + dx, NX), lax.rem(c + dc, NC)
            send(hid.at[cc * NX + xx], h_out.at[me], h_s.at[0], h_r.at[i], {"x": xx, "c": cc})
        h_out[me] = hid[me]
        w.own()
        tf = text[...].astype(F32)
        tn[...] = (tf / jnp.sqrt(jnp.sum(tf * tf, axis=1, keepdims=True) + EPSILON)).astype(BF16)
    with jax.named_scope("w123"):
        w.step(1)
        w.step(2)
        w.step(3)
    with jax.named_scope("tstart"):
        t.own()
        t.start()
    with jax.named_scope("w45far"):
        w.step(4)
        w.step(5)
        for j in range(8):
            w.far(j)

    with jax.named_scope("compact"):
        r_id = lax.broadcasted_iota(jnp.int32, (4 * ED, 4 * EP), 0)
        c_id = lax.broadcasted_iota(jnp.int32, (4 * ED, 4 * EP), 1)
        pick = jnp.zeros((4 * ED, 4 * EP), F32)
        for g in range(4):
            hit = (r_id >= ED * g) & (r_id < ED * (g + 1)) & (c_id - r_id == (EP - ED) * g)
            pick = jnp.where(hit, 1.0, pick)
        pick = pick.astype(BF16)
        for g in range(8):
            yy, z0 = g // 2, 4 * (g % 2)
            wc[pl.ds(4 * ED * g, 4 * ED), 0:WLA] = jnp.dot(
                pick, jnp.concatenate([wa[(z0 + k) * NY + yy] for k in range(4)], axis=0), preferred_element_type=F32
            ).astype(BF16)
            wc[pl.ds(4 * ED * g, 4 * ED), WLA:KP] = jnp.dot(
                pick, wb[yy * NZ + z0 : yy * NZ + z0 + 4].reshape(4 * EP, KP - WLA), preferred_element_type=F32
            ).astype(BF16)

    with jax.named_scope("hwait"):
        for i, (dx, dc) in enumerate(row_peers):
            xx, cc = mod(x - dx, NX), lax.rem(c + dc, NC)
            arrived(h_out.at[cc * NX + xx], h_s.at[0], h_r.at[i], {"x": xx, "c": cc})

    def project(half):
        rows = h_out[pl.ds(half * NX, NX)].reshape(NX * TOK, KP)
        for n in range(3):
            part[pl.ds(half * NX, NX), :, 384 * n : 384 * (n + 1)] = lax.dot_general(
                rows, wc[384 * n : 384 * (n + 1), :], (((1,), (1,)), ((), ())), preferred_element_type=F32
            ).reshape(NX, TOK, 384)

    hf_rows = [pl.ds(TOK // 2 * hf, TOK // 2) for hf in range(2)]

    def reduce_rows(val, gv, tk, sh, gt, ss, rs):
        for dx in (2, 1, 3, 0):
            xx = mod(x + dx, NX)
            gv[xx] = val[other * NX + xx].astype(gv.dtype)
            send(gv.at[xx], tk.at[xx], ss.at[0], rs.at[dx], {"c": other})
        yield
        for hf, rows in enumerate(hf_rows):
            for dx in (2, 1, 3):
                xx = mod(x + dx, NX)
                if hf == 0:
                    arrived(tk.at[xx], ss.at[0], rs.at[dx], {"c": other})
                    sh[dx - 1] = (val[c * NX + xx] + tk[xx].astype(F32)).astype(BF16)
                send(sh.at[dx - 1, rows], gt.at[dx - 1, rows], ss.at[1], rs.at[3 + 3 * hf + dx], {"x": xx})
        yield
        arrived(tk.at[x], ss.at[0], rs.at[0], {"c": other})
        for hf, rows in enumerate(hf_rows):
            total = val[me, rows] + tk[x, rows].astype(F32)
            for dx in (1, 3, 2):
                arrived(gt.at[dx - 1, rows], ss.at[1], rs.at[3 + 3 * hf + dx], {"x": mod(x - dx, NX)})
            for dx in (1, 2, 3):
                total = total + gt[dx - 1, rows].astype(F32)
            yield total
        all_sent(gv, ss.at[0], rs.at[0], {"c": other})
        all_sent(sh, ss.at[1], rs.at[4], {"x": mod(x + 1, NX)})
        yield

    def share_rows(buf, ss, rs):
        for hf, rows in enumerate(hf_rows):
            mine = buf.at[me, rows]
            for dx in (2, 1, 3):
                send(mine, mine, ss.at[0], rs.at[8 * hf + dx], {"x": mod(x + dx, NX)})
            send(mine, mine, ss.at[0], rs.at[8 * hf + 4], {"c": other})
            yield
        for hf, rows in enumerate(hf_rows):
            for dx in (1, 3, 2):
                got_at = buf.at[c * NX + mod(x - dx, NX), rows]
                arrived(got_at, ss.at[0], rs.at[8 * hf + dx], {"x": mod(x - dx, NX)})
                send(got_at, got_at, ss.at[0], rs.at[8 * hf + 4 + dx], {"c": other})
        for hf, rows in enumerate(hf_rows):
            for dx in (0, 1, 3, 2):
                at = buf.at[other * NX + mod(x - dx, NX), rows]
                arrived(at, ss.at[0], rs.at[8 * hf + 4 + dx], {"c": other})
        all_sent(buf.at[pl.ds(0, 7)], ss.at[0], rs.at[1], {"c": other})
        yield

    with jax.named_scope("proj1"):
        project(other)
    with jax.named_scope("red1a"):
        red = reduce_rows(part, give, take, share, got, p_s, p_r)
        next(red)
    with jax.named_scope("proj2"):
        project(c)
    with jax.named_scope("t1"):
        t.step(1)
    with jax.named_scope("red1b"):
        next(red)
    with jax.named_scope("t2"):
        t.step(2)
    with jax.named_scope("red1c_norm"):
        give_img = share_rows(img, i_s, i_r)
        for rows in hf_rows:
            mixed = pooled[rows].astype(F32) + next(red)
            ln = jnp.sqrt(jnp.sum(mixed * mixed, axis=1, keepdims=True) + EPSILON)
            length[rows] = jnp.broadcast_to(ln, (TOK // 2, 128))
            un = mixed / ln
            unit[rows] = un
            img[me, rows] = un.astype(BF16)
            next(give_img)
        next(red)
    with jax.named_scope("t3"):
        t.step(3)
    with jax.named_scope("imgshare"):
        next(give_img)
    with jax.named_scope("pairs"):
        scale = jnp.exp(jnp.broadcast_to(scale_ref[0], (8, 128)))[0:1, 0:1]
        bias = bias_ref[0]
        acc[...] = jnp.zeros_like(acc)
        loss_out[...] = jnp.zeros_like(loss_out)
        tile = NX * TOK
        t_dims = (((1,), (1,)), ((), ()))

        halves = (other, c)

        def texts(g):
            t_b = jnp.concatenate([tb[yy * NZ + g] for yy in range(NY)], axis=0)
            return ta[pl.ds(g * NY, NY)].reshape(NY * TOK, TLA), t_b

        def logits_of(g, h, out):
            t_a, t_b = texts(g)
            images = img[pl.ds(halves[h] * NX, NX)].reshape(tile, D)
            out[...] = lax.dot_general(
                images[:, :TLA], t_a, t_dims, preferred_element_type=F32
            ) + lax.dot_general(images[:, TLA:], t_b, t_dims, preferred_element_type=F32)

        def elementwise(src, out, own):
            m = scale * src[...] + bias
            if own:
                col = lax.broadcasted_iota(jnp.int32, (tile, NY * TOK), 1)
                row = lax.broadcasted_iota(jnp.int32, (tile, NY * TOK), 0)
                same = (row - col == TOK * (x - y)) & (col >= TOK * y) & (col < TOK * y + TOK)
                m = jnp.where(same, -m, m)
            e = jnp.exp(-jnp.abs(m))
            d = 1.0 + e
            r = 1.0 / d
            soft = jnp.maximum(m, 0.0) + (jnp.log(d) + (e - (d - 1.0)) * r)
            loss_out[...] += jnp.sum(soft.reshape(tile // 8, 8, NY * TOK), axis=0)
            sig = jnp.where(m >= 0.0, r, e * r)
            if own:
                sig = jnp.where(same, -sig, sig)
            out[...] = sig.astype(BF16)

        def to_images(g, h, src):
            t_a, t_b = texts(g)
            pg = src[...]
            rows = pl.ds(halves[h] * NX, NX)
            acc[rows, :, :TLA] += jnp.dot(pg, t_a, preferred_element_type=F32).reshape(NX, TOK, TLA)
            acc[rows, :, TLA:] += jnp.dot(pg, t_b, preferred_element_type=F32).reshape(NX, TOK, D - TLA)

        def group(j):
            hop = (j + 1) // 2
            return mod(z + hop * (1 - 2 * lax.rem(j, 2)), NZ)

        def body(j, carry):
            @pl.when(j == 3)
            def _():
                with jax.named_scope("p_t4"):
                    t.step(4)

            @pl.when(j == 5)
            def _():
                with jax.named_scope("p_t5"):
                    t.step(5)

            with jax.named_scope("p_far"):
                t.far_at(j)
            now, last = group(j), group(j - 1)
            logits_of(now, 0, logit_a)
            elementwise(logit_b, pg_b, False)
            to_images(last, 0, pg_a)
            logits_of(now, 1, logit_b)
            elementwise(logit_a, pg_a, False)
            to_images(last, 1, pg_b)
            return carry

        t.far_at(1)
        first, final = mod(z + OFFSETS[1], NZ), mod(z + OFFSETS[7], NZ)
        logits_of(first, 0, logit_a)
        logits_of(first, 1, logit_b)
        elementwise(logit_a, pg_a, False)
        lax.fori_loop(2, NZ, body, 0)
        t.far_at(0)
        logits_of(z, 0, logit_a)
        elementwise(logit_b, pg_b, False)
        to_images(final, 0, pg_a)
        logits_of(z, 1, logit_b)
        elementwise(logit_a, pg_a, False)
        to_images(final, 1, pg_b)
        to_images(z, 0, pg_a)
    with jax.named_scope("red2"):
        red = reduce_rows(acc, give2, take2, share2, got2, u_s, u_r)
        next(red)
        elementwise(logit_b, pg_b, True)
        to_images(z, 1, pg_b)
        next(red)
        give_mg = share_rows(mg_out, m_s, m_r)
        for rows in hf_rows:
            ug = (scale * (1.0 / BATCH)) * next(red)
            un = unit[rows]
            mg = (ug - un * jnp.sum(un * ug, axis=1, keepdims=True)) / length[rows, 0:1]
            mg_out[me, rows] = mg.astype(BF16)
            next(give_mg)
        next(red)
    with jax.named_scope("mgshare"):
        next(give_mg)

    def exchange(give_ref, take_ref, base, value, kind):
        give_ref[...] = value
        slot = EXCHANGES.index(base)
        sizes = {"row": row_peers, "y": range(1, NY), "z": range(1, NZ)}[kind]
        for i, d in enumerate(sizes):
            if kind == "row":
                device = {"x": mod(x + d[0], NX), "c": lax.rem(c + d[1], NC)}
            else:
                device = {kind: mod((y if kind == "y" else z) + d, NY if kind == "y" else NZ)}
            send(give_ref, take_ref.at[i], st_s.at[slot], st_r.at[base + i], device)

    def collected(take_ref, base, value, kind):
        slot = EXCHANGES.index(base)
        sizes = {"row": row_peers, "y": range(1, NY), "z": range(1, NZ)}[kind]
        for i, d in enumerate(sizes):
            if kind == "row":
                device = {"x": mod(x - d[0], NX), "c": lax.rem(c + d[1], NC)}
            else:
                device = {kind: mod((y if kind == "y" else z) - d, NY if kind == "y" else NZ)}
            arrived(take_ref.at[i], st_s.at[slot], st_r.at[base + i], device)
            value = value + take_ref[i]
        all_sent(take_ref, st_s.at[slot], st_r.at[base], device)
        return value

    zi = lax.broadcasted_iota(jnp.int32, (NZ, EG, 384), 0)
    ji = lax.broadcasted_iota(jnp.int32, (NZ, EG, 384), 1)
    li = lax.broadcasted_iota(jnp.int32, (NZ, EG, 384), 2)
    h_all = h_out[...].reshape(NX * NC * TOK, KP)

    def gradient_of(dy):
        yy = mod(y + dy, NY)
        choose = jnp.where((ji < ED) & (li == 32 * yy + ED * zi + ji), 1.0, 0.0)
        choose = choose.reshape(NZ * EG, 384).astype(BF16)
        mg = mg_out[:, :, pl.ds(pl.multiple_of(256 * yy, 128), 384)].reshape(NX * NC * TOK, 384)
        mg_t = lax.dot_general(choose, mg, (((1,), (1,)), ((), ())), preferred_element_type=F32).astype(BF16)
        grad[yy] = jnp.dot(mg_t, h_all, preferred_element_type=F32).reshape(NZ, EG, KP)
        b_give[:, dy] = grad[yy, :, :, GLA:GLB].astype(BF16)
        tail[:, :, 32 * dy : 32 * dy + 32] = grad[yy, :, :, GLB : GLB + 32]

    with jax.named_scope("loss1"):
        loss_sum = jnp.sum(jnp.sum(loss_out[...], axis=0, keepdims=True), axis=1, keepdims=True)
        loss_sum = jnp.broadcast_to(loss_sum, (1, 128))
        exchange(l_give, l_take, 34, loss_sum, "row")
    with jax.named_scope("g_far"):
        half = NZ // 2
        y_far, y_up, y_down = mod(y + 2, NY), mod(y + 1, NY), mod(y - 1, NY)
        up, down = {"y": y_up}, {"y": y_down}
        gradient_of(2)
        far_p[...] = grad[y_far, :half, :, :GLA].astype(BF16)
        far_m[...] = grad[y_far, half:, :, :GLA].astype(BF16)
        send(far_p, r_far_p, g_s.at[0], g_r.at[0], up)
        send(far_m, r_far_m, g_s.at[1], g_r.at[1], down)
    with jax.named_scope("g_rest"):
        gradient_of(1)
        near_p[...] = grad[y_up, half:, :, :GLA].astype(BF16)
        send(near_p, r_near_p, g_s.at[2], g_r.at[2], up)
        gradient_of(3)
        near_m[...] = grad[y_down, :half, :, :GLA].astype(BF16)
        send(near_m, r_near_m, g_s.at[3], g_r.at[3], down)
        gradient_of(0)
        b_give[:, NY] = tail[...].astype(BF16)
        z_order = (4, 3, 5, 2, 6, 1, 7)
        z_near = (1, 7, 2, 6, 3, 5, 4)
        for dz in z_order:
            zz = mod(z + dz, NZ)
            send(b_give.at[zz], b_take.at[dz - 1], b_s.at[0], b_r.at[dz - 1], {"z": zz})
    with jax.named_scope("g_relay"):
        arrived(r_far_p, g_s.at[0], g_r.at[0], down)
        relay_p[...] = (grad[y_up, :half, :, :GLA] + r_far_p[...].astype(F32)).astype(BF16)
        send(relay_p, r_relay_p, g_s.at[4], g_r.at[4], up)
        arrived(r_far_m, g_s.at[1], g_r.at[1], up)
        relay_m[...] = (grad[y_down, half:, :, :GLA] + r_far_m[...].astype(F32)).astype(BF16)
        send(relay_m, r_relay_m, g_s.at[5], g_r.at[5], down)
    with jax.named_scope("loss2"):
        loss_sum = collected(l_take, 34, loss_sum, "row")
        exchange(sy_give, sy_take, 24, loss_sum, "y")
    with jax.named_scope("g_ysum"):
        arrived(r_near_p, g_s.at[2], g_r.at[2], down)
        arrived(r_near_m, g_s.at[3], g_r.at[3], up)
        arrived(r_relay_p, g_s.at[4], g_r.at[4], down)
        arrived(r_relay_m, g_s.at[5], g_r.at[5], up)
        grad[y, :half, :, :GLA] += r_relay_p[...].astype(F32) + r_near_m[...].astype(F32)
        grad[y, half:, :, :GLA] += r_near_p[...].astype(F32) + r_relay_m[...].astype(F32)
        z_give[...] = grad[y, :, :, :GLA].astype(z_give.dtype)
        for dz in z_order:
            zz = mod(z + dz, NZ)
            send(z_give.at[zz], z_take.at[dz - 1], z_s.at[0], z_r.at[dz - 1], {"z": zz})
    with jax.named_scope("g_bz"):
        for dy in range(NY):
            yb_give[dy, 0] = grad[mod(y + dy, NY), pl.ds(z, 1), :, GLA:GLB].reshape(EG, GLB - GLA)
        last = tail[pl.ds(z, 1)].reshape(EG, 128)
        for dz in z_near:
            arrived(b_take.at[dz - 1], b_s.at[0], b_r.at[dz - 1], {"z": mod(z - dz, NZ)})
        for dz in z_near:
            yb_give[:, 0] += b_take[dz - 1, :NY].astype(F32)
            last = last + b_take[dz - 1, NY].astype(F32)
        for dy in range(NY):
            yb_give[dy, 1] = last
        for dy in (2, 1, 3):
            yy = mod(y + dy, NY)
            send(yb_give.at[dy], yb_take.at[dy - 1], yb_s.at[0], yb_r.at[dy - 1], {"y": yy})
    with jax.named_scope("g_by"):
        right = yb_give[0, 0]
        last = last[:, 0:32]
        for dy in (1, 3, 2):
            arrived(yb_take.at[dy - 1], yb_s.at[0], yb_r.at[dy - 1], {"y": mod(y - dy, NY)})
            right = right + yb_take[dy - 1, 0]
            last = last + yb_take[dy - 1, 1][:, 32 * dy : 32 * dy + 32]
    with jax.named_scope("loss3"):
        loss_sum = collected(sy_take, 24, loss_sum, "y")
        exchange(sz_give, sz_take, 27, loss_sum, "z")
    with jax.named_scope("g_z"):
        left = grad[y, pl.ds(z, 1), :, :GLA].reshape(EG, GLA)
        for dz in z_near:
            arrived(z_take.at[dz - 1], z_s.at[0], z_r.at[dz - 1], {"z": mod(z - dz, NZ)})
            left = left + z_take[dz - 1].astype(F32)
        grad[y, pl.ds(z, 1), :, :GLA] = left.reshape(1, EG, GLA)
        grad[y, pl.ds(z, 1), :, GLA:GLB] = right.reshape(1, EG, GLB - GLA)
        grad[y, pl.ds(z, 1), :, GLB : GLB + 32] = last.reshape(1, EG, 32)

    g = grad[y, pl.ds(z, 1)].reshape(EG, KP)
    e_id = lax.broadcasted_iota(jnp.int32, (EG, KP), 0)
    k_id = lax.broadcasted_iota(jnp.int32, (EG, KP), 1)
    squared = jnp.where((e_id < ED) & (k_id < KD), g * g + FLOOR_VALUE, 0.0)

    with jax.named_scope("st_row"):
        e_col = e_id[:, 0:128]
        l_col = k_id[:, 0:128]
        rows = jnp.broadcast_to(jnp.sum(squared, axis=1, keepdims=True), (EG, 128))
        exchange(row_give, row_take, 0, rows, "row")
        cols = jnp.sum(squared, axis=0, keepdims=True)
        rows = collected(row_take, 0, rows, "row")
        row_line = jnp.sum(jnp.where(e_col == l_col, rows, 0.0), axis=0, keepdims=True)[:, :ED]
        row_line = DECAY_RATE * row_moment[...].reshape(1, ED) + (1.0 - DECAY_RATE) * row_line / FF
        new_row = jnp.sum(
            jnp.where(
                e_id[:, :ED] == k_id[:, :ED], jnp.broadcast_to(row_line, (EG, ED)), 0.0
            ), axis=1, keepdims=True
        )
        new_row = jnp.where(e_col[:, 0:1] < ED, new_row, 1.0)
        ratio = jnp.sum(g * g / new_row, axis=0, keepdims=True)
    with jax.named_scope("st_col"):
        cols2 = jnp.concatenate([cols, ratio], axis=1)
        exchange(cy_give, cy_take, 7, cols2, "y")
        cols2 = collected(cy_take, 7, cols2, "y")
        exchange(cz_give, cz_take, 10, cols2, "z")
        cols2 = collected(cz_take, 10, cols2, "z")
    with jax.named_scope("st_tot"):
        cols, ratio = cols2[:, :KP], cols2[:, KP:]
        col_line = DECAY_RATE * col_moment[...].reshape(1, KD) + (1.0 - DECAY_RATE) * cols[:, :KD] / D
        raw_sum = jnp.sum(ratio[:, :KD] / col_line, axis=1, keepdims=True)
        exchange(s_give, s_take, 17, jnp.broadcast_to(raw_sum, (1, 128)), "row")
        raw = g[:ED, :KD] / jnp.sqrt(new_row[:ED] * col_line)
        loss_sum = collected(sz_take, 27, loss_sum, "z")
        small_out[...] = jnp.zeros_like(small_out)
        small_out[0:1, :KD] = col_line
        small_out[1:2, :ED] = row_line
        small_out[2:3, 0:128] = loss_sum * (1.0 / BATCH)
        both = collected(s_take, 17, jnp.broadcast_to(raw_sum, (1, 128)), "row")
    with jax.named_scope("upd"):
        rms = jnp.sqrt(both[:, 0:1] / (D * FF))
        update_out[...] = raw / jnp.maximum(1.0, rms / CLIP_LEVEL)
    with jax.named_scope("finish"):
        w.finish()
        t.finish()
        all_sent(h_out.at[pl.ds(0, 7)], h_s.at[0], h_r.at[0], {"c": other})
        for k, (ref, device) in enumerate(
            ((far_p, up), (far_m, down), (near_p, up), (near_m, down), (relay_p, up), (relay_m, down))
        ):
            all_sent(ref, g_s.at[k], g_r.at[k], device)
        all_sent(z_take, z_s.at[0], z_r.at[0], {"z": mod(z + 1, NZ)})
        all_sent(b_take, b_s.at[0], b_r.at[0], {"z": mod(z + 1, NZ)})
        all_sent(yb_take, yb_s.at[0], yb_r.at[0], up)


def step_kernel(hidden, weight, text, pooled, row_moment, col_moment, scale, bias):
    vmem = pl.BlockSpec(memory_space=pltpu.VMEM)
    smem = pl.BlockSpec(memory_space=pltpu.SMEM)
    n_row = NX * NC
    dma = pltpu.SemaphoreType.DMA
    return pl.pallas_call(
        whole_kernel,
        out_shape=(
            jax.ShapeDtypeStruct((ED, KD), F32),
            jax.ShapeDtypeStruct((8, KP), F32),
        ),
        in_specs=[pl.BlockSpec(memory_space=pl.ANY)] * 6 + [smem] * 2,
        out_specs=(vmem,) * 2,
        scratch_shapes=[
            pltpu.VMEM((TOK, FF), BF16),
            pltpu.VMEM((ED, KD), F32),
            pltpu.VMEM((TOK, D), BF16),
            pltpu.VMEM((TOK, D), BF16),
            pltpu.VMEM((ED,), F32),
            pltpu.VMEM((KD,), F32),
            dma((6,)),
            pltpu.VMEM((n_row, TOK, KP), BF16),
            pltpu.VMEM((EP, KP), BF16),
            pltpu.VMEM((NX * TOK, NY * TOK), F32),
            pltpu.VMEM((NX * TOK, NY * TOK), F32),
            pltpu.VMEM((NX * TOK, NY * TOK), BF16),
            pltpu.VMEM((NX * TOK, NY * TOK), BF16),
            pltpu.VMEM((n_row, TOK, KP), BF16),
            pltpu.VMEM((n_row, TOK, D), BF16),
            pltpu.VMEM((8, NY * TOK), F32),
            pltpu.VMEM((NZ * NY, EP, WLA), BF16),
            pltpu.VMEM((NY * NZ, EP, KP - WLA), BF16),
            pltpu.VMEM((D, KP), BF16),
            pltpu.VMEM((NZ * NY, TOK, TLA), BF16),
            pltpu.VMEM((NY * NZ, TOK, D - TLA), BF16),
            pltpu.VMEM((TOK, D), BF16),
            pltpu.VMEM((n_row, TOK, D), F32),
            pltpu.VMEM((NX, TOK, D), F32),
            pltpu.VMEM((NX, TOK, D), F32),
            pltpu.VMEM((NX - 1, TOK, D), BF16),
            pltpu.VMEM((NX - 1, TOK, D), BF16),
            pltpu.VMEM((n_row, TOK, D), BF16),
            pltpu.VMEM((TOK, D), F32),
            pltpu.VMEM((TOK, 128), F32),
            pltpu.VMEM((n_row, TOK, D), F32),
            pltpu.VMEM((NX, TOK, D), BF16),
            pltpu.VMEM((NX, TOK, D), BF16),
            pltpu.VMEM((NX - 1, TOK, D), BF16),
            pltpu.VMEM((NX - 1, TOK, D), BF16),
            pltpu.VMEM((NY, NZ, EG, KP), F32),
            *[pltpu.VMEM((NZ // 2, EG, GLA), BF16)] * 12,
            pltpu.VMEM((NZ, EG, GLA), BF16),
            pltpu.VMEM((NZ - 1, EG, GLA), BF16),
            pltpu.VMEM((NZ, EG, 128), F32),
            pltpu.VMEM((NZ, NY + 1, EG, 128), BF16),
            pltpu.VMEM((NZ - 1, NY + 1, EG, 128), BF16),
            pltpu.VMEM((NY, 2, EG, 128), F32),
            pltpu.VMEM((NY - 1, 2, EG, 128), F32),
            pltpu.VMEM((EG, 128), F32),
            pltpu.VMEM((n_row - 1, EG, 128), F32),
            pltpu.VMEM((1, 2 * KP), F32),
            pltpu.VMEM((NY - 1, 1, 2 * KP), F32),
            pltpu.VMEM((1, 2 * KP), F32),
            pltpu.VMEM((NZ - 1, 1, 2 * KP), F32),
            pltpu.VMEM((1, 128), F32),
            pltpu.VMEM((n_row - 1, 1, 128), F32),
            pltpu.VMEM((1, 128), F32),
            pltpu.VMEM((n_row - 1, 1, 128), F32),
            pltpu.VMEM((1, 128), F32),
            pltpu.VMEM((NY - 1, 1, 128), F32),
            pltpu.VMEM((1, 128), F32),
            pltpu.VMEM((NZ - 1, 1, 128), F32),
            dma((2,)), dma((N_MSG,)), dma((2,)), dma((N_MSG,)),
            dma((1,)), dma((7,)), dma((2,)), dma((10,)), dma((1,)), dma((16,)),
            dma((2,)), dma((10,)), dma((1,)), dma((16,)),
            dma((6,)), dma((6,)), dma((1,)), dma((7,)), dma((1,)), dma((7,)),
            dma((1,)), dma((3,)), dma((7,)), dma((41,)),
        ],
        compiler_params=pltpu.CompilerParams(
            collective_id=0, has_side_effects=True, vmem_limit_bytes=60 * 1024 * 1024
        ),
        name="step",
    )(hidden, weight, text, pooled, row_moment, col_moment, scale, bias)


def out_kernel(update_in, small, update, new_row, new_col, loss):
    update[...] = update_in[...]
    new_row[...] = small[1:2, :ED].reshape(ED)
    new_col[...] = small[0:1, :KD].reshape(KD)
    loss[0] = small[2, 0]


def per_device(pooled, hidden, text, weight, row_moment, col_moment, log_scale, bias):
    update, small = step_kernel(
        hidden, weight, text, pooled, row_moment, col_moment, log_scale.reshape(1), bias.reshape(1)
    )
    vmem = pl.BlockSpec(memory_space=pltpu.VMEM)
    update, new_row, new_col, loss = pl.pallas_call(
        out_kernel,
        out_shape=(
            jax.ShapeDtypeStruct((ED, KD), F32),
            jax.ShapeDtypeStruct((ED,), F32),
            jax.ShapeDtypeStruct((KD,), F32),
            jax.ShapeDtypeStruct((1,), F32),
        ),
        in_specs=[vmem] * 2,
        out_specs=(vmem, vmem, vmem, pl.BlockSpec(memory_space=pltpu.SMEM)),
        name="out",
    )(update, small)
    return (update, new_row, new_col, loss.reshape(()))


def solution(mesh):
    finer = Mesh(mesh.devices.reshape(NX, NC, NY, NZ), ALL)
    return jax.shard_map(
        per_device,
        mesh=finer,
        in_specs=(
            P(ALL, None), P(ALL, None), P(ALL, None), P(COL, ROW), P(COL), P(ROW), P(), P(),
        ),
        out_specs=(P(COL, ROW), P(COL), P(ROW), P()),
        check_vma=False,
    )
```

```python
import functools

import jax
import jax.numpy as jnp
from jax import lax
from jax.experimental import pallas as pl
from jax.experimental.pallas import tpu as pltpu
from jax.sharding import Mesh
from jax.sharding import PartitionSpec as P

D = 1152
FF = 4304
NX, NC, NY, NZ = 4, 2, 4, 8
TOK = 64
KD = FF // (NX * NC)
KP = 640
ED = D // (NY * NZ)
EP = 48
WLA = 256
TLA = 512
EG = 40
GLA = 384
GLB = 512
ROW = ("x", "c")
COL = ("y", "z")
ALL = ("x", "c", "y", "z")
BATCH = TOK * NX * NC * NY * NZ

EPSILON = 1e-06
DECAY_RATE = 0.8
CLIP_LEVEL = 1.0
FLOOR_VALUE = 1e-30

MESH = pl.DeviceIdType.MESH
F32 = jnp.float32
BF16 = jnp.bfloat16


def mod(value, size):
    return lax.rem(value + 2 * size, size)


def send(src, dst, ssem, rsem, device):
    pltpu.make_async_remote_copy(src, dst, ssem, rsem, device_id=device, device_id_type=MESH).start()


def arrived(dst, ssem, rsem, device):
    pltpu.make_async_remote_copy(dst, dst, ssem, rsem, device_id=device, device_id_type=MESH).wait_recv()


def all_sent(ref, ssem, rsem, device):
    pltpu.make_async_remote_copy(ref, ref, ssem, rsem, device_id=device, device_id_type=MESH).wait_send()


A0, AP, AM, BP, BM, YP, YM, Y2 = 0, 4, 20, 36, 40, 44, 52, 60
N_MSG = 68
B_PLACE = (3, 1, 0, 2)
EXCHANGES = (0, 7, 10, 17, 24, 27, 34)
A_MSG = range(A0, BP)
OFFSETS = [0, -1, 1, -2, 2, -3, 3, -4]


class PlaneGather:
    def __init__(self, piece, a, b, la, rows, direct, ssem, rsem, y, z):
        self.direct = direct
        self.piece, self.a, self.b, self.la, self.rows = piece, a, b, la, pl.ds(0, rows)
        self.piece_a = piece.at[self.rows, pl.ds(0, la)]
        self.piece_b = piece.at[self.rows, pl.ds(la, piece.shape[1] - la)]
        self.ssem, self.rsem, self.y, self.z = ssem, rsem, y, z
        self.ys = {o: mod(y + o, NY) for o in range(1 - NY, NY)}
        self.zs = {o: mod(z + o, NZ) for o in range(-(NZ // 2), NZ // 2 + 1)}
        self.sems = [(ssem.at[0 if i in A_MSG else 1], rsem.at[i]) for i in range(N_MSG)]
        self.a_at = {(o, dy): a.at[self.zs[o] * NY + self.ys[-dy], self.rows] for o in self.zs for dy in range(NY)}
        self.b_at = {(yo, o): b.at[self.ys[yo] * NZ + self.zs[o], self.rows] for o in self.zs for yo in range(-2, 3)}

    def _send(self, src, dst, i, device):
        send(src, dst, *self.sems[i], device)

    def _wait(self, dst, i, device):
        sems = self.sems[i] if isinstance(i, int) else (self.ssem.at[1], self.rsem.at[i])
        arrived(dst, *sems, device)

    def own(self):
        self.a[self.z * NY + self.y] = self.piece[:, : self.la]
        self.b[self.y * NZ + self.z] = self.piece[:, self.la :]

    def finish(self):
        n = pl.ds(0, NY * NZ - 1)
        all_sent(self.a.at[n, self.rows], *self.sems[A0], self._zdev(1))
        all_sent(self.b.at[n, self.rows], *self.sems[BP], self._zdev(1))

    def _a(self, zo, dy):
        return self.a_at[zo, dy]

    def _b(self, yo, zo):
        return self.b_at[yo, zo]

    def _zdev(self, o):
        return {"z": self.zs[o]}

    def _ydev(self, o):
        return {"y": self.ys[o]}

    @staticmethod
    def _has(sign, s, dy):
        if s < NZ // 2:
            return s >= 1
        return s == NZ // 2 and (dy < NY // 2) == (sign > 0)

    def _ring_a(self, s, dy, sign):
        if not self._has(sign, s, dy):
            return
        src = self._a(-sign * (s - 1), dy)
        dst = src
        if s == 1 and dy == 0:
            src = self.piece_a
        self._send(src, dst, (AP if sign > 0 else AM) + (s - 1) * 4 + dy, self._zdev(sign))

    def _ring_b(self, s, sign):
        if s > (NZ // 2 if sign > 0 else NZ // 2 - 1):
            return
        dst = self._b(0, -sign * (s - 1))
        src = self.piece_b if s == 1 else dst
        self._send(src, dst, (BP if sign > 0 else BM) + s - 1, self._zdev(sign))

    def _spread_b(self, j):
        dst = self._b(0, OFFSETS[j])
        src = self.piece_b if j == 0 else dst
        self._send(src, dst, YP + j, self._ydev(1))
        self._send(src, dst, YM + j, self._ydev(-1))

    def _near_b(self, j):
        o = OFFSETS[j]
        self._wait(self._b(-1, o), YP + j, self._ydev(-1))
        if j % 2 == 0:
            self._send(self._b(-1, o), self._b(-1, o), Y2 + j, self._ydev(1))
        self._wait(self._b(1, o), YM + j, self._ydev(1))
        if j % 2 == 1:
            self._send(self._b(1, o), self._b(1, o), Y2 + j, self._ydev(-1))

    def far(self, j):
        o = OFFSETS[j]
        yo = -2 if j % 2 == 0 else 2
        self._wait(self._b(yo, o), Y2 + j, self._ydev(-1 if j % 2 == 0 else 1))

    def far_at(self, j):
        if isinstance(j, int):
            return self.far(j)
        hop = (j + 1) // 2
        zz = mod(self.z + hop * (1 - 2 * lax.rem(j, 2)), NZ)
        self._wait(self.b.at[self.ys[2] * NZ + zz, self.rows], Y2 + j, self._ydev(1))

    def start(self):
        for dy in range(1, NY):
            self._send(self.piece_a, self._a(0, 0), A0 + dy - 1, self._ydev(dy))
        if self.direct:
            for s, sign in ((4, 1), (3, -1), (3, 1), (2, -1), (2, 1), (1, -1), (1, 1)):
                self._send(self.piece_b, self._b(0, 0), (BP if sign > 0 else BM) + s - 1, self._zdev(sign * s))
        for sign in (1, -1):
            if not self.direct:
                self._ring_b(1, sign)
            self._ring_a(1, 0, sign)
        self._spread_b(0)

    def step(self, k):
        for s_sign in (1, -1):
            if k <= (NZ // 2 if s_sign > 0 else NZ // 2 - 1):
                self._wait(self._b(0, -s_sign * k), (BP if s_sign > 0 else BM) + k - 1, self._zdev(-s_sign))
                if not self.direct:
                    self._ring_b(k + 1, s_sign)
                self._spread_b(OFFSETS.index(-s_sign * k))
        for dy in range(NY):
            if k == 1:
                if dy == 0:
                    continue
                self._wait(self._a(0, dy), A0 + dy - 1, self._ydev(-dy))
                self._ring_a(1, dy, 1)
                self._ring_a(1, dy, -1)
                continue
            s = k - 1
            for sign in (1, -1):
                if self._has(sign, s, dy):
                    self._wait(
                        self._a(-sign * s, dy), (AP if sign > 0 else AM) + (s - 1) * 4 + dy, self._zdev(-sign)
                    )
                    self._ring_a(s + 1, dy, sign)
        for j, o in enumerate(OFFSETS):
            if abs(o) == k - 1:
                self._near_b(j)


def whole_kernel(
    hidden_in, weight_in, text_in, pooled_in, row_in, col_in, scale_ref, bias_ref,
    update_out, small_out,
    hidden, weight, text, pooled, row_moment, col_moment, in_s,
    hid, wp, logit_a, logit_b, pg_a, pg_b,
    h_out, mg_out, loss_out,
    wa, wb, wc, ta, tb, tn, part, give, take, share, got, img, unit, length,
    acc, give2, take2, share2, got2,
    grad, far_p, far_m, near_p, near_m, relay_p, relay_m,
    r_far_p, r_far_m, r_near_p, r_near_m, r_relay_p, r_relay_m,
    z_give, z_take, tail, b_give, b_take, yb_give, yb_take,
    row_give, row_take, cy_give, cy_take, cz_give, cz_take,
    s_give, s_take, l_give, l_take, sy_give, sy_take, sz_give, sz_take,
    w_s, w_r, t_s, t_r, h_s, h_r, p_s, p_r, i_s, i_r, u_s, u_r, m_s, m_r,
    g_s, g_r, z_s, z_r, b_s, b_r, yb_s, yb_r, st_s, st_r,
):
    x, c = lax.axis_index("x"), lax.axis_index("c")
    y, z = lax.axis_index("y"), lax.axis_index("z")
    me = c * NX + x
    other = 1 - c

    loads = [
        pltpu.make_async_copy(src, dst, in_s.at[i])
        for i, (src, dst) in enumerate(
            (
                (weight_in, weight), (hidden_in, hidden), (text_in, text), (pooled_in, pooled),
                (row_in, row_moment), (col_in, col_moment),
            )
        )
    ]
    for load in loads:
        load.start()
    wa[...] = jnp.zeros_like(wa)
    wb[...] = jnp.zeros_like(wb)
    with jax.named_scope("signal"):
        barrier = pltpu.get_barrier_semaphore()
        peers = [{"z": mod(z + dz, NZ)} for dz in range(1, NZ)]
        peers += [{"y": mod(y + dy, NY)} for dy in range(1, NY)]
        peers += [
            {"x": mod(x + dx, NX), "c": lax.rem(c + dc, NC)}
            for dx in range(NX) for dc in range(NC) if dx + dc > 0
        ]
        for peer in peers:
            pl.semaphore_signal(barrier, inc=1, device_id=peer, device_id_type=MESH)

    with jax.named_scope("prep"):
        for load in loads:
            load.wait()
        wp[...] = jnp.zeros_like(wp)
        wp[:ED, :KD] = weight[...].astype(BF16)
        hid[...] = jnp.zeros_like(hid)
        for r in range(NX * NC):
            hid[(r % NC) * NX + r // NC, :, :KD] = hidden[:, KD * r : KD * (r + 1)]
    with jax.named_scope("barrier"):
        pl.semaphore_wait(barrier, len(peers))
    w = PlaneGather(wp, wa, wb, WLA, EG, False, w_s, w_r, y, z)
    t = PlaneGather(tn, ta, tb, TLA, TOK, False, t_s, t_r, y, z)

    with jax.named_scope("wstart"):
        w.start()
        row_peers = [(dx, dc) for dx in range(NX) for dc in range(NC) if dx + dc > 0]
        for i, (dx, dc) in enumerate(row_peers):
            xx, cc = mod(x + dx, NX), lax.rem(c + dc, NC)
            send(hid.at[cc * NX + xx], h_out.at[me], h_s.at[0], h_r.at[i], {"x": xx, "c": cc})
        h_out[me] = hid[me]
        w.own()
        tf = text[...].astype(F32)
        tn[...] = (tf / jnp.sqrt(jnp.sum(tf * tf, axis=1, keepdims=True) + EPSILON)).astype(BF16)
    with jax.named_scope("w123"):
        w.step(1)
        w.step(2)
        w.step(3)
    with jax.named_scope("tstart"):
        t.own()
        t.start()
    with jax.named_scope("w45far"):
        w.step(4)
        w.step(5)
    with jax.named_scope("t1"):
        t.step(1)
    with jax.named_scope("wfar"):
        for j in range(8):
            w.far(j)

    with jax.named_scope("compact"):
        r_id = lax.broadcasted_iota(jnp.int32, (4 * ED, 4 * EP), 0)
        c_id = lax.broadcasted_iota(jnp.int32, (4 * ED, 4 * EP), 1)
        pick = jnp.zeros((4 * ED, 4 * EP), F32)
        for g in range(4):
            hit = (r_id >= ED * g) & (r_id < ED * (g + 1)) & (c_id - r_id == (EP - ED) * g)
            pick = jnp.where(hit, 1.0, pick)
        pick = pick.astype(BF16)
        for g in range(8):
            yy, z0 = g // 2, 4 * (g % 2)
            wc[pl.ds(4 * ED * g, 4 * ED), 0:WLA] = jnp.dot(
                pick, jnp.concatenate([wa[(z0 + k) * NY + yy] for k in range(4)], axis=0), preferred_element_type=F32
            ).astype(BF16)
            wc[pl.ds(4 * ED * g, 4 * ED), WLA:KP] = jnp.dot(
                pick, wb[yy * NZ + z0 : yy * NZ + z0 + 4].reshape(4 * EP, KP - WLA), preferred_element_type=F32
            ).astype(BF16)

    with jax.named_scope("hwait"):
        for i, (dx, dc) in enumerate(row_peers):
            xx, cc = mod(x - dx, NX), lax.rem(c + dc, NC)
            arrived(h_out.at[cc * NX + xx], h_s.at[0], h_r.at[i], {"x": xx, "c": cc})

    def project(half):
        rows = h_out[pl.ds(half * NX, NX)].reshape(NX * TOK, KP)
        for n in range(3):
            part[pl.ds(half * NX, NX), :, 384 * n : 384 * (n + 1)] = lax.dot_general(
                rows, wc[384 * n : 384 * (n + 1), :], (((1,), (1,)), ((), ())), preferred_element_type=F32
            ).reshape(NX, TOK, 384)

    hf_rows = [pl.ds(TOK // 2 * hf, TOK // 2) for hf in range(2)]

    def reduce_rows(val, gv, tk, sh, gt, ss, rs):
        for dx in (2, 1, 3, 0):
            xx = mod(x + dx, NX)
            gv[xx] = val[other * NX + xx].astype(gv.dtype)
            send(gv.at[xx], tk.at[xx], ss.at[0], rs.at[dx], {"c": other})
        yield
        for hf, rows in enumerate(hf_rows):
            for dx in (2, 1, 3):
                xx = mod(x + dx, NX)
                if hf == 0:
                    arrived(tk.at[xx], ss.at[0], rs.at[dx], {"c": other})
                    sh[dx - 1] = (val[c * NX + xx] + tk[xx].astype(F32)).astype(BF16)
                send(sh.at[dx - 1, rows], gt.at[dx - 1, rows], ss.at[1], rs.at[3 + 3 * hf + dx], {"x": xx})
        yield
        arrived(tk.at[x], ss.at[0], rs.at[0], {"c": other})
        for hf, rows in enumerate(hf_rows):
            total = val[me, rows] + tk[x, rows].astype(F32)
            for dx in (1, 3, 2):
                arrived(gt.at[dx - 1, rows], ss.at[1], rs.at[3 + 3 * hf + dx], {"x": mod(x - dx, NX)})
            for dx in (1, 2, 3):
                total = total + gt[dx - 1, rows].astype(F32)
            yield total
        all_sent(gv, ss.at[0], rs.at[0], {"c": other})
        all_sent(sh, ss.at[1], rs.at[4], {"x": mod(x + 1, NX)})
        yield

    def share_rows(buf, ss, rs):
        for hf, rows in enumerate(hf_rows):
            mine = buf.at[me, rows]
            for dx in (2, 1, 3):
                send(mine, mine, ss.at[0], rs.at[8 * hf + dx], {"x": mod(x + dx, NX)})
            send(mine, mine, ss.at[0], rs.at[8 * hf + 4], {"c": other})
            yield
        for hf, rows in enumerate(hf_rows):
            for dx in (1, 3, 2):
                got_at = buf.at[c * NX + mod(x - dx, NX), rows]
                arrived(got_at, ss.at[0], rs.at[8 * hf + dx], {"x": mod(x - dx, NX)})
                send(got_at, got_at, ss.at[0], rs.at[8 * hf + 4 + dx], {"c": other})
        for hf, rows in enumerate(hf_rows):
            for dx in (0, 1, 3, 2):
                at = buf.at[other * NX + mod(x - dx, NX), rows]
                arrived(at, ss.at[0], rs.at[8 * hf + 4 + dx], {"c": other})
        all_sent(buf.at[pl.ds(0, 7)], ss.at[0], rs.at[1], {"c": other})
        yield

    with jax.named_scope("proj1"):
        project(other)
    with jax.named_scope("red1a"):
        red = reduce_rows(part, give, take, share, got, p_s, p_r)
        next(red)
    with jax.named_scope("proj2"):
        project(c)
    with jax.named_scope("red1b"):
        next(red)
    with jax.named_scope("t2"):
        t.step(2)
    with jax.named_scope("red1c_norm"):
        give_img = share_rows(img, i_s, i_r)
        for hf, rows in enumerate(hf_rows):
            mixed = pooled[rows].astype(F32) + next(red)
            ln = jnp.sqrt(jnp.sum(mixed * mixed, axis=1, keepdims=True) + EPSILON)
            length[rows] = jnp.broadcast_to(ln, (TOK // 2, 128))
            un = mixed / ln
            unit[rows] = un
            img[me, rows] = un.astype(BF16)
            next(give_img)
            if hf == 0:
                t.step(3)
        next(red)
    with jax.named_scope("imgshare"):
        next(give_img)
    with jax.named_scope("t4"):
        t.step(4)
    with jax.named_scope("pairs"):
        scale = jnp.exp(jnp.broadcast_to(scale_ref[0], (8, 128)))[0:1, 0:1]
        bias = bias_ref[0]
        acc[...] = jnp.zeros_like(acc)
        loss_out[...] = jnp.zeros_like(loss_out)
        tile = NX * TOK
        t_dims = (((1,), (1,)), ((), ()))

        halves = (other, c)

        def texts(g):
            t_b = jnp.concatenate([tb[yy * NZ + g] for yy in range(NY)], axis=0)
            return ta[pl.ds(g * NY, NY)].reshape(NY * TOK, TLA), t_b

        def logits_of(g, h, out):
            t_a, t_b = texts(g)
            images = img[pl.ds(halves[h] * NX, NX)].reshape(tile, D)
            out[...] = lax.dot_general(
                images[:, :TLA], t_a, t_dims, preferred_element_type=F32
            ) + lax.dot_general(images[:, TLA:], t_b, t_dims, preferred_element_type=F32)

        def elementwise(src, out, own):
            m = scale * src[...] + bias
            if own:
                col = lax.broadcasted_iota(jnp.int32, (tile, NY * TOK), 1)
                row = lax.broadcasted_iota(jnp.int32, (tile, NY * TOK), 0)
                same = (row - col == TOK * (x - y)) & (col >= TOK * y) & (col < TOK * y + TOK)
                m = jnp.where(same, -m, m)
            e = jnp.exp(-jnp.abs(m))
            d = 1.0 + e
            r = 1.0 / d
            soft = jnp.maximum(m, 0.0) + (jnp.log(d) + (e - (d - 1.0)) * r)
            loss_out[...] += jnp.sum(soft.reshape(tile // 8, 8, NY * TOK), axis=0)
            sig = jnp.where(m >= 0.0, r, e * r)
            if own:
                sig = jnp.where(same, -sig, sig)
            out[...] = sig.astype(BF16)

        def to_images(g, h, src):
            t_a, t_b = texts(g)
            pg = src[...]
            rows = pl.ds(halves[h] * NX, NX)
            acc[rows, :, :TLA] += jnp.dot(pg, t_a, preferred_element_type=F32).reshape(NX, TOK, TLA)
            acc[rows, :, TLA:] += jnp.dot(pg, t_b, preferred_element_type=F32).reshape(NX, TOK, D - TLA)

        def group(j):
            hop = (j + 1) // 2
            return mod(z + hop * (1 - 2 * lax.rem(j, 2)), NZ)

        def body(j, carry):
            @pl.when(j == 5)
            def _():
                with jax.named_scope("p_t5"):
                    t.step(5)

            with jax.named_scope("p_far"):
                t.far_at(j)
            now, last = group(j), group(j - 1)
            logits_of(now, 0, logit_a)
            elementwise(logit_b, pg_b, False)
            to_images(last, 0, pg_a)
            logits_of(now, 1, logit_b)
            elementwise(logit_a, pg_a, False)
            to_images(last, 1, pg_b)
            return carry

        t.far_at(1)
        first, final = mod(z + OFFSETS[1], NZ), mod(z + OFFSETS[7], NZ)
        logits_of(first, 0, logit_a)
        logits_of(first, 1, logit_b)
        elementwise(logit_a, pg_a, False)
        lax.fori_loop(2, NZ, body, 0)
        t.far_at(0)
        logits_of(z, 0, logit_a)
        elementwise(logit_b, pg_b, False)
        to_images(final, 0, pg_a)
        logits_of(z, 1, logit_b)
        elementwise(logit_a, pg_a, False)
        to_images(final, 1, pg_b)
        to_images(z, 0, pg_a)
    with jax.named_scope("red2"):
        red = reduce_rows(acc, give2, take2, share2, got2, u_s, u_r)
        next(red)
        elementwise(logit_b, pg_b, True)
        to_images(z, 1, pg_b)
        next(red)
        give_mg = share_rows(mg_out, m_s, m_r)
        for rows in hf_rows:
            ug = (scale * (1.0 / BATCH)) * next(red)
            un = unit[rows]
            mg = (ug - un * jnp.sum(un * ug, axis=1, keepdims=True)) / length[rows, 0:1]
            mg_out[me, rows] = mg.astype(BF16)
            next(give_mg)
        next(red)
    with jax.named_scope("mgshare"):
        next(give_mg)

    def exchange(give_ref, take_ref, base, value, kind):
        give_ref[...] = value
        slot = EXCHANGES.index(base)
        sizes = {"row": row_peers, "y": range(1, NY), "z": range(1, NZ)}[kind]
        for i, d in enumerate(sizes):
            if kind == "row":
                device = {"x": mod(x + d[0], NX), "c": lax.rem(c + d[1], NC)}
            else:
                device = {kind: mod((y if kind == "y" else z) + d, NY if kind == "y" else NZ)}
            send(give_ref, take_ref.at[i], st_s.at[slot], st_r.at[base + i], device)

    def collected(take_ref, base, value, kind):
        slot = EXCHANGES.index(base)
        sizes = {"row": row_peers, "y": range(1, NY), "z": range(1, NZ)}[kind]
        for i, d in enumerate(sizes):
            if kind == "row":
                device = {"x": mod(x - d[0], NX), "c": lax.rem(c + d[1], NC)}
            else:
                device = {kind: mod((y if kind == "y" else z) - d, NY if kind == "y" else NZ)}
            arrived(take_ref.at[i], st_s.at[slot], st_r.at[base + i], device)
            value = value + take_ref[i]
        all_sent(take_ref, st_s.at[slot], st_r.at[base], device)
        return value

    zi = lax.broadcasted_iota(jnp.int32, (NZ, EG, 384), 0)
    ji = lax.broadcasted_iota(jnp.int32, (NZ, EG, 384), 1)
    li = lax.broadcasted_iota(jnp.int32, (NZ, EG, 384), 2)
    h_all = h_out[...].reshape(NX * NC * TOK, KP)

    def gradient_of(dy):
        yy = mod(y + dy, NY)
        choose = jnp.where((ji < ED) & (li == 32 * yy + ED * zi + ji), 1.0, 0.0)
        choose = choose.reshape(NZ * EG, 384).astype(BF16)
        mg = mg_out[:, :, pl.ds(pl.multiple_of(256 * yy, 128), 384)].reshape(NX * NC * TOK, 384)
        mg_t = lax.dot_general(choose, mg, (((1,), (1,)), ((), ())), preferred_element_type=F32).astype(BF16)
        grad[yy] = jnp.dot(mg_t, h_all, preferred_element_type=F32).reshape(NZ, EG, KP)
        b_give[:, B_PLACE[dy]] = grad[yy, :, :, GLA:GLB].astype(BF16)
        tail[:, :, 32 * dy : 32 * dy + 32] = grad[yy, :, :, GLB : GLB + 32]

    z_order = (4, 3, 5, 2, 6, 1, 7)
    z_near = (1, 7, 2, 6, 3, 5, 4)
    b_parts = (pl.ds(0, 2), pl.ds(2, 3))

    def give_b(k):
        for dz in z_order:
            zz = mod(z + dz, NZ)
            send(
                b_give.at[zz, b_parts[k]], b_take.at[dz - 1, b_parts[k]],
                b_s.at[0], b_r.at[7 * k + dz - 1], {"z": zz},
            )

    with jax.named_scope("loss1"):
        loss_sum = jnp.sum(jnp.sum(loss_out[...], axis=0, keepdims=True), axis=1, keepdims=True)
        loss_sum = jnp.broadcast_to(loss_sum, (1, 128))
        exchange(l_give, l_take, 34, loss_sum, "row")
    with jax.named_scope("g_far"):
        half = NZ // 2
        y_far, y_up, y_down = mod(y + 2, NY), mod(y + 1, NY), mod(y - 1, NY)
        up, down = {"y": y_up}, {"y": y_down}
        gradient_of(2)
        far_p[...] = grad[y_far, :half, :, :GLA].astype(BF16)
        far_m[...] = grad[y_far, half:, :, :GLA].astype(BF16)
        send(far_p, r_far_p, g_s.at[0], g_r.at[0], up)
        send(far_m, r_far_m, g_s.at[1], g_r.at[1], down)
    with jax.named_scope("g_rest"):
        gradient_of(1)
        near_p[...] = grad[y_up, half:, :, :GLA].astype(BF16)
        send(near_p, r_near_p, g_s.at[2], g_r.at[2], up)
        give_b(0)
        gradient_of(3)
        near_m[...] = grad[y_down, :half, :, :GLA].astype(BF16)
        send(near_m, r_near_m, g_s.at[3], g_r.at[3], down)
        gradient_of(0)
        b_give[:, NY] = tail[...].astype(BF16)
        give_b(1)
    with jax.named_scope("g_relay"):
        arrived(r_far_p, g_s.at[0], g_r.at[0], down)
        relay_p[...] = (grad[y_up, :half, :, :GLA] + r_far_p[...].astype(F32)).astype(BF16)
        send(relay_p, r_relay_p, g_s.at[4], g_r.at[4], up)
        arrived(r_far_m, g_s.at[1], g_r.at[1], up)
        relay_m[...] = (grad[y_down, half:, :, :GLA] + r_far_m[...].astype(F32)).astype(BF16)
        send(relay_m, r_relay_m, g_s.at[5], g_r.at[5], down)
    with jax.named_scope("loss2"):
        loss_sum = collected(l_take, 34, loss_sum, "row")
        exchange(sy_give, sy_take, 24, loss_sum, "y")
    with jax.named_scope("g_ysum"):
        arrived(r_near_p, g_s.at[2], g_r.at[2], down)
        arrived(r_near_m, g_s.at[3], g_r.at[3], up)
        arrived(r_relay_p, g_s.at[4], g_r.at[4], down)
        arrived(r_relay_m, g_s.at[5], g_r.at[5], up)
        grad[y, :half, :, :GLA] += r_relay_p[...].astype(F32) + r_near_m[...].astype(F32)
        grad[y, half:, :, :GLA] += r_near_p[...].astype(F32) + r_relay_m[...].astype(F32)
        z_give[...] = grad[y, :, :, :GLA].astype(z_give.dtype)
        for dz in z_order:
            zz = mod(z + dz, NZ)
            send(z_give.at[zz], z_take.at[dz - 1], z_s.at[0], z_r.at[dz - 1], {"z": zz})
    with jax.named_scope("g_bz"):
        for dy in range(NY):
            yb_give[dy, 0] = grad[mod(y + dy, NY), pl.ds(z, 1), :, GLA:GLB].reshape(EG, GLB - GLA)
        last = tail[pl.ds(z, 1)].reshape(EG, 128)
        for dz in z_near:
            for k in range(2):
                arrived(b_take.at[dz - 1, b_parts[k]], b_s.at[0], b_r.at[7 * k + dz - 1], {"z": mod(z - dz, NZ)})
        for dz in z_near:
            for dy in range(NY):
                yb_give[dy, 0] += b_take[dz - 1, B_PLACE[dy]].astype(F32)
            last = last + b_take[dz - 1, NY].astype(F32)
        for dy in range(NY):
            yb_give[dy, 1] = last
        for dy in (2, 1, 3):
            yy = mod(y + dy, NY)
            send(yb_give.at[dy], yb_take.at[dy - 1], yb_s.at[0], yb_r.at[dy - 1], {"y": yy})
    with jax.named_scope("g_by"):
        right = yb_give[0, 0]
        last = last[:, 0:32]
        for dy in (1, 3, 2):
            arrived(yb_take.at[dy - 1], yb_s.at[0], yb_r.at[dy - 1], {"y": mod(y - dy, NY)})
            right = right + yb_take[dy - 1, 0]
            last = last + yb_take[dy - 1, 1][:, 32 * dy : 32 * dy + 32]
    with jax.named_scope("loss3"):
        loss_sum = collected(sy_take, 24, loss_sum, "y")
        exchange(sz_give, sz_take, 27, loss_sum, "z")
    with jax.named_scope("g_z"):
        left = grad[y, pl.ds(z, 1), :, :GLA].reshape(EG, GLA)
        for dz in z_near:
            arrived(z_take.at[dz - 1], z_s.at[0], z_r.at[dz - 1], {"z": mod(z - dz, NZ)})
            left = left + z_take[dz - 1].astype(F32)
        grad[y, pl.ds(z, 1), :, :GLA] = left.reshape(1, EG, GLA)
        grad[y, pl.ds(z, 1), :, GLA:GLB] = right.reshape(1, EG, GLB - GLA)
        grad[y, pl.ds(z, 1), :, GLB : GLB + 32] = last.reshape(1, EG, 32)

    g = grad[y, pl.ds(z, 1)].reshape(EG, KP)
    e_id = lax.broadcasted_iota(jnp.int32, (EG, KP), 0)
    k_id = lax.broadcasted_iota(jnp.int32, (EG, KP), 1)
    squared = jnp.where((e_id < ED) & (k_id < KD), g * g + FLOOR_VALUE, 0.0)

    with jax.named_scope("st_row"):
        e_col = e_id[:, 0:128]
        l_col = k_id[:, 0:128]
        rows = jnp.broadcast_to(jnp.sum(squared, axis=1, keepdims=True), (EG, 128))
        exchange(row_give, row_take, 0, rows, "row")
        cols = jnp.sum(squared, axis=0, keepdims=True)
        rows = collected(row_take, 0, rows, "row")
        row_line = jnp.sum(jnp.where(e_col == l_col, rows, 0.0), axis=0, keepdims=True)[:, :ED]
        row_line = DECAY_RATE * row_moment[...].reshape(1, ED) + (1.0 - DECAY_RATE) * row_line / FF
        new_row = jnp.sum(
            jnp.where(
                e_id[:, :ED] == k_id[:, :ED], jnp.broadcast_to(row_line, (EG, ED)), 0.0
            ), axis=1, keepdims=True
        )
        new_row = jnp.where(e_col[:, 0:1] < ED, new_row, 1.0)
        ratio = jnp.sum(g * g / new_row, axis=0, keepdims=True)
    with jax.named_scope("st_col"):
        cols2 = jnp.concatenate([cols, ratio], axis=1)
        exchange(cy_give, cy_take, 7, cols2, "y")
        cols2 = collected(cy_take, 7, cols2, "y")
        exchange(cz_give, cz_take, 10, cols2, "z")
        cols2 = collected(cz_take, 10, cols2, "z")
    with jax.named_scope("st_tot"):
        cols, ratio = cols2[:, :KP], cols2[:, KP:]
        col_line = DECAY_RATE * col_moment[...].reshape(1, KD) + (1.0 - DECAY_RATE) * cols[:, :KD] / D
        raw_sum = jnp.sum(ratio[:, :KD] / col_line, axis=1, keepdims=True)
        exchange(s_give, s_take, 17, jnp.broadcast_to(raw_sum, (1, 128)), "row")
        raw = g[:ED, :KD] / jnp.sqrt(new_row[:ED] * col_line)
        loss_sum = collected(sz_take, 27, loss_sum, "z")
        small_out[...] = jnp.zeros_like(small_out)
        small_out[0:1, :KD] = col_line
        small_out[1:2, :ED] = row_line
        small_out[2:3, 0:128] = loss_sum * (1.0 / BATCH)
        both = collected(s_take, 17, jnp.broadcast_to(raw_sum, (1, 128)), "row")
    with jax.named_scope("upd"):
        rms = jnp.sqrt(both[:, 0:1] / (D * FF))
        update_out[...] = raw / jnp.maximum(1.0, rms / CLIP_LEVEL)
    with jax.named_scope("finish"):
        w.finish()
        t.finish()
        all_sent(h_out.at[pl.ds(0, 7)], h_s.at[0], h_r.at[0], {"c": other})
        for k, (ref, device) in enumerate(
            ((far_p, up), (far_m, down), (near_p, up), (near_m, down), (relay_p, up), (relay_m, down))
        ):
            all_sent(ref, g_s.at[k], g_r.at[k], device)
        all_sent(z_take, z_s.at[0], z_r.at[0], {"z": mod(z + 1, NZ)})
        all_sent(b_take, b_s.at[0], b_r.at[0], {"z": mod(z + 1, NZ)})
        all_sent(yb_take, yb_s.at[0], yb_r.at[0], up)


def step_kernel(hidden, weight, text, pooled, row_moment, col_moment, scale, bias):
    vmem = pl.BlockSpec(memory_space=pltpu.VMEM)
    smem = pl.BlockSpec(memory_space=pltpu.SMEM)
    n_row = NX * NC
    dma = pltpu.SemaphoreType.DMA
    return pl.pallas_call(
        whole_kernel,
        out_shape=(
            jax.ShapeDtypeStruct((ED, KD), F32),
            jax.ShapeDtypeStruct((8, KP), F32),
        ),
        in_specs=[pl.BlockSpec(memory_space=pl.ANY)] * 6 + [smem] * 2,
        out_specs=(vmem,) * 2,
        scratch_shapes=[
            pltpu.VMEM((TOK, FF), BF16),
            pltpu.VMEM((ED, KD), F32),
            pltpu.VMEM((TOK, D), BF16),
            pltpu.VMEM((TOK, D), BF16),
            pltpu.VMEM((ED,), F32),
            pltpu.VMEM((KD,), F32),
            dma((6,)),
            pltpu.VMEM((n_row, TOK, KP), BF16),
            pltpu.VMEM((EP, KP), BF16),
            pltpu.VMEM((NX * TOK, NY * TOK), F32),
            pltpu.VMEM((NX * TOK, NY * TOK), F32),
            pltpu.VMEM((NX * TOK, NY * TOK), BF16),
            pltpu.VMEM((NX * TOK, NY * TOK), BF16),
            pltpu.VMEM((n_row, TOK, KP), BF16),
            pltpu.VMEM((n_row, TOK, D), BF16),
            pltpu.VMEM((8, NY * TOK), F32),
            pltpu.VMEM((NZ * NY, EP, WLA), BF16),
            pltpu.VMEM((NY * NZ, EP, KP - WLA), BF16),
            pltpu.VMEM((D, KP), BF16),
            pltpu.VMEM((NZ * NY, TOK, TLA), BF16),
            pltpu.VMEM((NY * NZ, TOK, D - TLA), BF16),
            pltpu.VMEM((TOK, D), BF16),
            pltpu.VMEM((n_row, TOK, D), F32),
            pltpu.VMEM((NX, TOK, D), F32),
            pltpu.VMEM((NX, TOK, D), F32),
            pltpu.VMEM((NX - 1, TOK, D), BF16),
            pltpu.VMEM((NX - 1, TOK, D), BF16),
            pltpu.VMEM((n_row, TOK, D), BF16),
            pltpu.VMEM((TOK, D), F32),
            pltpu.VMEM((TOK, 128), F32),
            pltpu.VMEM((n_row, TOK, D), F32),
            pltpu.VMEM((NX, TOK, D), BF16),
            pltpu.VMEM((NX, TOK, D), BF16),
            pltpu.VMEM((NX - 1, TOK, D), BF16),
            pltpu.VMEM((NX - 1, TOK, D), BF16),
            pltpu.VMEM((NY, NZ, EG, KP), F32),
            *[pltpu.VMEM((NZ // 2, EG, GLA), BF16)] * 12,
            pltpu.VMEM((NZ, EG, GLA), BF16),
            pltpu.VMEM((NZ - 1, EG, GLA), BF16),
            pltpu.VMEM((NZ, EG, 128), F32),
            pltpu.VMEM((NZ, NY + 1, EG, 128), BF16),
            pltpu.VMEM((NZ - 1, NY + 1, EG, 128), BF16),
            pltpu.VMEM((NY, 2, EG, 128), F32),
            pltpu.VMEM((NY - 1, 2, EG, 128), F32),
            pltpu.VMEM((EG, 128), F32),
            pltpu.VMEM((n_row - 1, EG, 128), F32),
            pltpu.VMEM((1, 2 * KP), F32),
            pltpu.VMEM((NY - 1, 1, 2 * KP), F32),
            pltpu.VMEM((1, 2 * KP), F32),
            pltpu.VMEM((NZ - 1, 1, 2 * KP), F32),
            pltpu.VMEM((1, 128), F32),
            pltpu.VMEM((n_row - 1, 1, 128), F32),
            pltpu.VMEM((1, 128), F32),
            pltpu.VMEM((n_row - 1, 1, 128), F32),
            pltpu.VMEM((1, 128), F32),
            pltpu.VMEM((NY - 1, 1, 128), F32),
            pltpu.VMEM((1, 128), F32),
            pltpu.VMEM((NZ - 1, 1, 128), F32),
            dma((2,)), dma((N_MSG,)), dma((2,)), dma((N_MSG,)),
            dma((1,)), dma((7,)), dma((2,)), dma((10,)), dma((1,)), dma((16,)),
            dma((2,)), dma((10,)), dma((1,)), dma((16,)),
            dma((6,)), dma((6,)), dma((1,)), dma((7,)), dma((1,)), dma((14,)),
            dma((1,)), dma((3,)), dma((7,)), dma((41,)),
        ],
        compiler_params=pltpu.CompilerParams(
            collective_id=0, has_side_effects=True, vmem_limit_bytes=60 * 1024 * 1024
        ),
        name="step",
    )(hidden, weight, text, pooled, row_moment, col_moment, scale, bias)


def out_kernel(update_in, small, update, new_row, new_col, loss):
    update[...] = update_in[...]
    new_row[...] = small[1:2, :ED].reshape(ED)
    new_col[...] = small[0:1, :KD].reshape(KD)
    loss[0] = small[2, 0]


def per_device(pooled, hidden, text, weight, row_moment, col_moment, log_scale, bias):
    update, small = step_kernel(
        hidden, weight, text, pooled, row_moment, col_moment, log_scale.reshape(1), bias.reshape(1)
    )
    vmem = pl.BlockSpec(memory_space=pltpu.VMEM)
    update, new_row, new_col, loss = pl.pallas_call(
        out_kernel,
        out_shape=(
            jax.ShapeDtypeStruct((ED, KD), F32),
            jax.ShapeDtypeStruct((ED,), F32),
            jax.ShapeDtypeStruct((KD,), F32),
            jax.ShapeDtypeStruct((1,), F32),
        ),
        in_specs=[vmem] * 2,
        out_specs=(vmem, vmem, vmem, pl.BlockSpec(memory_space=pltpu.SMEM)),
        name="out",
    )(update, small)
    return (update, new_row, new_col, loss.reshape(()))


def solution(mesh):
    finer = Mesh(mesh.devices.reshape(NX, NC, NY, NZ), ALL)
    return jax.shard_map(
        per_device,
        mesh=finer,
        in_specs=(
            P(ALL, None), P(ALL, None), P(ALL, None), P(COL, ROW), P(COL), P(ROW), P(), P(),
        ),
        out_specs=(P(COL, ROW), P(COL), P(ROW), P()),
        check_vma=False,
    )
```

```python
import functools

import jax
import jax.numpy as jnp
from jax import lax
from jax.experimental import pallas as pl
from jax.experimental.pallas import tpu as pltpu
from jax.sharding import Mesh
from jax.sharding import PartitionSpec as P

D = 1152
FF = 4304
NX, NC, NY, NZ = 4, 2, 4, 8
TOK = 64
KD = FF // (NX * NC)
KP = 640
ED = D // (NY * NZ)
EP = 48
WLA = 256
TLA = 512
EG = 40
GLA = 384
GLB = 512
ROW = ("x", "c")
COL = ("y", "z")
ALL = ("x", "c", "y", "z")
BATCH = TOK * NX * NC * NY * NZ

EPSILON = 1e-06
DECAY_RATE = 0.8
CLIP_LEVEL = 1.0
FLOOR_VALUE = 1e-30

MESH = pl.DeviceIdType.MESH
F32 = jnp.float32
BF16 = jnp.bfloat16


def mod(value, size):
    return lax.rem(value + 2 * size, size)


def send(src, dst, ssem, rsem, device):
    pltpu.make_async_remote_copy(src, dst, ssem, rsem, device_id=device, device_id_type=MESH).start()


def arrived(dst, ssem, rsem, device):
    pltpu.make_async_remote_copy(dst, dst, ssem, rsem, device_id=device, device_id_type=MESH).wait_recv()


def all_sent(ref, ssem, rsem, device):
    pltpu.make_async_remote_copy(ref, ref, ssem, rsem, device_id=device, device_id_type=MESH).wait_send()


A0, AP, AM, BP, BM, YP, YM, Y2 = 0, 3, 17, 33, 37, 40, 48, 56
N_MSG = 64
B_PLACE = (3, 1, 0, 2)
EXCHANGES = (0, 7, 10, 17, 24, 27, 34)
A_MSG = range(A0, BP)
OFFSETS = [0, -1, 1, -2, 2, -3, 3, -4]


class PlaneGather:
    def __init__(self, piece, a, b, la, rows, direct, ssem, rsem, y, z):
        self.direct = direct
        self.piece, self.a, self.b, self.la, self.rows = piece, a, b, la, pl.ds(0, rows)
        self.piece_a = piece.at[self.rows, pl.ds(0, la)]
        self.piece_b = piece.at[self.rows, pl.ds(la, piece.shape[1] - la)]
        self.ssem, self.rsem, self.y, self.z = ssem, rsem, y, z
        self.ys = {o: mod(y + o, NY) for o in range(1 - NY, NY)}
        self.zs = {o: mod(z + o, NZ) for o in range(-(NZ // 2), NZ // 2 + 1)}
        self.sems = [(ssem.at[0 if i in A_MSG else 1], rsem.at[i]) for i in range(N_MSG)]
        self.a_at = {(o, dy): a.at[self.zs[o] * NY + self.ys[-dy], self.rows] for o in self.zs for dy in range(NY)}
        self.b_at = {(yo, o): b.at[self.ys[yo] * NZ + self.zs[o], self.rows] for o in self.zs for yo in range(-2, 3)}

    def _send(self, src, dst, i, device):
        send(src, dst, *self.sems[i], device)

    def _wait(self, dst, i, device):
        sems = self.sems[i] if isinstance(i, int) else (self.ssem.at[1], self.rsem.at[i])
        arrived(dst, *sems, device)

    def own(self):
        self.a[self.z * NY + self.y] = self.piece[:, : self.la]
        self.b[self.y * NZ + self.z] = self.piece[:, self.la :]

    def finish(self):
        n = pl.ds(0, NY * NZ - 1)
        all_sent(self.a.at[n, self.rows], *self.sems[A0], self._zdev(1))
        all_sent(self.b.at[n, self.rows], *self.sems[BP], self._zdev(1))

    def _a(self, zo, dy):
        return self.a_at[zo, dy]

    def _b(self, yo, zo):
        return self.b_at[yo, zo]

    def _zdev(self, o):
        return {"z": self.zs[o]}

    def _ydev(self, o):
        return {"y": self.ys[o]}

    @staticmethod
    def _has(sign, s, dy):
        if s < NZ // 2:
            return s >= 1
        return s == NZ // 2 and (dy < NY // 2) == (sign > 0)

    def _ring_a(self, s, dy, sign):
        if not self._has(sign, s, dy):
            return
        src = self._a(-sign * (s - 1), dy)
        dst = src
        if s == 1 and dy == 0:
            src = self.piece_a
        self._send(src, dst, (AP if sign > 0 else AM) + (s - 1) * 4 + dy, self._zdev(sign))

    def _ring_b(self, s, sign):
        if s > (NZ // 2 if sign > 0 else NZ // 2 - 1):
            return
        dst = self._b(0, -sign * (s - 1))
        src = self.piece_b if s == 1 else dst
        self._send(src, dst, (BP if sign > 0 else BM) + s - 1, self._zdev(sign))

    def _spread_b(self, j):
        dst = self._b(0, OFFSETS[j])
        src = self.piece_b if j == 0 else dst
        self._send(src, dst, YP + j, self._ydev(1))
        self._send(src, dst, YM + j, self._ydev(-1))

    def _near_b(self, j):
        o = OFFSETS[j]
        self._wait(self._b(-1, o), YP + j, self._ydev(-1))
        if j % 2 == 0:
            self._send(self._b(-1, o), self._b(-1, o), Y2 + j, self._ydev(1))
        self._wait(self._b(1, o), YM + j, self._ydev(1))
        if j % 2 == 1:
            self._send(self._b(1, o), self._b(1, o), Y2 + j, self._ydev(-1))

    def far(self, j):
        o = OFFSETS[j]
        yo = -2 if j % 2 == 0 else 2
        self._wait(self._b(yo, o), Y2 + j, self._ydev(-1 if j % 2 == 0 else 1))

    def far_at(self, j):
        if isinstance(j, int):
            return self.far(j)
        hop = (j + 1) // 2
        zz = mod(self.z + hop * (1 - 2 * lax.rem(j, 2)), NZ)
        self._wait(self.b.at[self.ys[2] * NZ + zz, self.rows], Y2 + j, self._ydev(1))

    def start(self):
        for dy in range(1, NY):
            self._send(self.piece_a, self._a(0, 0), A0 + dy - 1, self._ydev(dy))
        if self.direct:
            for s, sign in ((4, 1), (3, -1), (3, 1), (2, -1), (2, 1), (1, -1), (1, 1)):
                self._send(self.piece_b, self._b(0, 0), (BP if sign > 0 else BM) + s - 1, self._zdev(sign * s))
        for sign in (1, -1):
            if not self.direct:
                self._ring_b(1, sign)
            self._ring_a(1, 0, sign)
        self._spread_b(0)

    def step(self, k):
        for s_sign in (1, -1):
            if k <= (NZ // 2 if s_sign > 0 else NZ // 2 - 1):
                self._wait(self._b(0, -s_sign * k), (BP if s_sign > 0 else BM) + k - 1, self._zdev(-s_sign))
                if not self.direct:
                    self._ring_b(k + 1, s_sign)
                self._spread_b(OFFSETS.index(-s_sign * k))
        for dy in range(NY):
            if k == 1:
                if dy == 0:
                    continue
                self._wait(self._a(0, dy), A0 + dy - 1, self._ydev(-dy))
                self._ring_a(1, dy, 1)
                self._ring_a(1, dy, -1)
                continue
            s = k - 1
            for sign in (1, -1):
                if self._has(sign, s, dy):
                    self._wait(
                        self._a(-sign * s, dy), (AP if sign > 0 else AM) + (s - 1) * 4 + dy, self._zdev(-sign)
                    )
                    self._ring_a(s + 1, dy, sign)
        for j, o in enumerate(OFFSETS):
            if abs(o) == k - 1:
                self._near_b(j)


def whole_kernel(
    hidden_in, weight_in, text_in, pooled_in, row_in, col_in, scale_ref, bias_ref,
    update_out, small_out,
    hidden, weight, text, pooled, row_moment, col_moment, in_s,
    hid, wp, logit_a, logit_b, pg_a, pg_b,
    h_out, mg_out, loss_out,
    wa, wb, wc, ta, tb, tn, part, give, take, share, got, img, unit, length,
    acc, give2, take2, share2, got2,
    grad, far_p, far_m, near_p, near_m, relay_p, relay_m,
    r_far_p, r_far_m, r_near_p, r_near_m, r_relay_p, r_relay_m,
    z_give, z_take, choose, tail, b_give, b_take, yb_give, yb_take,
    row_give, row_take, cy_give, cy_take, cz_give, cz_take,
    s_give, s_take, l_give, l_take, sy_give, sy_take, sz_give, sz_take,
    w_s, w_r, t_s, t_r, h_s, h_r, p_s, p_r, i_s, i_r, u_s, u_r, m_s, m_r,
    g_s, g_r, z_s, z_r, b_s, b_r, yb_s, yb_r, st_s, st_r,
):
    x, c = lax.axis_index("x"), lax.axis_index("c")
    y, z = lax.axis_index("y"), lax.axis_index("z")
    me = c * NX + x
    other = 1 - c

    loads = [
        pltpu.make_async_copy(src, dst, in_s.at[i])
        for i, (src, dst) in enumerate(
            (
                (weight_in, weight), (hidden_in, hidden), (text_in, text), (pooled_in, pooled),
                (row_in, row_moment), (col_in, col_moment),
            )
        )
    ]
    for load in loads:
        load.start()
    wa[...] = jnp.zeros_like(wa)
    wb[...] = jnp.zeros_like(wb)
    with jax.named_scope("signal"):
        barrier = pltpu.get_barrier_semaphore()
        peers = [{"z": mod(z + dz, NZ)} for dz in range(1, NZ)]
        peers += [{"y": mod(y + dy, NY)} for dy in range(1, NY)]
        peers += [
            {"x": mod(x + dx, NX), "c": lax.rem(c + dc, NC)}
            for dx in range(NX) for dc in range(NC) if dx + dc > 0
        ]
        for peer in peers:
            pl.semaphore_signal(barrier, inc=1, device_id=peer, device_id_type=MESH)

    with jax.named_scope("prep"):
        for load in loads:
            load.wait()
        wp[...] = jnp.zeros_like(wp)
        wp[:ED, :KD] = weight[...].astype(BF16)
        hid[...] = jnp.zeros_like(hid)
        for r in range(NX * NC):
            hid[(r % NC) * NX + r // NC, :, :KD] = hidden[:, KD * r : KD * (r + 1)]
    with jax.named_scope("barrier"):
        pl.semaphore_wait(barrier, len(peers))
    w = PlaneGather(wp, wa, wb, WLA, EG, False, w_s, w_r, y, z)
    t = PlaneGather(tn, ta, tb, TLA, TOK, False, t_s, t_r, y, z)

    def project(half, k0, k1):
        rows = h_out[pl.ds(half * NX, NX), :, k0:k1].reshape(NX * TOK, k1 - k0)
        for n in range(3):
            lanes = slice(384 * n, 384 * (n + 1))
            product = lax.dot_general(
                rows, wc[lanes, k0:k1], (((1,), (1,)), ((), ())), preferred_element_type=F32
            ).reshape(NX, TOK, 384)
            at = pl.ds(half * NX, NX)
            part[at, :, lanes] = product if k0 == 0 else part[at, :, lanes] + product

    with jax.named_scope("wstart"):
        w.start()
        row_peers = [(dx, dc) for dx in range(NX) for dc in range(NC) if dx + dc > 0]
        for i, (dx, dc) in enumerate(row_peers):
            xx, cc = mod(x + dx, NX), lax.rem(c + dc, NC)
            send(hid.at[cc * NX + xx], h_out.at[me], h_s.at[0], h_r.at[i], {"x": xx, "c": cc})
        h_out[me] = hid[me]
        w.own()
        tf = text[...].astype(F32)
        tn[...] = (tf / jnp.sqrt(jnp.sum(tf * tf, axis=1, keepdims=True) + EPSILON)).astype(BF16)
    with jax.named_scope("w123"):
        w.step(1)
        w.step(2)
        w.step(3)
    with jax.named_scope("tstart"):
        t.own()
        t.start()
    with jax.named_scope("w45far"):
        w.step(4)
        w.step(5)
    with jax.named_scope("t1"):
        t.step(1)
    with jax.named_scope("hwait"):
        for i, (dx, dc) in enumerate(row_peers):
            xx, cc = mod(x - dx, NX), lax.rem(c + dc, NC)
            arrived(h_out.at[cc * NX + xx], h_s.at[0], h_r.at[i], {"x": xx, "c": cc})

    with jax.named_scope("compactA"):
        r_id = lax.broadcasted_iota(jnp.int32, (4 * ED, 4 * EP), 0)
        c_id = lax.broadcasted_iota(jnp.int32, (4 * ED, 4 * EP), 1)
        pick = jnp.zeros((4 * ED, 4 * EP), F32)
        for g in range(4):
            hit = (r_id >= ED * g) & (r_id < ED * (g + 1)) & (c_id - r_id == (EP - ED) * g)
            pick = jnp.where(hit, 1.0, pick)
        pick = pick.astype(BF16)
        for g in range(8):
            yy, z0 = g // 2, 4 * (g % 2)
            pieces = jnp.concatenate([wa[(z0 + k) * NY + yy] for k in range(4)], axis=0)
            wc[pl.ds(4 * ED * g, 4 * ED), 0:WLA] = jnp.dot(pick, pieces, preferred_element_type=F32).astype(BF16)
        for half in range(2):
            project(half, 0, WLA)
    with jax.named_scope("wfar"):
        for j in range(8):
            w.far(j)

    hf_rows = [pl.ds(TOK // 2 * hf, TOK // 2) for hf in range(2)]

    def reduce_rows(val, gv, tk, sh, gt, ss, rs):
        for dx in (2, 1, 3, 0):
            xx = mod(x + dx, NX)
            gv[xx] = val[other * NX + xx].astype(gv.dtype)
            send(gv.at[xx], tk.at[xx], ss.at[0], rs.at[dx], {"c": other})
        yield
        for hf, rows in enumerate(hf_rows):
            for dx in (2, 1, 3):
                xx = mod(x + dx, NX)
                if hf == 0:
                    arrived(tk.at[xx], ss.at[0], rs.at[dx], {"c": other})
                    sh[dx - 1] = (val[c * NX + xx] + tk[xx].astype(F32)).astype(BF16)
                send(sh.at[dx - 1, rows], gt.at[dx - 1, rows], ss.at[1], rs.at[3 + 3 * hf + dx], {"x": xx})
        yield
        arrived(tk.at[x], ss.at[0], rs.at[0], {"c": other})
        for hf, rows in enumerate(hf_rows):
            total = val[me, rows] + tk[x, rows].astype(F32)
            for dx in (1, 3, 2):
                arrived(gt.at[dx - 1, rows], ss.at[1], rs.at[3 + 3 * hf + dx], {"x": mod(x - dx, NX)})
            for dx in (1, 2, 3):
                total = total + gt[dx - 1, rows].astype(F32)
            yield total
        all_sent(gv, ss.at[0], rs.at[0], {"c": other})
        all_sent(sh, ss.at[1], rs.at[4], {"x": mod(x + 1, NX)})
        yield

    def share_rows(buf, ss, rs):
        for hf, rows in enumerate(hf_rows):
            mine = buf.at[me, rows]
            for dx in (2, 1, 3):
                send(mine, mine, ss.at[0], rs.at[8 * hf + dx], {"x": mod(x + dx, NX)})
            send(mine, mine, ss.at[0], rs.at[8 * hf + 4], {"c": other})
            yield
        for hf, rows in enumerate(hf_rows):
            for dx in (1, 3, 2):
                got_at = buf.at[c * NX + mod(x - dx, NX), rows]
                arrived(got_at, ss.at[0], rs.at[8 * hf + dx], {"x": mod(x - dx, NX)})
                send(got_at, got_at, ss.at[0], rs.at[8 * hf + 4 + dx], {"c": other})
        yield
        for hf, rows in enumerate(hf_rows):
            for dx in (0, 1, 3, 2):
                at = buf.at[other * NX + mod(x - dx, NX), rows]
                arrived(at, ss.at[0], rs.at[8 * hf + 4 + dx], {"c": other})
        all_sent(buf.at[pl.ds(0, 7)], ss.at[0], rs.at[1], {"c": other})
        yield

    with jax.named_scope("compactB"):
        for g in range(8):
            yy, z0 = g // 2, 4 * (g % 2)
            pieces = wb[yy * NZ + z0 : yy * NZ + z0 + 4].reshape(4 * EP, KP - WLA)
            wc[pl.ds(4 * ED * g, 4 * ED), WLA:KP] = jnp.dot(pick, pieces, preferred_element_type=F32).astype(BF16)
    with jax.named_scope("proj1"):
        project(other, WLA, KP)
    with jax.named_scope("red1a"):
        red = reduce_rows(part, give, take, share, got, p_s, p_r)
        next(red)
    with jax.named_scope("proj2"):
        project(c, WLA, KP)
    with jax.named_scope("red1b"):
        next(red)
    with jax.named_scope("t2"):
        t.step(2)
    with jax.named_scope("red1c_norm"):
        give_img = share_rows(img, i_s, i_r)
        for hf, rows in enumerate(hf_rows):
            mixed = pooled[rows].astype(F32) + next(red)
            ln = jnp.sqrt(jnp.sum(mixed * mixed, axis=1, keepdims=True) + EPSILON)
            length[rows] = jnp.broadcast_to(ln, (TOK // 2, 128))
            un = mixed / ln
            unit[rows] = un
            img[me, rows] = un.astype(BF16)
            next(give_img)
            if hf == 0:
                t.step(3)
        next(red)
    with jax.named_scope("imgshare"):
        next(give_img)
        next(give_img)
    with jax.named_scope("t4"):
        t.step(4)
    with jax.named_scope("pairs"):
        scale = jnp.exp(jnp.broadcast_to(scale_ref[0], (8, 128)))[0:1, 0:1]
        bias = bias_ref[0]
        acc[...] = jnp.zeros_like(acc)
        loss_out[...] = jnp.zeros_like(loss_out)
        tile = NX * TOK
        t_dims = (((1,), (1,)), ((), ()))

        halves = (other, c)

        def texts(g):
            t_b = jnp.concatenate([tb[yy * NZ + g] for yy in range(NY)], axis=0)
            return ta[pl.ds(g * NY, NY)].reshape(NY * TOK, TLA), t_b

        def logits_of(g, h, out):
            t_a, t_b = texts(g)
            images = img[pl.ds(halves[h] * NX, NX)].reshape(tile, D)
            out[...] = lax.dot_general(
                images[:, :TLA], t_a, t_dims, preferred_element_type=F32
            ) + lax.dot_general(images[:, TLA:], t_b, t_dims, preferred_element_type=F32)

        def elementwise(src, out, own):
            m = scale * src[...] + bias
            if own:
                col = lax.broadcasted_iota(jnp.int32, (tile, NY * TOK), 1)
                row = lax.broadcasted_iota(jnp.int32, (tile, NY * TOK), 0)
                same = (row - col == TOK * (x - y)) & (col >= TOK * y) & (col < TOK * y + TOK)
                m = jnp.where(same, -m, m)
            e = jnp.exp(-jnp.abs(m))
            d = 1.0 + e
            r = 1.0 / d
            soft = jnp.maximum(m, 0.0) + (jnp.log(d) + (e - (d - 1.0)) * r)
            loss_out[...] += jnp.sum(soft.reshape(tile // 8, 8, NY * TOK), axis=0)
            sig = jnp.where(m >= 0.0, r, e * r)
            if own:
                sig = jnp.where(same, -sig, sig)
            out[...] = sig.astype(BF16)

        def to_images(g, h, src):
            t_a, t_b = texts(g)
            pg = src[...]
            rows = pl.ds(halves[h] * NX, NX)
            acc[rows, :, :TLA] += jnp.dot(pg, t_a, preferred_element_type=F32).reshape(NX, TOK, TLA)
            acc[rows, :, TLA:] += jnp.dot(pg, t_b, preferred_element_type=F32).reshape(NX, TOK, D - TLA)

        def group(j):
            hop = (j + 1) // 2
            return mod(z + hop * (1 - 2 * lax.rem(j, 2)), NZ)

        def body(j, carry):
            @pl.when(j == 5)
            def _():
                with jax.named_scope("p_t5"):
                    t.step(5)

            with jax.named_scope("p_far"):
                t.far_at(j)
            now, last = group(j), group(j - 1)
            logits_of(now, 0, logit_a)
            elementwise(logit_b, pg_b, False)
            to_images(last, 0, pg_a)
            logits_of(now, 1, logit_b)
            elementwise(logit_a, pg_a, False)
            to_images(last, 1, pg_b)
            return carry

        t.far_at(1)
        first, final = mod(z + OFFSETS[1], NZ), mod(z + OFFSETS[7], NZ)
        logits_of(first, 0, logit_a)
        logits_of(first, 1, logit_b)
        elementwise(logit_a, pg_a, False)
        lax.fori_loop(2, NZ, body, 0)
        t.far_at(0)
        logits_of(z, 0, logit_a)
        elementwise(logit_b, pg_b, False)
        to_images(final, 0, pg_a)
        logits_of(z, 1, logit_b)
        elementwise(logit_a, pg_a, False)
        to_images(final, 1, pg_b)
        to_images(z, 0, pg_a)
    with jax.named_scope("red2"):
        red = reduce_rows(acc, give2, take2, share2, got2, u_s, u_r)
        next(red)
        elementwise(logit_b, pg_b, True)
        to_images(z, 1, pg_b)
        next(red)
        give_mg = share_rows(mg_out, m_s, m_r)
        for rows in hf_rows:
            ug = (scale * (1.0 / BATCH)) * next(red)
            un = unit[rows]
            mg = (ug - un * jnp.sum(un * ug, axis=1, keepdims=True)) / length[rows, 0:1]
            mg_out[me, rows] = mg.astype(BF16)
            next(give_mg)
        next(red)
    with jax.named_scope("mgshare"):
        next(give_mg)

    def exchange(give_ref, take_ref, base, value, kind):
        give_ref[...] = value
        slot = EXCHANGES.index(base)
        sizes = {"row": row_peers, "y": range(1, NY), "z": range(1, NZ)}[kind]
        for i, d in enumerate(sizes):
            if kind == "row":
                device = {"x": mod(x + d[0], NX), "c": lax.rem(c + d[1], NC)}
            else:
                device = {kind: mod((y if kind == "y" else z) + d, NY if kind == "y" else NZ)}
            send(give_ref, take_ref.at[i], st_s.at[slot], st_r.at[base + i], device)

    def collected(take_ref, base, value, kind):
        slot = EXCHANGES.index(base)
        sizes = {"row": row_peers, "y": range(1, NY), "z": range(1, NZ)}[kind]
        for i, d in enumerate(sizes):
            if kind == "row":
                device = {"x": mod(x - d[0], NX), "c": lax.rem(c + d[1], NC)}
            else:
                device = {kind: mod((y if kind == "y" else z) - d, NY if kind == "y" else NZ)}
            arrived(take_ref.at[i], st_s.at[slot], st_r.at[base + i], device)
            value = value + take_ref[i]
        all_sent(take_ref, st_s.at[slot], st_r.at[base], device)
        return value

    zi = lax.broadcasted_iota(jnp.int32, (NZ, EG, 384), 0)
    ji = lax.broadcasted_iota(jnp.int32, (NZ, EG, 384), 1)
    li = lax.broadcasted_iota(jnp.int32, (NZ, EG, 384), 2)

    def product(dy, h):
        yy = mod(y + dy, NY)
        at = pl.ds(h * NX, NX)
        mg = mg_out[at, :, pl.ds(pl.multiple_of(256 * yy, 128), 384)].reshape(NX * TOK, 384)
        mg_t = lax.dot_general(choose[dy], mg, (((1,), (1,)), ((), ())), preferred_element_type=F32).astype(BF16)
        rows = h_out[at].reshape(NX * TOK, KP)
        return jnp.dot(mg_t, rows, preferred_element_type=F32).reshape(NZ, EG, KP)

    def gradient_of(dy):
        yy = mod(y + dy, NY)
        if dy == 0:
            grad[yy] = product(dy, c)
        grad[yy] += product(dy, other)
        b_give[:, B_PLACE[dy]] = grad[yy, :, :, GLA:GLB].astype(BF16)
        tail[:, :, 32 * dy : 32 * dy + 32] = grad[yy, :, :, GLB : GLB + 32]

    with jax.named_scope("g_own"):
        for dy in (2, 1, 3, 0):
            mask = (ji < ED) & (li == 32 * mod(y + dy, NY) + ED * zi + ji)
            choose[dy] = jnp.where(mask, 1.0, 0.0).reshape(NZ * EG, 384).astype(BF16)
            if dy > 0:
                grad[mod(y + dy, NY)] = product(dy, c)
    with jax.named_scope("mgwait"):
        next(give_mg)
    z_order = (4, 3, 5, 2, 6, 1, 7)
    z_near = (1, 7, 2, 6, 3, 5, 4)
    b_parts = (pl.ds(0, 2), pl.ds(2, 3))

    def give_b(k):
        for dz in z_order:
            zz = mod(z + dz, NZ)
            send(
                b_give.at[zz, b_parts[k]], b_take.at[dz - 1, b_parts[k]],
                b_s.at[0], b_r.at[7 * k + dz - 1], {"z": zz},
            )

    with jax.named_scope("loss1"):
        loss_sum = jnp.sum(jnp.sum(loss_out[...], axis=0, keepdims=True), axis=1, keepdims=True)
        loss_sum = jnp.broadcast_to(loss_sum, (1, 128))
        exchange(l_give, l_take, 34, loss_sum, "row")
    with jax.named_scope("g_far"):
        half = NZ // 2
        y_far, y_up, y_down = mod(y + 2, NY), mod(y + 1, NY), mod(y - 1, NY)
        up, down = {"y": y_up}, {"y": y_down}
        gradient_of(2)
        far_p[...] = grad[y_far, :half, :, :GLA].astype(BF16)
        far_m[...] = grad[y_far, half:, :, :GLA].astype(BF16)
        send(far_p, r_far_p, g_s.at[0], g_r.at[0], up)
        send(far_m, r_far_m, g_s.at[1], g_r.at[1], down)
    with jax.named_scope("g_rest"):
        gradient_of(1)
        near_p[...] = grad[y_up, half:, :, :GLA].astype(BF16)
        send(near_p, r_near_p, g_s.at[2], g_r.at[2], up)
        give_b(0)
        gradient_of(3)
        near_m[...] = grad[y_down, :half, :, :GLA].astype(BF16)
        send(near_m, r_near_m, g_s.at[3], g_r.at[3], down)
        gradient_of(0)
        b_give[:, NY] = tail[...].astype(BF16)
        give_b(1)
    with jax.named_scope("g_relay"):
        arrived(r_far_p, g_s.at[0], g_r.at[0], down)
        relay_p[...] = (grad[y_up, :half, :, :GLA] + r_far_p[...].astype(F32)).astype(BF16)
        send(relay_p, r_relay_p, g_s.at[4], g_r.at[4], up)
        arrived(r_far_m, g_s.at[1], g_r.at[1], up)
        relay_m[...] = (grad[y_down, half:, :, :GLA] + r_far_m[...].astype(F32)).astype(BF16)
        send(relay_m, r_relay_m, g_s.at[5], g_r.at[5], down)
    with jax.named_scope("loss2"):
        loss_sum = collected(l_take, 34, loss_sum, "row")
        exchange(sy_give, sy_take, 24, loss_sum, "y")
    with jax.named_scope("g_ysum"):
        arrived(r_near_p, g_s.at[2], g_r.at[2], down)
        arrived(r_near_m, g_s.at[3], g_r.at[3], up)
        arrived(r_relay_p, g_s.at[4], g_r.at[4], down)
        arrived(r_relay_m, g_s.at[5], g_r.at[5], up)
        grad[y, :half, :, :GLA] += r_relay_p[...].astype(F32) + r_near_m[...].astype(F32)
        grad[y, half:, :, :GLA] += r_near_p[...].astype(F32) + r_relay_m[...].astype(F32)
        z_give[...] = grad[y, :, :, :GLA].astype(z_give.dtype)
        for dz in z_order:
            zz = mod(z + dz, NZ)
            send(z_give.at[zz], z_take.at[dz - 1], z_s.at[0], z_r.at[dz - 1], {"z": zz})
    with jax.named_scope("g_bz"):
        for dy in range(NY):
            yb_give[dy, 0] = grad[mod(y + dy, NY), pl.ds(z, 1), :, GLA:GLB].reshape(EG, GLB - GLA)
        last = tail[pl.ds(z, 1)].reshape(EG, 128)
        for dz in z_near:
            for k in range(2):
                arrived(b_take.at[dz - 1, b_parts[k]], b_s.at[0], b_r.at[7 * k + dz - 1], {"z": mod(z - dz, NZ)})
        for dz in z_near:
            for dy in range(NY):
                yb_give[dy, 0] += b_take[dz - 1, B_PLACE[dy]].astype(F32)
            last = last + b_take[dz - 1, NY].astype(F32)
        for dy in range(NY):
            yb_give[dy, 1] = last
        for dy in (2, 1, 3):
            yy = mod(y + dy, NY)
            send(yb_give.at[dy], yb_take.at[dy - 1], yb_s.at[0], yb_r.at[dy - 1], {"y": yy})
    with jax.named_scope("g_by"):
        right = yb_give[0, 0]
        last = last[:, 0:32]
        for dy in (1, 3, 2):
            arrived(yb_take.at[dy - 1], yb_s.at[0], yb_r.at[dy - 1], {"y": mod(y - dy, NY)})
            right = right + yb_take[dy - 1, 0]
            last = last + yb_take[dy - 1, 1][:, 32 * dy : 32 * dy + 32]
    with jax.named_scope("loss3"):
        loss_sum = collected(sy_take, 24, loss_sum, "y")
        exchange(sz_give, sz_take, 27, loss_sum, "z")
    with jax.named_scope("g_z"):
        left = grad[y, pl.ds(z, 1), :, :GLA].reshape(EG, GLA)
        for dz in z_near:
            arrived(z_take.at[dz - 1], z_s.at[0], z_r.at[dz - 1], {"z": mod(z - dz, NZ)})
            left = left + z_take[dz - 1].astype(F32)
        grad[y, pl.ds(z, 1), :, :GLA] = left.reshape(1, EG, GLA)
        grad[y, pl.ds(z, 1), :, GLA:GLB] = right.reshape(1, EG, GLB - GLA)
        grad[y, pl.ds(z, 1), :, GLB : GLB + 32] = last.reshape(1, EG, 32)

    g = grad[y, pl.ds(z, 1)].reshape(EG, KP)
    e_id = lax.broadcasted_iota(jnp.int32, (EG, KP), 0)
    k_id = lax.broadcasted_iota(jnp.int32, (EG, KP), 1)
    squared = jnp.where((e_id < ED) & (k_id < KD), g * g + FLOOR_VALUE, 0.0)

    with jax.named_scope("st_row"):
        e_col = e_id[:, 0:128]
        l_col = k_id[:, 0:128]
        rows = jnp.broadcast_to(jnp.sum(squared, axis=1, keepdims=True), (EG, 128))
        exchange(row_give, row_take, 0, rows, "row")
        cols = jnp.sum(squared, axis=0, keepdims=True)
        rows = collected(row_take, 0, rows, "row")
        row_line = jnp.sum(jnp.where(e_col == l_col, rows, 0.0), axis=0, keepdims=True)[:, :ED]
        row_line = DECAY_RATE * row_moment[...].reshape(1, ED) + (1.0 - DECAY_RATE) * row_line / FF
        new_row = jnp.sum(
            jnp.where(
                e_id[:, :ED] == k_id[:, :ED], jnp.broadcast_to(row_line, (EG, ED)), 0.0
            ), axis=1, keepdims=True
        )
        new_row = jnp.where(e_col[:, 0:1] < ED, new_row, 1.0)
        ratio = jnp.sum(g * g / new_row, axis=0, keepdims=True)
    with jax.named_scope("st_col"):
        cols2 = jnp.concatenate([cols, ratio], axis=1)
        exchange(cy_give, cy_take, 7, cols2, "y")
        cols2 = collected(cy_take, 7, cols2, "y")
        exchange(cz_give, cz_take, 10, cols2, "z")
        cols2 = collected(cz_take, 10, cols2, "z")
    with jax.named_scope("st_tot"):
        cols, ratio = cols2[:, :KP], cols2[:, KP:]
        col_line = DECAY_RATE * col_moment[...].reshape(1, KD) + (1.0 - DECAY_RATE) * cols[:, :KD] / D
        raw_sum = jnp.sum(ratio[:, :KD] / col_line, axis=1, keepdims=True)
        exchange(s_give, s_take, 17, jnp.broadcast_to(raw_sum, (1, 128)), "row")
        raw = g[:ED, :KD] / jnp.sqrt(new_row[:ED] * col_line)
        loss_sum = collected(sz_take, 27, loss_sum, "z")
        small_out[...] = jnp.zeros_like(small_out)
        small_out[0:1, :KD] = col_line
        small_out[1:2, :ED] = row_line
        small_out[2:3, 0:128] = loss_sum * (1.0 / BATCH)
        both = collected(s_take, 17, jnp.broadcast_to(raw_sum, (1, 128)), "row")
    with jax.named_scope("upd"):
        rms = jnp.sqrt(both[:, 0:1] / (D * FF))
        update_out[...] = raw / jnp.maximum(1.0, rms / CLIP_LEVEL)
    with jax.named_scope("finish"):
        w.finish()
        t.finish()
        all_sent(h_out.at[pl.ds(0, 7)], h_s.at[0], h_r.at[0], {"c": other})
        for k, (ref, device) in enumerate(
            ((far_p, up), (far_m, down), (near_p, up), (near_m, down), (relay_p, up), (relay_m, down))
        ):
            all_sent(ref, g_s.at[k], g_r.at[k], device)
        all_sent(z_take, z_s.at[0], z_r.at[0], {"z": mod(z + 1, NZ)})
        all_sent(b_take, b_s.at[0], b_r.at[0], {"z": mod(z + 1, NZ)})
        all_sent(yb_take, yb_s.at[0], yb_r.at[0], up)


def step_kernel(hidden, weight, text, pooled, row_moment, col_moment, scale, bias):
    vmem = pl.BlockSpec(memory_space=pltpu.VMEM)
    smem = pl.BlockSpec(memory_space=pltpu.SMEM)
    n_row = NX * NC
    dma = pltpu.SemaphoreType.DMA
    return pl.pallas_call(
        whole_kernel,
        out_shape=(
            jax.ShapeDtypeStruct((ED, KD), F32),
            jax.ShapeDtypeStruct((8, KP), F32),
        ),
        in_specs=[pl.BlockSpec(memory_space=pl.ANY)] * 6 + [smem] * 2,
        out_specs=(vmem,) * 2,
        scratch_shapes=[
            pltpu.VMEM((TOK, FF), BF16),
            pltpu.VMEM((ED, KD), F32),
            pltpu.VMEM((TOK, D), BF16),
            pltpu.VMEM((TOK, D), BF16),
            pltpu.VMEM((ED,), F32),
            pltpu.VMEM((KD,), F32),
            dma((6,)),
            pltpu.VMEM((n_row, TOK, KP), BF16),
            pltpu.VMEM((EP, KP), BF16),
            pltpu.VMEM((NX * TOK, NY * TOK), F32),
            pltpu.VMEM((NX * TOK, NY * TOK), F32),
            pltpu.VMEM((NX * TOK, NY * TOK), BF16),
            pltpu.VMEM((NX * TOK, NY * TOK), BF16),
            pltpu.VMEM((n_row, TOK, KP), BF16),
            pltpu.VMEM((n_row, TOK, D), BF16),
            pltpu.VMEM((8, NY * TOK), F32),
            pltpu.VMEM((NZ * NY, EP, WLA), BF16),
            pltpu.VMEM((NY * NZ, EP, KP - WLA), BF16),
            pltpu.VMEM((D, KP), BF16),
            pltpu.VMEM((NZ * NY, TOK, TLA), BF16),
            pltpu.VMEM((NY * NZ, TOK, D - TLA), BF16),
            pltpu.VMEM((TOK, D), BF16),
            pltpu.VMEM((n_row, TOK, D), F32),
            pltpu.VMEM((NX, TOK, D), F32),
            pltpu.VMEM((NX, TOK, D), F32),
            pltpu.VMEM((NX - 1, TOK, D), BF16),
            pltpu.VMEM((NX - 1, TOK, D), BF16),
            pltpu.VMEM((n_row, TOK, D), BF16),
            pltpu.VMEM((TOK, D), F32),
            pltpu.VMEM((TOK, 128), F32),
            pltpu.VMEM((n_row, TOK, D), F32),
            pltpu.VMEM((NX, TOK, D), BF16),
            pltpu.VMEM((NX, TOK, D), BF16),
            pltpu.VMEM((NX - 1, TOK, D), BF16),
            pltpu.VMEM((NX - 1, TOK, D), BF16),
            pltpu.VMEM((NY, NZ, EG, KP), F32),
            *[pltpu.VMEM((NZ // 2, EG, GLA), BF16)] * 12,
            pltpu.VMEM((NZ, EG, GLA), BF16),
            pltpu.VMEM((NZ - 1, EG, GLA), BF16),
            pltpu.VMEM((NY, NZ * EG, 384), BF16),
            pltpu.VMEM((NZ, EG, 128), F32),
            pltpu.VMEM((NZ, NY + 1, EG, 128), BF16),
            pltpu.VMEM((NZ - 1, NY + 1, EG, 128), BF16),
            pltpu.VMEM((NY, 2, EG, 128), F32),
            pltpu.VMEM((NY - 1, 2, EG, 128), F32),
            pltpu.VMEM((EG, 128), F32),
            pltpu.VMEM((n_row - 1, EG, 128), F32),
            pltpu.VMEM((1, 2 * KP), F32),
            pltpu.VMEM((NY - 1, 1, 2 * KP), F32),
            pltpu.VMEM((1, 2 * KP), F32),
            pltpu.VMEM((NZ - 1, 1, 2 * KP), F32),
            pltpu.VMEM((1, 128), F32),
            pltpu.VMEM((n_row - 1, 1, 128), F32),
            pltpu.VMEM((1, 128), F32),
            pltpu.VMEM((n_row - 1, 1, 128), F32),
            pltpu.VMEM((1, 128), F32),
            pltpu.VMEM((NY - 1, 1, 128), F32),
            pltpu.VMEM((1, 128), F32),
            pltpu.VMEM((NZ - 1, 1, 128), F32),
            dma((2,)), dma((N_MSG,)), dma((2,)), dma((N_MSG,)),
            dma((1,)), dma((7,)), dma((2,)), dma((10,)), dma((1,)), dma((16,)),
            dma((2,)), dma((10,)), dma((1,)), dma((16,)),
            dma((6,)), dma((6,)), dma((1,)), dma((7,)), dma((1,)), dma((14,)),
            dma((1,)), dma((3,)), dma((7,)), dma((41,)),
        ],
        compiler_params=pltpu.CompilerParams(
            collective_id=0, has_side_effects=True, vmem_limit_bytes=60 * 1024 * 1024
        ),
        name="step",
    )(hidden, weight, text, pooled, row_moment, col_moment, scale, bias)


def out_kernel(update_in, small, update, new_row, new_col, loss):
    update[...] = update_in[...]
    new_row[...] = small[1:2, :ED].reshape(ED)
    new_col[...] = small[0:1, :KD].reshape(KD)
    loss[0] = small[2, 0]


def per_device(pooled, hidden, text, weight, row_moment, col_moment, log_scale, bias):
    update, small = step_kernel(
        hidden, weight, text, pooled, row_moment, col_moment, log_scale.reshape(1), bias.reshape(1)
    )
    vmem = pl.BlockSpec(memory_space=pltpu.VMEM)
    update, new_row, new_col, loss = pl.pallas_call(
        out_kernel,
        out_shape=(
            jax.ShapeDtypeStruct((ED, KD), F32),
            jax.ShapeDtypeStruct((ED,), F32),
            jax.ShapeDtypeStruct((KD,), F32),
            jax.ShapeDtypeStruct((1,), F32),
        ),
        in_specs=[vmem] * 2,
        out_specs=(vmem, vmem, vmem, pl.BlockSpec(memory_space=pltpu.SMEM)),
        name="out",
    )(update, small)
    return (update, new_row, new_col, loss.reshape(()))


def solution(mesh):
    finer = Mesh(mesh.devices.reshape(NX, NC, NY, NZ), ALL)
    return jax.shard_map(
        per_device,
        mesh=finer,
        in_specs=(
            P(ALL, None), P(ALL, None), P(ALL, None), P(COL, ROW), P(COL), P(ROW), P(), P(),
        ),
        out_specs=(P(COL, ROW), P(COL), P(ROW), P()),
        check_vma=False,
    )
```

```python
import functools

import jax
import jax.numpy as jnp
from jax import lax
from jax.experimental import pallas as pl
from jax.experimental.pallas import tpu as pltpu
from jax.sharding import Mesh
from jax.sharding import PartitionSpec as P

D = 1152
FF = 4304
NX, NC, NY, NZ = 4, 2, 4, 8
TOK = 64
KD = FF // (NX * NC)
KP = 640
ED = D // (NY * NZ)
EP = 48
WLA = 256
TLA = 512
EG = 40
GLA = 384
GLB = 512
ROW = ("x", "c")
COL = ("y", "z")
ALL = ("x", "c", "y", "z")
BATCH = TOK * NX * NC * NY * NZ

EPSILON = 1e-06
DECAY_RATE = 0.8
CLIP_LEVEL = 1.0
FLOOR_VALUE = 1e-30

MESH = pl.DeviceIdType.MESH
F32 = jnp.float32
BF16 = jnp.bfloat16


def mod(value, size):
    return lax.rem(value + 2 * size, size)


def send(src, dst, ssem, rsem, device):
    pltpu.make_async_remote_copy(src, dst, ssem, rsem, device_id=device, device_id_type=MESH).start()


def arrived(dst, ssem, rsem, device):
    pltpu.make_async_remote_copy(dst, dst, ssem, rsem, device_id=device, device_id_type=MESH).wait_recv()


def all_sent(ref, ssem, rsem, device):
    pltpu.make_async_remote_copy(ref, ref, ssem, rsem, device_id=device, device_id_type=MESH).wait_send()


A0, AP, AM, BP, BM, YP, YM, Y2 = 0, 3, 17, 33, 37, 40, 48, 56
N_MSG = 64
B_PLACE = (3, 1, 0, 2)
EXCHANGES = (0, 7, 10, 17, 24, 27, 34)
A_MSG = range(A0, BP)
OFFSETS = [0, -1, 1, -2, 2, -3, 3, -4]


class PlaneGather:
    def __init__(self, piece, a, b, la, rows, late, ssem, rsem, y, z):
        self.late = late
        self.piece, self.a, self.b, self.la, self.rows = piece, a, b, la, pl.ds(0, rows)
        self.piece_a = piece.at[self.rows, pl.ds(0, la)]
        self.piece_b = piece.at[self.rows, pl.ds(la, piece.shape[1] - la)]
        self.ssem, self.rsem, self.y, self.z = ssem, rsem, y, z
        self.ys = {o: mod(y + o, NY) for o in range(1 - NY, NY)}
        self.zs = {o: mod(z + o, NZ) for o in range(-(NZ // 2), NZ // 2 + 1)}
        self.sems = [(ssem.at[0 if i in A_MSG else 1], rsem.at[i]) for i in range(N_MSG)]
        self.a_at = {(o, dy): a.at[self.zs[o] * NY + self.ys[-dy], self.rows] for o in self.zs for dy in range(NY)}
        self.b_at = {(yo, o): b.at[self.ys[yo] * NZ + self.zs[o], self.rows] for o in self.zs for yo in range(-2, 3)}

    def _send(self, src, dst, i, device):
        send(src, dst, *self.sems[i], device)

    def _wait(self, dst, i, device):
        sems = self.sems[i] if isinstance(i, int) else (self.ssem.at[1], self.rsem.at[i])
        arrived(dst, *sems, device)

    def own(self):
        self.a[self.z * NY + self.y] = self.piece[:, : self.la]
        self.b[self.y * NZ + self.z] = self.piece[:, self.la :]

    def finish(self):
        n = pl.ds(0, NY * NZ - 1)
        all_sent(self.a.at[n, self.rows], *self.sems[A0], self._zdev(1))
        all_sent(self.b.at[n, self.rows], *self.sems[BP], self._zdev(1))

    def _a(self, zo, dy):
        return self.a_at[zo, dy]

    def _b(self, yo, zo):
        return self.b_at[yo, zo]

    def _zdev(self, o):
        return {"z": self.zs[o]}

    def _ydev(self, o):
        return {"y": self.ys[o]}

    @staticmethod
    def _has(sign, s, dy):
        if s < NZ // 2:
            return s >= 1
        return s == NZ // 2 and (dy < NY // 2) == (sign > 0)

    def _ring_a(self, s, dy, sign):
        if not self._has(sign, s, dy):
            return
        src = self._a(-sign * (s - 1), dy)
        dst = src
        if s == 1 and dy == 0:
            src = self.piece_a
        self._send(src, dst, (AP if sign > 0 else AM) + (s - 1) * 4 + dy, self._zdev(sign))

    def _ring_b(self, s, sign):
        if s > (NZ // 2 if sign > 0 else NZ // 2 - 1):
            return
        dst = self._b(0, -sign * (s - 1))
        src = self.piece_b if s == 1 else dst
        self._send(src, dst, (BP if sign > 0 else BM) + s - 1, self._zdev(sign))

    def _spread_b(self, j):
        dst = self._b(0, OFFSETS[j])
        src = self.piece_b if j == 0 else dst
        self._send(src, dst, YP + j, self._ydev(1))
        self._send(src, dst, YM + j, self._ydev(-1))

    def _near_b(self, j):
        o = OFFSETS[j]
        self._wait(self._b(-1, o), YP + j, self._ydev(-1))
        if j % 2 == 0:
            self._send(self._b(-1, o), self._b(-1, o), Y2 + j, self._ydev(1))
        self._wait(self._b(1, o), YM + j, self._ydev(1))
        if j % 2 == 1:
            self._send(self._b(1, o), self._b(1, o), Y2 + j, self._ydev(-1))

    def far(self, j):
        o = OFFSETS[j]
        yo = -2 if j % 2 == 0 else 2
        self._wait(self._b(yo, o), Y2 + j, self._ydev(-1 if j % 2 == 0 else 1))

    def far_at(self, j):
        if isinstance(j, int):
            return self.far(j)
        hop = (j + 1) // 2
        zz = mod(self.z + hop * (1 - 2 * lax.rem(j, 2)), NZ)
        self._wait(self.b.at[self.ys[2] * NZ + zz, self.rows], Y2 + j, self._ydev(1))

    def start(self):
        for dy in range(1, NY):
            self._send(self.piece_a, self._a(0, 0), A0 + dy - 1, self._ydev(dy))
        for sign in (1, -1):
            self._ring_b(1, sign)
            self._ring_a(1, 0, sign)
        if not self.late:
            self._spread_b(0)

    def step(self, k):
        if self.late and k == 1:
            self._spread_b(0)
        for s_sign in (1, -1):
            if k <= (NZ // 2 if s_sign > 0 else NZ // 2 - 1):
                self._wait(self._b(0, -s_sign * k), (BP if s_sign > 0 else BM) + k - 1, self._zdev(-s_sign))
                self._ring_b(k + 1, s_sign)
                self._spread_b(OFFSETS.index(-s_sign * k))
        for dy in range(NY):
            if k == 1:
                if dy == 0:
                    continue
                self._wait(self._a(0, dy), A0 + dy - 1, self._ydev(-dy))
                self._ring_a(1, dy, 1)
                self._ring_a(1, dy, -1)
                continue
            s = k - 1
            for sign in (1, -1):
                if self._has(sign, s, dy):
                    self._wait(
                        self._a(-sign * s, dy), (AP if sign > 0 else AM) + (s - 1) * 4 + dy, self._zdev(-sign)
                    )
                    self._ring_a(s + 1, dy, sign)
        for j, o in enumerate(OFFSETS):
            if abs(o) == k - 1 and (j > 0 or not self.late) or (j == 0 and self.late and k == 2):
                self._near_b(j)


def whole_kernel(
    hidden_in, weight_in, text_in, pooled_in, row_in, col_in, scale_ref, bias_ref,
    update_out, small_out,
    hidden, weight, text, pooled, row_moment, col_moment, in_s,
    hid, wp, logit_a, logit_b, pg_a, pg_b,
    h_out, mg_out, loss_out,
    wa, wb, wc, ta, tb, tn, part, give, take, share, got, img, unit, length,
    acc, give2, take2, share2, got2,
    grad, far_p, far_m, near_p, near_m, relay_p, relay_m,
    r_far_p, r_far_m, r_near_p, r_near_m, r_relay_p, r_relay_m,
    z_give, z_take, choose, tail, b_give, b_take, yb_give, yb_take,
    row_give, row_take, cy_give, cy_take, cz_give, cz_take,
    s_give, s_take, l_give, l_take, sy_give, sy_take, sz_give, sz_take,
    w_s, w_r, t_s, t_r, h_s, h_r, p_s, p_r, i_s, i_r, u_s, u_r, m_s, m_r,
    g_s, g_r, z_s, z_r, b_s, b_r, yb_s, yb_r, st_s, st_r,
):
    x, c = lax.axis_index("x"), lax.axis_index("c")
    y, z = lax.axis_index("y"), lax.axis_index("z")
    me = c * NX + x
    other = 1 - c

    loads = [
        pltpu.make_async_copy(src, dst, in_s.at[i])
        for i, (src, dst) in enumerate(
            (
                (weight_in, weight), (hidden_in, hidden), (text_in, text), (pooled_in, pooled),
                (row_in, row_moment), (col_in, col_moment),
            )
        )
    ]
    for load in loads:
        load.start()
    wa[...] = jnp.zeros_like(wa)
    wb[...] = jnp.zeros_like(wb)
    with jax.named_scope("signal"):
        barrier = pltpu.get_barrier_semaphore()
        peers = [{"z": mod(z + dz, NZ)} for dz in range(1, NZ)]
        peers += [{"y": mod(y + dy, NY)} for dy in range(1, NY)]
        peers += [
            {"x": mod(x + dx, NX), "c": lax.rem(c + dc, NC)}
            for dx in range(NX) for dc in range(NC) if dx + dc > 0
        ]
        for peer in peers:
            pl.semaphore_signal(barrier, inc=1, device_id=peer, device_id_type=MESH)

    with jax.named_scope("prep"):
        for load in loads:
            load.wait()
        wp[...] = jnp.zeros_like(wp)
        wp[:ED, :KD] = weight[...].astype(BF16)
        hid[...] = jnp.zeros_like(hid)
        for r in range(NX * NC):
            hid[(r % NC) * NX + r // NC, :, :KD] = hidden[:, KD * r : KD * (r + 1)]
    with jax.named_scope("barrier"):
        pl.semaphore_wait(barrier, len(peers))
    w = PlaneGather(wp, wa, wb, WLA, EG, False, w_s, w_r, y, z)
    t = PlaneGather(tn, ta, tb, TLA, TOK, True, t_s, t_r, y, z)

    def project(half, k0, k1):
        rows = h_out[pl.ds(half * NX, NX), :, k0:k1].reshape(NX * TOK, k1 - k0)
        for n in range(3):
            lanes = slice(384 * n, 384 * (n + 1))
            product = lax.dot_general(
                rows, wc[lanes, k0:k1], (((1,), (1,)), ((), ())), preferred_element_type=F32
            ).reshape(NX, TOK, 384)
            at = pl.ds(half * NX, NX)
            part[at, :, lanes] = product if k0 == 0 else part[at, :, lanes] + product

    with jax.named_scope("wstart"):
        w.start()
        row_peers = [(dx, dc) for dx in range(NX) for dc in range(NC) if dx + dc > 0]
        for i, (dx, dc) in enumerate(row_peers):
            xx, cc = mod(x + dx, NX), lax.rem(c + dc, NC)
            send(hid.at[cc * NX + xx], h_out.at[me], h_s.at[0], h_r.at[i], {"x": xx, "c": cc})
        h_out[me] = hid[me]
        w.own()
        tf = text[...].astype(F32)
        tn[...] = (tf / jnp.sqrt(jnp.sum(tf * tf, axis=1, keepdims=True) + EPSILON)).astype(BF16)
    with jax.named_scope("w123"):
        w.step(1)
        w.step(2)
        w.step(3)
    with jax.named_scope("tstart"):
        t.own()
        t.start()
    with jax.named_scope("w45far"):
        w.step(4)
        w.step(5)
    with jax.named_scope("t1"):
        t.step(1)
    with jax.named_scope("hwait"):
        for i, (dx, dc) in enumerate(row_peers):
            xx, cc = mod(x - dx, NX), lax.rem(c + dc, NC)
            arrived(h_out.at[cc * NX + xx], h_s.at[0], h_r.at[i], {"x": xx, "c": cc})

    with jax.named_scope("compactA"):
        r_id = lax.broadcasted_iota(jnp.int32, (4 * ED, 4 * EP), 0)
        c_id = lax.broadcasted_iota(jnp.int32, (4 * ED, 4 * EP), 1)
        pick = jnp.zeros((4 * ED, 4 * EP), F32)
        for g in range(4):
            hit = (r_id >= ED * g) & (r_id < ED * (g + 1)) & (c_id - r_id == (EP - ED) * g)
            pick = jnp.where(hit, 1.0, pick)
        pick = pick.astype(BF16)
        for g in range(8):
            yy, z0 = g // 2, 4 * (g % 2)
            pieces = jnp.concatenate([wa[(z0 + k) * NY + yy] for k in range(4)], axis=0)
            wc[pl.ds(4 * ED * g, 4 * ED), 0:WLA] = jnp.dot(pick, pieces, preferred_element_type=F32).astype(BF16)
        for half in range(2):
            project(half, 0, WLA)
    with jax.named_scope("wfar"):
        for j in range(8):
            w.far(j)

    hf_rows = [pl.ds(TOK // 2 * hf, TOK // 2) for hf in range(2)]

    def reduce_rows(val, gv, tk, sh, gt, ss, rs):
        for dx in (2, 1, 3, 0):
            xx = mod(x + dx, NX)
            gv[xx] = val[other * NX + xx].astype(gv.dtype)
            send(gv.at[xx], tk.at[xx], ss.at[0], rs.at[dx], {"c": other})
        yield
        for hf, rows in enumerate(hf_rows):
            for dx in (2, 1, 3):
                xx = mod(x + dx, NX)
                if hf == 0:
                    arrived(tk.at[xx], ss.at[0], rs.at[dx], {"c": other})
                    sh[dx - 1] = (val[c * NX + xx] + tk[xx].astype(F32)).astype(BF16)
                send(sh.at[dx - 1, rows], gt.at[dx - 1, rows], ss.at[1], rs.at[3 + 3 * hf + dx], {"x": xx})
        yield
        arrived(tk.at[x], ss.at[0], rs.at[0], {"c": other})
        for hf, rows in enumerate(hf_rows):
            total = val[me, rows] + tk[x, rows].astype(F32)
            for dx in (1, 3, 2):
                arrived(gt.at[dx - 1, rows], ss.at[1], rs.at[3 + 3 * hf + dx], {"x": mod(x - dx, NX)})
            for dx in (1, 2, 3):
                total = total + gt[dx - 1, rows].astype(F32)
            yield total
        all_sent(gv, ss.at[0], rs.at[0], {"c": other})
        all_sent(sh, ss.at[1], rs.at[4], {"x": mod(x + 1, NX)})
        yield

    def share_rows(buf, ss, rs):
        for hf, rows in enumerate(hf_rows):
            mine = buf.at[me, rows]
            for dx in (2, 1, 3):
                send(mine, mine, ss.at[0], rs.at[8 * hf + dx], {"x": mod(x + dx, NX)})
            send(mine, mine, ss.at[0], rs.at[8 * hf + 4], {"c": other})
            yield
        for hf, rows in enumerate(hf_rows):
            for dx in (1, 3, 2):
                got_at = buf.at[c * NX + mod(x - dx, NX), rows]
                arrived(got_at, ss.at[0], rs.at[8 * hf + dx], {"x": mod(x - dx, NX)})
                send(got_at, got_at, ss.at[0], rs.at[8 * hf + 4 + dx], {"c": other})
        yield
        for hf, rows in enumerate(hf_rows):
            for dx in (0, 1, 3, 2):
                at = buf.at[other * NX + mod(x - dx, NX), rows]
                arrived(at, ss.at[0], rs.at[8 * hf + 4 + dx], {"c": other})
        all_sent(buf.at[pl.ds(0, 7)], ss.at[0], rs.at[1], {"c": other})
        yield

    with jax.named_scope("compactB"):
        for g in range(8):
            yy, z0 = g // 2, 4 * (g % 2)
            pieces = wb[yy * NZ + z0 : yy * NZ + z0 + 4].reshape(4 * EP, KP - WLA)
            wc[pl.ds(4 * ED * g, 4 * ED), WLA:KP] = jnp.dot(pick, pieces, preferred_element_type=F32).astype(BF16)
    with jax.named_scope("proj1"):
        project(other, WLA, KP)
    with jax.named_scope("red1a"):
        red = reduce_rows(part, give, take, share, got, p_s, p_r)
        next(red)
    with jax.named_scope("proj2"):
        project(c, WLA, KP)
    with jax.named_scope("red1b"):
        next(red)
    with jax.named_scope("t2"):
        t.step(2)
    with jax.named_scope("red1c_norm"):
        give_img = share_rows(img, i_s, i_r)
        for hf, rows in enumerate(hf_rows):
            mixed = pooled[rows].astype(F32) + next(red)
            ln = jnp.sqrt(jnp.sum(mixed * mixed, axis=1, keepdims=True) + EPSILON)
            length[rows] = jnp.broadcast_to(ln, (TOK // 2, 128))
            un = mixed / ln
            unit[rows] = un
            img[me, rows] = un.astype(BF16)
            next(give_img)
            if hf == 0:
                t.step(3)
        next(red)
    with jax.named_scope("imgshare"):
        next(give_img)
        next(give_img)
    with jax.named_scope("t4"):
        t.step(4)
    with jax.named_scope("pairs"):
        scale = jnp.exp(jnp.broadcast_to(scale_ref[0], (8, 128)))[0:1, 0:1]
        bias = bias_ref[0]
        acc[...] = jnp.zeros_like(acc)
        loss_out[...] = jnp.zeros_like(loss_out)
        tile = NX * TOK
        t_dims = (((1,), (1,)), ((), ()))

        halves = (other, c)

        def texts(g):
            t_b = jnp.concatenate([tb[yy * NZ + g] for yy in range(NY)], axis=0)
            return ta[pl.ds(g * NY, NY)].reshape(NY * TOK, TLA), t_b

        def logits_of(g, h, out):
            t_a, t_b = texts(g)
            images = img[pl.ds(halves[h] * NX, NX)].reshape(tile, D)
            out[...] = lax.dot_general(
                images[:, :TLA], t_a, t_dims, preferred_element_type=F32
            ) + lax.dot_general(images[:, TLA:], t_b, t_dims, preferred_element_type=F32)

        def elementwise(src, out, own):
            m = scale * src[...] + bias
            if own:
                col = lax.broadcasted_iota(jnp.int32, (tile, NY * TOK), 1)
                row = lax.broadcasted_iota(jnp.int32, (tile, NY * TOK), 0)
                same = (row - col == TOK * (x - y)) & (col >= TOK * y) & (col < TOK * y + TOK)
                m = jnp.where(same, -m, m)
            e = jnp.exp(-jnp.abs(m))
            d = 1.0 + e
            r = 1.0 / d
            soft = jnp.maximum(m, 0.0) + (jnp.log(d) + (e - (d - 1.0)) * r)
            loss_out[...] += jnp.sum(soft.reshape(tile // 8, 8, NY * TOK), axis=0)
            sig = jnp.where(m >= 0.0, r, e * r)
            if own:
                sig = jnp.where(same, -sig, sig)
            out[...] = sig.astype(BF16)

        def to_images(g, h, src):
            t_a, t_b = texts(g)
            pg = src[...]
            rows = pl.ds(halves[h] * NX, NX)
            acc[rows, :, :TLA] += jnp.dot(pg, t_a, preferred_element_type=F32).reshape(NX, TOK, TLA)
            acc[rows, :, TLA:] += jnp.dot(pg, t_b, preferred_element_type=F32).reshape(NX, TOK, D - TLA)

        def group(j):
            hop = (j + 1) // 2
            return mod(z + hop * (1 - 2 * lax.rem(j, 2)), NZ)

        def body(j, carry):
            @pl.when(j == 5)
            def _():
                with jax.named_scope("p_t5"):
                    t.step(5)

            with jax.named_scope("p_far"):
                t.far_at(j)
            now, last = group(j), group(j - 1)
            logits_of(now, 0, logit_a)
            elementwise(logit_b, pg_b, False)
            to_images(last, 0, pg_a)
            logits_of(now, 1, logit_b)
            elementwise(logit_a, pg_a, False)
            to_images(last, 1, pg_b)
            return carry

        t.far_at(1)
        first, final = mod(z + OFFSETS[1], NZ), mod(z + OFFSETS[7], NZ)
        logits_of(first, 0, logit_a)
        logits_of(first, 1, logit_b)
        elementwise(logit_a, pg_a, False)
        lax.fori_loop(2, NZ, body, 0)
        t.far_at(0)
        logits_of(z, 0, logit_a)
        elementwise(logit_b, pg_b, False)
        to_images(final, 0, pg_a)
        logits_of(z, 1, logit_b)
        elementwise(logit_a, pg_a, False)
        to_images(final, 1, pg_b)
        to_images(z, 0, pg_a)
    with jax.named_scope("red2"):
        red = reduce_rows(acc, give2, take2, share2, got2, u_s, u_r)
        next(red)
        elementwise(logit_b, pg_b, True)
        to_images(z, 1, pg_b)
        next(red)
        give_mg = share_rows(mg_out, m_s, m_r)
        for rows in hf_rows:
            ug = (scale * (1.0 / BATCH)) * next(red)
            un = unit[rows]
            mg = (ug - un * jnp.sum(un * ug, axis=1, keepdims=True)) / length[rows, 0:1]
            mg_out[me, rows] = mg.astype(BF16)
            next(give_mg)
        next(red)
    with jax.named_scope("mgshare"):
        next(give_mg)

    def exchange(give_ref, take_ref, base, value, kind):
        give_ref[...] = value
        slot = EXCHANGES.index(base)
        sizes = {"row": row_peers, "y": range(1, NY), "z": range(1, NZ)}[kind]
        for i, d in enumerate(sizes):
            if kind == "row":
                device = {"x": mod(x + d[0], NX), "c": lax.rem(c + d[1], NC)}
            else:
                device = {kind: mod((y if kind == "y" else z) + d, NY if kind == "y" else NZ)}
            send(give_ref, take_ref.at[i], st_s.at[slot], st_r.at[base + i], device)

    def collected(take_ref, base, value, kind):
        slot = EXCHANGES.index(base)
        sizes = {"row": row_peers, "y": range(1, NY), "z": range(1, NZ)}[kind]
        for i, d in enumerate(sizes):
            if kind == "row":
                device = {"x": mod(x - d[0], NX), "c": lax.rem(c + d[1], NC)}
            else:
                device = {kind: mod((y if kind == "y" else z) - d, NY if kind == "y" else NZ)}
            arrived(take_ref.at[i], st_s.at[slot], st_r.at[base + i], device)
            value = value + take_ref[i]
        all_sent(take_ref, st_s.at[slot], st_r.at[base], device)
        return value

    zi = lax.broadcasted_iota(jnp.int32, (NZ, EG, 384), 0)
    ji = lax.broadcasted_iota(jnp.int32, (NZ, EG, 384), 1)
    li = lax.broadcasted_iota(jnp.int32, (NZ, EG, 384), 2)

    def product(dy, h):
        yy = mod(y + dy, NY)
        at = pl.ds(h * NX, NX)
        mg = mg_out[at, :, pl.ds(pl.multiple_of(256 * yy, 128), 384)].reshape(NX * TOK, 384)
        mg_t = lax.dot_general(choose[dy], mg, (((1,), (1,)), ((), ())), preferred_element_type=F32).astype(BF16)
        rows = h_out[at].reshape(NX * TOK, KP)
        return jnp.dot(mg_t, rows, preferred_element_type=F32).reshape(NZ, EG, KP)

    def gradient_of(dy):
        yy = mod(y + dy, NY)
        if dy == 0:
            grad[yy] = product(dy, c)
        grad[yy] += product(dy, other)
        b_give[:, B_PLACE[dy]] = grad[yy, :, :, GLA:GLB].astype(BF16)
        tail[:, :, 32 * dy : 32 * dy + 32] = grad[yy, :, :, GLB : GLB + 32]

    with jax.named_scope("g_own"):
        for dy in (2, 1, 3, 0):
            mask = (ji < ED) & (li == 32 * mod(y + dy, NY) + ED * zi + ji)
            choose[dy] = jnp.where(mask, 1.0, 0.0).reshape(NZ * EG, 384).astype(BF16)
            if dy > 0:
                grad[mod(y + dy, NY)] = product(dy, c)
    with jax.named_scope("mgwait"):
        next(give_mg)
    z_order = (4, 3, 5, 2, 6, 1, 7)
    z_near = (1, 7, 2, 6, 3, 5, 4)
    b_parts = (pl.ds(0, 2), pl.ds(2, 3))

    def give_b(k):
        for dz in z_order:
            zz = mod(z + dz, NZ)
            send(
                b_give.at[zz, b_parts[k]], b_take.at[dz - 1, b_parts[k]],
                b_s.at[0], b_r.at[7 * k + dz - 1], {"z": zz},
            )

    with jax.named_scope("loss1"):
        loss_sum = jnp.sum(jnp.sum(loss_out[...], axis=0, keepdims=True), axis=1, keepdims=True)
        loss_sum = jnp.broadcast_to(loss_sum, (1, 128))
        exchange(l_give, l_take, 34, loss_sum, "row")
    with jax.named_scope("g_far"):
        half = NZ // 2
        y_far, y_up, y_down = mod(y + 2, NY), mod(y + 1, NY), mod(y - 1, NY)
        up, down = {"y": y_up}, {"y": y_down}
        gradient_of(2)
        far_p[...] = grad[y_far, :half, :, :GLA].astype(BF16)
        far_m[...] = grad[y_far, half:, :, :GLA].astype(BF16)
        send(far_p, r_far_p, g_s.at[0], g_r.at[0], up)
        send(far_m, r_far_m, g_s.at[1], g_r.at[1], down)
    with jax.named_scope("g_rest"):
        gradient_of(1)
        near_p[...] = grad[y_up, half:, :, :GLA].astype(BF16)
        send(near_p, r_near_p, g_s.at[2], g_r.at[2], up)
        give_b(0)
        gradient_of(3)
        near_m[...] = grad[y_down, :half, :, :GLA].astype(BF16)
        send(near_m, r_near_m, g_s.at[3], g_r.at[3], down)
        gradient_of(0)
        b_give[:, NY] = tail[...].astype(BF16)
        give_b(1)
    with jax.named_scope("g_relay"):
        arrived(r_far_p, g_s.at[0], g_r.at[0], down)
        relay_p[...] = (grad[y_up, :half, :, :GLA] + r_far_p[...].astype(F32)).astype(BF16)
        send(relay_p, r_relay_p, g_s.at[4], g_r.at[4], up)
        arrived(r_far_m, g_s.at[1], g_r.at[1], up)
        relay_m[...] = (grad[y_down, half:, :, :GLA] + r_far_m[...].astype(F32)).astype(BF16)
        send(relay_m, r_relay_m, g_s.at[5], g_r.at[5], down)
    with jax.named_scope("loss2"):
        loss_sum = collected(l_take, 34, loss_sum, "row")
        exchange(sy_give, sy_take, 24, loss_sum, "y")
    with jax.named_scope("g_ysum"):
        arrived(r_near_p, g_s.at[2], g_r.at[2], down)
        arrived(r_near_m, g_s.at[3], g_r.at[3], up)
        arrived(r_relay_p, g_s.at[4], g_r.at[4], down)
        arrived(r_relay_m, g_s.at[5], g_r.at[5], up)
        grad[y, :half, :, :GLA] += r_relay_p[...].astype(F32) + r_near_m[...].astype(F32)
        grad[y, half:, :, :GLA] += r_near_p[...].astype(F32) + r_relay_m[...].astype(F32)
        z_give[...] = grad[y, :, :, :GLA].astype(z_give.dtype)
        for dz in z_order:
            zz = mod(z + dz, NZ)
            send(z_give.at[zz], z_take.at[dz - 1], z_s.at[0], z_r.at[dz - 1], {"z": zz})
    with jax.named_scope("g_bz"):
        for dy in range(NY):
            yb_give[dy, 0] = grad[mod(y + dy, NY), pl.ds(z, 1), :, GLA:GLB].reshape(EG, GLB - GLA)
        last = tail[pl.ds(z, 1)].reshape(EG, 128)
        for dz in z_near:
            for k in range(2):
                arrived(b_take.at[dz - 1, b_parts[k]], b_s.at[0], b_r.at[7 * k + dz - 1], {"z": mod(z - dz, NZ)})
        for dz in z_near:
            for dy in range(NY):
                yb_give[dy, 0] += b_take[dz - 1, B_PLACE[dy]].astype(F32)
            last = last + b_take[dz - 1, NY].astype(F32)
        for dy in range(NY):
            yb_give[dy, 1] = last
        for dy in (2, 1, 3):
            yy = mod(y + dy, NY)
            send(yb_give.at[dy], yb_take.at[dy - 1], yb_s.at[0], yb_r.at[dy - 1], {"y": yy})
    with jax.named_scope("g_by"):
        right = yb_give[0, 0]
        last = last[:, 0:32]
        for dy in (1, 3, 2):
            arrived(yb_take.at[dy - 1], yb_s.at[0], yb_r.at[dy - 1], {"y": mod(y - dy, NY)})
            right = right + yb_take[dy - 1, 0]
            last = last + yb_take[dy - 1, 1][:, 32 * dy : 32 * dy + 32]
    with jax.named_scope("loss3"):
        loss_sum = collected(sy_take, 24, loss_sum, "y")
        exchange(sz_give, sz_take, 27, loss_sum, "z")
    with jax.named_scope("g_z"):
        left = grad[y, pl.ds(z, 1), :, :GLA].reshape(EG, GLA)
        for dz in z_near:
            arrived(z_take.at[dz - 1], z_s.at[0], z_r.at[dz - 1], {"z": mod(z - dz, NZ)})
            left = left + z_take[dz - 1].astype(F32)
        grad[y, pl.ds(z, 1), :, :GLA] = left.reshape(1, EG, GLA)
        grad[y, pl.ds(z, 1), :, GLA:GLB] = right.reshape(1, EG, GLB - GLA)
        grad[y, pl.ds(z, 1), :, GLB : GLB + 32] = last.reshape(1, EG, 32)

    g = grad[y, pl.ds(z, 1)].reshape(EG, KP)
    e_id = lax.broadcasted_iota(jnp.int32, (EG, KP), 0)
    k_id = lax.broadcasted_iota(jnp.int32, (EG, KP), 1)
    squared = jnp.where((e_id < ED) & (k_id < KD), g * g + FLOOR_VALUE, 0.0)

    with jax.named_scope("st_row"):
        e_col = e_id[:, 0:128]
        l_col = k_id[:, 0:128]
        rows = jnp.broadcast_to(jnp.sum(squared, axis=1, keepdims=True), (EG, 128))
        row_line = jnp.sum(jnp.where(e_col == l_col, rows, 0.0), axis=0, keepdims=True)
        exchange(row_give, row_take, 0, row_line, "row")
        cols = jnp.sum(squared, axis=0, keepdims=True)
        row_line = collected(row_take, 0, row_line, "row")[:, :ED]
        row_line = DECAY_RATE * row_moment[...].reshape(1, ED) + (1.0 - DECAY_RATE) * row_line / FF
        new_row = jnp.sum(
            jnp.where(
                e_id[:, :ED] == k_id[:, :ED], jnp.broadcast_to(row_line, (EG, ED)), 0.0
            ), axis=1, keepdims=True
        )
        new_row = jnp.where(e_col[:, 0:1] < ED, new_row, 1.0)
        ratio = jnp.sum(g * g / new_row, axis=0, keepdims=True)
    with jax.named_scope("st_col"):
        cols2 = jnp.concatenate([cols, ratio], axis=1)
        exchange(cy_give, cy_take, 7, cols2, "y")
        cols2 = collected(cy_take, 7, cols2, "y")
        exchange(cz_give, cz_take, 10, cols2, "z")
        cols2 = collected(cz_take, 10, cols2, "z")
    with jax.named_scope("st_tot"):
        cols, ratio = cols2[:, :KP], cols2[:, KP:]
        col_line = DECAY_RATE * col_moment[...].reshape(1, KD) + (1.0 - DECAY_RATE) * cols[:, :KD] / D
        raw_sum = jnp.sum(ratio[:, :KD] / col_line, axis=1, keepdims=True)
        exchange(s_give, s_take, 17, jnp.broadcast_to(raw_sum, (1, 128)), "row")
        raw = g[:ED, :KD] / jnp.sqrt(new_row[:ED] * col_line)
        loss_sum = collected(sz_take, 27, loss_sum, "z")
        small_out[...] = jnp.zeros_like(small_out)
        small_out[0:1, :KD] = col_line
        small_out[1:2, :ED] = row_line
        small_out[2:3, 0:128] = loss_sum * (1.0 / BATCH)
        both = collected(s_take, 17, jnp.broadcast_to(raw_sum, (1, 128)), "row")
    with jax.named_scope("upd"):
        rms = jnp.sqrt(both[:, 0:1] / (D * FF))
        update_out[...] = raw / jnp.maximum(1.0, rms / CLIP_LEVEL)
    with jax.named_scope("finish"):
        w.finish()
        t.finish()
        all_sent(h_out.at[pl.ds(0, 7)], h_s.at[0], h_r.at[0], {"c": other})
        for k, (ref, device) in enumerate(
            ((far_p, up), (far_m, down), (near_p, up), (near_m, down), (relay_p, up), (relay_m, down))
        ):
            all_sent(ref, g_s.at[k], g_r.at[k], device)
        all_sent(z_take, z_s.at[0], z_r.at[0], {"z": mod(z + 1, NZ)})
        all_sent(b_take, b_s.at[0], b_r.at[0], {"z": mod(z + 1, NZ)})
        all_sent(yb_take, yb_s.at[0], yb_r.at[0], up)


def step_kernel(hidden, weight, text, pooled, row_moment, col_moment, scale, bias):
    vmem = pl.BlockSpec(memory_space=pltpu.VMEM)
    smem = pl.BlockSpec(memory_space=pltpu.SMEM)
    n_row = NX * NC
    dma = pltpu.SemaphoreType.DMA
    return pl.pallas_call(
        whole_kernel,
        out_shape=(
            jax.ShapeDtypeStruct((ED, KD), F32),
            jax.ShapeDtypeStruct((8, KP), F32),
        ),
        in_specs=[pl.BlockSpec(memory_space=pl.ANY)] * 6 + [smem] * 2,
        out_specs=(vmem,) * 2,
        scratch_shapes=[
            pltpu.VMEM((TOK, FF), BF16),
            pltpu.VMEM((ED, KD), F32),
            pltpu.VMEM((TOK, D), BF16),
            pltpu.VMEM((TOK, D), BF16),
            pltpu.VMEM((ED,), F32),
            pltpu.VMEM((KD,), F32),
            dma((6,)),
            pltpu.VMEM((n_row, TOK, KP), BF16),
            pltpu.VMEM((EP, KP), BF16),
            pltpu.VMEM((NX * TOK, NY * TOK), F32),
            pltpu.VMEM((NX * TOK, NY * TOK), F32),
            pltpu.VMEM((NX * TOK, NY * TOK), BF16),
            pltpu.VMEM((NX * TOK, NY * TOK), BF16),
            pltpu.VMEM((n_row, TOK, KP), BF16),
            pltpu.VMEM((n_row, TOK, D), BF16),
            pltpu.VMEM((8, NY * TOK), F32),
            pltpu.VMEM((NZ * NY, EP, WLA), BF16),
            pltpu.VMEM((NY * NZ, EP, KP - WLA), BF16),
            pltpu.VMEM((D, KP), BF16),
            pltpu.VMEM((NZ * NY, TOK, TLA), BF16),
            pltpu.VMEM((NY * NZ, TOK, D - TLA), BF16),
            pltpu.VMEM((TOK, D), BF16),
            pltpu.VMEM((n_row, TOK, D), F32),
            pltpu.VMEM((NX, TOK, D), F32),
            pltpu.VMEM((NX, TOK, D), F32),
            pltpu.VMEM((NX - 1, TOK, D), BF16),
            pltpu.VMEM((NX - 1, TOK, D), BF16),
            pltpu.VMEM((n_row, TOK, D), BF16),
            pltpu.VMEM((TOK, D), F32),
            pltpu.VMEM((TOK, 128), F32),
            pltpu.VMEM((n_row, TOK, D), F32),
            pltpu.VMEM((NX, TOK, D), BF16),
            pltpu.VMEM((NX, TOK, D), BF16),
            pltpu.VMEM((NX - 1, TOK, D), BF16),
            pltpu.VMEM((NX - 1, TOK, D), BF16),
            pltpu.VMEM((NY, NZ, EG, KP), F32),
            *[pltpu.VMEM((NZ // 2, EG, GLA), BF16)] * 12,
            pltpu.VMEM((NZ, EG, GLA), BF16),
            pltpu.VMEM((NZ - 1, EG, GLA), BF16),
            pltpu.VMEM((NY, NZ * EG, 384), BF16),
            pltpu.VMEM((NZ, EG, 128), F32),
            pltpu.VMEM((NZ, NY + 1, EG, 128), BF16),
            pltpu.VMEM((NZ - 1, NY + 1, EG, 128), BF16),
            pltpu.VMEM((NY, 2, EG, 128), F32),
            pltpu.VMEM((NY - 1, 2, EG, 128), F32),
            pltpu.VMEM((1, 128), F32),
            pltpu.VMEM((n_row - 1, 1, 128), F32),
            pltpu.VMEM((1, 2 * KP), F32),
            pltpu.VMEM((NY - 1, 1, 2 * KP), F32),
            pltpu.VMEM((1, 2 * KP), F32),
            pltpu.VMEM((NZ - 1, 1, 2 * KP), F32),
            pltpu.VMEM((1, 128), F32),
            pltpu.VMEM((n_row - 1, 1, 128), F32),
            pltpu.VMEM((1, 128), F32),
            pltpu.VMEM((n_row - 1, 1, 128), F32),
            pltpu.VMEM((1, 128), F32),
            pltpu.VMEM((NY - 1, 1, 128), F32),
            pltpu.VMEM((1, 128), F32),
            pltpu.VMEM((NZ - 1, 1, 128), F32),
            dma((2,)), dma((N_MSG,)), dma((2,)), dma((N_MSG,)),
            dma((1,)), dma((7,)), dma((2,)), dma((10,)), dma((1,)), dma((16,)),
            dma((2,)), dma((10,)), dma((1,)), dma((16,)),
            dma((6,)), dma((6,)), dma((1,)), dma((7,)), dma((1,)), dma((14,)),
            dma((1,)), dma((3,)), dma((7,)), dma((41,)),
        ],
        compiler_params=pltpu.CompilerParams(
            collective_id=0, has_side_effects=True, vmem_limit_bytes=60 * 1024 * 1024
        ),
        name="step",
    )(hidden, weight, text, pooled, row_moment, col_moment, scale, bias)


def out_kernel(update_in, small, update, new_row, new_col, loss):
    update[...] = update_in[...]
    new_row[...] = small[1:2, :ED].reshape(ED)
    new_col[...] = small[0:1, :KD].reshape(KD)
    loss[0] = small[2, 0]


def per_device(pooled, hidden, text, weight, row_moment, col_moment, log_scale, bias):
    update, small = step_kernel(
        hidden, weight, text, pooled, row_moment, col_moment, log_scale.reshape(1), bias.reshape(1)
    )
    vmem = pl.BlockSpec(memory_space=pltpu.VMEM)
    update, new_row, new_col, loss = pl.pallas_call(
        out_kernel,
        out_shape=(
            jax.ShapeDtypeStruct((ED, KD), F32),
            jax.ShapeDtypeStruct((ED,), F32),
            jax.ShapeDtypeStruct((KD,), F32),
            jax.ShapeDtypeStruct((1,), F32),
        ),
        in_specs=[vmem] * 2,
        out_specs=(vmem, vmem, vmem, pl.BlockSpec(memory_space=pltpu.SMEM)),
        name="out",
    )(update, small)
    return (update, new_row, new_col, loss.reshape(()))


def solution(mesh):
    finer = Mesh(mesh.devices.reshape(NX, NC, NY, NZ), ALL)
    return jax.shard_map(
        per_device,
        mesh=finer,
        in_specs=(
            P(ALL, None), P(ALL, None), P(ALL, None), P(COL, ROW), P(COL), P(ROW), P(), P(),
        ),
        out_specs=(P(COL, ROW), P(COL), P(ROW), P()),
        check_vma=False,
    )
```

```python
import functools

import jax
import jax.numpy as jnp
from jax import lax
from jax.experimental import pallas as pl
from jax.experimental.pallas import tpu as pltpu
from jax.sharding import Mesh
from jax.sharding import PartitionSpec as P

D = 1152
FF = 4304
NX, NC, NY, NZ = 4, 2, 4, 8
TOK = 64
KD = FF // (NX * NC)
KP = 640
ED = D // (NY * NZ)
EP = 48
WLA = 256
TLA = 512
EG = 40
GLA = 384
GLB = 512
ROW = ("x", "c")
COL = ("y", "z")
ALL = ("x", "c", "y", "z")
BATCH = TOK * NX * NC * NY * NZ

EPSILON = 1e-06
DECAY_RATE = 0.8
CLIP_LEVEL = 1.0
FLOOR_VALUE = 1e-30

MESH = pl.DeviceIdType.MESH
F32 = jnp.float32
BF16 = jnp.bfloat16


def mod(value, size):
    return lax.rem(value + 2 * size, size)


def send(src, dst, ssem, rsem, device):
    pltpu.make_async_remote_copy(src, dst, ssem, rsem, device_id=device, device_id_type=MESH).start()


def arrived(dst, ssem, rsem, device):
    pltpu.make_async_remote_copy(dst, dst, ssem, rsem, device_id=device, device_id_type=MESH).wait_recv()


def all_sent(ref, ssem, rsem, device):
    pltpu.make_async_remote_copy(ref, ref, ssem, rsem, device_id=device, device_id_type=MESH).wait_send()


A0, AP, AM, BP, BM, YP, YM, Y2 = 0, 3, 17, 33, 37, 40, 48, 56
N_MSG = 64
B_PLACE = (3, 1, 0, 2)
EXCHANGES = (0, 7, 10, 17, 24, 27, 34)
A_MSG = range(A0, BP)
OFFSETS = [0, -1, 1, -2, 2, -3, 3, -4]


class PlaneGather:
    def __init__(self, piece, a, b, la, rows, late, ssem, rsem, y, z):
        self.late = late
        self.piece, self.a, self.b, self.la, self.rows = piece, a, b, la, pl.ds(0, rows)
        self.piece_a = piece.at[self.rows, pl.ds(0, la)]
        self.piece_b = piece.at[self.rows, pl.ds(la, piece.shape[1] - la)]
        self.ssem, self.rsem, self.y, self.z = ssem, rsem, y, z
        self.ys = {o: mod(y + o, NY) for o in range(1 - NY, NY)}
        self.zs = {o: mod(z + o, NZ) for o in range(-(NZ // 2), NZ // 2 + 1)}
        self.sems = [(ssem.at[0 if i in A_MSG else 1], rsem.at[i]) for i in range(N_MSG)]
        self.a_at = {(o, dy): a.at[self.zs[o] * NY + self.ys[-dy], self.rows] for o in self.zs for dy in range(NY)}
        self.b_at = {(yo, o): b.at[self.ys[yo] * NZ + self.zs[o], self.rows] for o in self.zs for yo in range(-2, 3)}

    def _send(self, src, dst, i, device):
        send(src, dst, *self.sems[i], device)

    def _wait(self, dst, i, device):
        sems = self.sems[i] if isinstance(i, int) else (self.ssem.at[1], self.rsem.at[i])
        arrived(dst, *sems, device)

    def own(self):
        self.a[self.z * NY + self.y] = self.piece[:, : self.la]
        self.b[self.y * NZ + self.z] = self.piece[:, self.la :]

    def finish(self):
        n = pl.ds(0, NY * NZ - 1)
        all_sent(self.a.at[n, self.rows], *self.sems[A0], self._zdev(1))
        all_sent(self.b.at[n, self.rows], *self.sems[BP], self._zdev(1))

    def _a(self, zo, dy):
        return self.a_at[zo, dy]

    def _b(self, yo, zo):
        return self.b_at[yo, zo]

    def _zdev(self, o):
        return {"z": self.zs[o]}

    def _ydev(self, o):
        return {"y": self.ys[o]}

    @staticmethod
    def _has(sign, s, dy):
        if s < NZ // 2:
            return s >= 1
        return s == NZ // 2 and (dy < NY // 2) == (sign > 0)

    def _ring_a(self, s, dy, sign):
        if not self._has(sign, s, dy):
            return
        src = self._a(-sign * (s - 1), dy)
        dst = src
        if s == 1 and dy == 0:
            src = self.piece_a
        self._send(src, dst, (AP if sign > 0 else AM) + (s - 1) * 4 + dy, self._zdev(sign))

    def _ring_b(self, s, sign):
        if s > (NZ // 2 if sign > 0 else NZ // 2 - 1):
            return
        dst = self._b(0, -sign * (s - 1))
        src = self.piece_b if s == 1 else dst
        self._send(src, dst, (BP if sign > 0 else BM) + s - 1, self._zdev(sign))

    def _spread_b(self, j):
        dst = self._b(0, OFFSETS[j])
        src = self.piece_b if j == 0 else dst
        self._send(src, dst, YP + j, self._ydev(1))
        self._send(src, dst, YM + j, self._ydev(-1))

    def _near_b(self, j):
        o = OFFSETS[j]
        self._wait(self._b(-1, o), YP + j, self._ydev(-1))
        if j % 2 == 0:
            self._send(self._b(-1, o), self._b(-1, o), Y2 + j, self._ydev(1))
        self._wait(self._b(1, o), YM + j, self._ydev(1))
        if j % 2 == 1:
            self._send(self._b(1, o), self._b(1, o), Y2 + j, self._ydev(-1))

    def far(self, j):
        o = OFFSETS[j]
        yo = -2 if j % 2 == 0 else 2
        self._wait(self._b(yo, o), Y2 + j, self._ydev(-1 if j % 2 == 0 else 1))

    def far_at(self, j):
        if isinstance(j, int):
            return self.far(j)
        hop = (j + 1) // 2
        zz = mod(self.z + hop * (1 - 2 * lax.rem(j, 2)), NZ)
        self._wait(self.b.at[self.ys[2] * NZ + zz, self.rows], Y2 + j, self._ydev(1))

    def start(self):
        for dy in range(1, NY):
            self._send(self.piece_a, self._a(0, 0), A0 + dy - 1, self._ydev(dy))
        for sign in (1, -1):
            self._ring_b(1, sign)
            self._ring_a(1, 0, sign)
        if not self.late:
            self._spread_b(0)

    def step(self, k):
        if self.late and k == 1:
            self._spread_b(0)
        for s_sign in (1, -1):
            if k <= (NZ // 2 if s_sign > 0 else NZ // 2 - 1):
                self._wait(self._b(0, -s_sign * k), (BP if s_sign > 0 else BM) + k - 1, self._zdev(-s_sign))
                self._ring_b(k + 1, s_sign)
                self._spread_b(OFFSETS.index(-s_sign * k))
        for dy in range(NY):
            if k == 1:
                if dy == 0:
                    continue
                self._wait(self._a(0, dy), A0 + dy - 1, self._ydev(-dy))
                self._ring_a(1, dy, 1)
                self._ring_a(1, dy, -1)
                continue
            s = k - 1
            for sign in (1, -1):
                if self._has(sign, s, dy):
                    self._wait(
                        self._a(-sign * s, dy), (AP if sign > 0 else AM) + (s - 1) * 4 + dy, self._zdev(-sign)
                    )
                    self._ring_a(s + 1, dy, sign)
        for j, o in enumerate(OFFSETS):
            if abs(o) == k - 1 and (j > 0 or not self.late) or (j == 0 and self.late and k == 2):
                self._near_b(j)


def whole_kernel(
    hidden_in, weight_in, text_in, pooled_in, row_in, col_in, scale_ref, bias_ref,
    update_out, small_out,
    hidden, weight, text, pooled, row_moment, col_moment, in_s,
    hid, wp, logit_a, logit_b, pg_a, pg_b,
    h_out, mg_out, loss_out,
    wa, wb, wc, ta, tb, tn, part, give, take, share, got, img, unit, length,
    acc, give2, take2, share2, got2,
    grad, far_p, far_m, near_p, near_m, relay_p, relay_m,
    r_far_p, r_far_m, r_near_p, r_near_m, r_relay_p, r_relay_m,
    z_give, z_take, choose, tail, b_give, b_take, yb_give, yb_take,
    row_give, row_take, cy_give, cy_take, cz_give, cz_take,
    s_give, s_take, l_give, l_take, sy_give, sy_take, sz_give, sz_take,
    w_s, w_r, t_s, t_r, h_s, h_r, p_s, p_r, i_s, i_r,
    g_s, g_r, z_s, z_r, b_s, b_r, yb_s, yb_r, st_s, st_r,
):
    x, c = lax.axis_index("x"), lax.axis_index("c")
    y, z = lax.axis_index("y"), lax.axis_index("z")
    me = c * NX + x
    other = 1 - c

    loads = [
        pltpu.make_async_copy(src, dst, in_s.at[i])
        for i, (src, dst) in enumerate(
            (
                (weight_in, weight), (hidden_in, hidden), (text_in, text), (pooled_in, pooled),
                (row_in, row_moment), (col_in, col_moment),
            )
        )
    ]
    for load in loads:
        load.start()
    wa[...] = jnp.zeros_like(wa)
    wb[...] = jnp.zeros_like(wb)
    with jax.named_scope("signal"):
        barrier = pltpu.get_barrier_semaphore()
        peers = [{"z": mod(z + dz, NZ)} for dz in range(1, NZ)]
        peers += [{"y": mod(y + dy, NY)} for dy in range(1, NY)]
        peers += [
            {"x": mod(x + dx, NX), "c": lax.rem(c + dc, NC)}
            for dx in range(NX) for dc in range(NC) if dx + dc > 0
        ]
        for peer in peers:
            pl.semaphore_signal(barrier, inc=1, device_id=peer, device_id_type=MESH)

    with jax.named_scope("prep"):
        for load in loads:
            load.wait()
        wp[...] = jnp.zeros_like(wp)
        wp[:ED, :KD] = weight[...].astype(BF16)
        hid[...] = jnp.zeros_like(hid)
        for r in range(NX * NC):
            hid[(r % NC) * NX + r // NC, :, :KD] = hidden[:, KD * r : KD * (r + 1)]
    with jax.named_scope("barrier"):
        pl.semaphore_wait(barrier, len(peers))
    w = PlaneGather(wp, wa, wb, WLA, EG, False, w_s, w_r, y, z)
    t = PlaneGather(tn, ta, tb, TLA, TOK, True, t_s, t_r, y, z)

    def project(half, k0, k1):
        rows = h_out[pl.ds(half * NX, NX), :, k0:k1].reshape(NX * TOK, k1 - k0)
        for n in range(3):
            lanes = slice(384 * n, 384 * (n + 1))
            product = lax.dot_general(
                rows, wc[lanes, k0:k1], (((1,), (1,)), ((), ())), preferred_element_type=F32
            ).reshape(NX, TOK, 384)
            at = pl.ds(half * NX, NX)
            part[at, :, lanes] = product if k0 == 0 else part[at, :, lanes] + product

    with jax.named_scope("wstart"):
        w.start()
        row_peers = [(dx, dc) for dx in range(NX) for dc in range(NC) if dx + dc > 0]
        for i, (dx, dc) in enumerate(row_peers):
            xx, cc = mod(x + dx, NX), lax.rem(c + dc, NC)
            send(hid.at[cc * NX + xx], h_out.at[me], h_s.at[0], h_r.at[i], {"x": xx, "c": cc})
        h_out[me] = hid[me]
        w.own()
        tf = text[...].astype(F32)
        tn[...] = (tf / jnp.sqrt(jnp.sum(tf * tf, axis=1, keepdims=True) + EPSILON)).astype(BF16)
    with jax.named_scope("w123"):
        w.step(1)
        w.step(2)
        w.step(3)
    with jax.named_scope("tstart"):
        t.own()
        t.start()
    with jax.named_scope("w45far"):
        w.step(4)
        w.step(5)
    with jax.named_scope("t1"):
        t.step(1)
    with jax.named_scope("hwait"):
        for i, (dx, dc) in enumerate(row_peers):
            xx, cc = mod(x - dx, NX), lax.rem(c + dc, NC)
            arrived(h_out.at[cc * NX + xx], h_s.at[0], h_r.at[i], {"x": xx, "c": cc})

    with jax.named_scope("compactA"):
        r_id = lax.broadcasted_iota(jnp.int32, (4 * ED, 4 * EP), 0)
        c_id = lax.broadcasted_iota(jnp.int32, (4 * ED, 4 * EP), 1)
        pick = jnp.zeros((4 * ED, 4 * EP), F32)
        for g in range(4):
            hit = (r_id >= ED * g) & (r_id < ED * (g + 1)) & (c_id - r_id == (EP - ED) * g)
            pick = jnp.where(hit, 1.0, pick)
        pick = pick.astype(BF16)
        for g in range(8):
            yy, z0 = g // 2, 4 * (g % 2)
            pieces = jnp.concatenate([wa[(z0 + k) * NY + yy] for k in range(4)], axis=0)
            wc[pl.ds(4 * ED * g, 4 * ED), 0:WLA] = jnp.dot(pick, pieces, preferred_element_type=F32).astype(BF16)
        for half in range(2):
            project(half, 0, WLA)
    with jax.named_scope("wfar"):
        for j in range(8):
            w.far(j)

    hf_rows = [pl.ds(TOK // 2 * hf, TOK // 2) for hf in range(2)]

    def reduce_rows(val, gv, tk, sh, gt, ss, rs):
        for dx in (2, 1, 3, 0):
            xx = mod(x + dx, NX)
            gv[xx] = val[other * NX + xx].astype(gv.dtype)
            send(gv.at[xx], tk.at[xx], ss.at[0], rs.at[dx], {"c": other})
        yield
        for hf, rows in enumerate(hf_rows):
            for dx in (2, 1, 3):
                xx = mod(x + dx, NX)
                if hf == 0:
                    arrived(tk.at[xx], ss.at[0], rs.at[dx], {"c": other})
                    sh[dx - 1] = (val[c * NX + xx] + tk[xx].astype(F32)).astype(BF16)
                send(sh.at[dx - 1, rows], gt.at[dx - 1, rows], ss.at[1], rs.at[3 + 3 * hf + dx], {"x": xx})
        yield
        arrived(tk.at[x], ss.at[0], rs.at[0], {"c": other})
        for hf, rows in enumerate(hf_rows):
            total = val[me, rows] + tk[x, rows].astype(F32)
            for dx in (1, 3, 2):
                arrived(gt.at[dx - 1, rows], ss.at[1], rs.at[3 + 3 * hf + dx], {"x": mod(x - dx, NX)})
            for dx in (1, 2, 3):
                total = total + gt[dx - 1, rows].astype(F32)
            yield total
        all_sent(gv, ss.at[0], rs.at[0], {"c": other})
        all_sent(sh, ss.at[1], rs.at[4], {"x": mod(x + 1, NX)})
        yield

    def share_rows(buf, ss, rs):
        for hf, rows in enumerate(hf_rows):
            mine = buf.at[me, rows]
            for dx in (2, 1, 3):
                send(mine, mine, ss.at[0], rs.at[8 * hf + dx], {"x": mod(x + dx, NX)})
            send(mine, mine, ss.at[0], rs.at[8 * hf + 4], {"c": other})
            yield
        for hf, rows in enumerate(hf_rows):
            for dx in (1, 3, 2):
                got_at = buf.at[c * NX + mod(x - dx, NX), rows]
                arrived(got_at, ss.at[0], rs.at[8 * hf + dx], {"x": mod(x - dx, NX)})
                send(got_at, got_at, ss.at[0], rs.at[8 * hf + 4 + dx], {"c": other})
        yield
        for hf, rows in enumerate(hf_rows):
            for dx in (0, 1, 3, 2):
                at = buf.at[other * NX + mod(x - dx, NX), rows]
                arrived(at, ss.at[0], rs.at[8 * hf + 4 + dx], {"c": other})
        all_sent(buf.at[pl.ds(0, 7)], ss.at[0], rs.at[1], {"c": other})
        yield

    with jax.named_scope("compactB"):
        for g in range(8):
            yy, z0 = g // 2, 4 * (g % 2)
            pieces = wb[yy * NZ + z0 : yy * NZ + z0 + 4].reshape(4 * EP, KP - WLA)
            wc[pl.ds(4 * ED * g, 4 * ED), WLA:KP] = jnp.dot(pick, pieces, preferred_element_type=F32).astype(BF16)
    with jax.named_scope("proj1"):
        project(other, WLA, KP)
    with jax.named_scope("red1a"):
        red = reduce_rows(part, give, take, share, got, p_s, p_r)
        next(red)
    with jax.named_scope("proj2"):
        project(c, WLA, KP)
    with jax.named_scope("red1b"):
        next(red)
    with jax.named_scope("t2"):
        t.step(2)
    with jax.named_scope("red1c_norm"):
        give_img = share_rows(img, i_s, i_r)
        for hf, rows in enumerate(hf_rows):
            mixed = pooled[rows].astype(F32) + next(red)
            ln = jnp.sqrt(jnp.sum(mixed * mixed, axis=1, keepdims=True) + EPSILON)
            length[rows] = jnp.broadcast_to(ln, (TOK // 2, 128))
            un = mixed / ln
            unit[rows] = un
            img[me, rows] = un.astype(BF16)
            next(give_img)
            if hf == 0:
                t.step(3)
        next(red)
    with jax.named_scope("imgshare"):
        next(give_img)
        next(give_img)
    with jax.named_scope("t4"):
        t.step(4)
    with jax.named_scope("pairs"):
        scale = jnp.exp(jnp.broadcast_to(scale_ref[0], (8, 128)))[0:1, 0:1]
        bias = bias_ref[0]
        acc[...] = jnp.zeros_like(acc)
        loss_out[...] = jnp.zeros_like(loss_out)
        tile = NX * TOK
        t_dims = (((1,), (1,)), ((), ()))

        halves = (other, c)

        def texts(g):
            t_b = jnp.concatenate([tb[yy * NZ + g] for yy in range(NY)], axis=0)
            return ta[pl.ds(g * NY, NY)].reshape(NY * TOK, TLA), t_b

        def logits_of(g, h, out):
            t_a, t_b = texts(g)
            images = img[pl.ds(halves[h] * NX, NX)].reshape(tile, D)
            out[...] = lax.dot_general(
                images[:, :TLA], t_a, t_dims, preferred_element_type=F32
            ) + lax.dot_general(images[:, TLA:], t_b, t_dims, preferred_element_type=F32)

        def elementwise(src, out, own):
            m = scale * src[...] + bias
            if own:
                col = lax.broadcasted_iota(jnp.int32, (tile, NY * TOK), 1)
                row = lax.broadcasted_iota(jnp.int32, (tile, NY * TOK), 0)
                same = (row - col == TOK * (x - y)) & (col >= TOK * y) & (col < TOK * y + TOK)
                m = jnp.where(same, -m, m)
            e = jnp.exp(-jnp.abs(m))
            d = 1.0 + e
            r = 1.0 / d
            soft = jnp.maximum(m, 0.0) + (jnp.log(d) + (e - (d - 1.0)) * r)
            loss_out[...] += jnp.sum(soft.reshape(tile // 8, 8, NY * TOK), axis=0)
            sig = jnp.where(m >= 0.0, r, e * r)
            if own:
                sig = jnp.where(same, -sig, sig)
            out[...] = sig.astype(BF16)

        def to_images(g, h, src):
            t_a, t_b = texts(g)
            pg = src[...]
            rows = pl.ds(halves[h] * NX, NX)
            acc[rows, :, :TLA] += jnp.dot(pg, t_a, preferred_element_type=F32).reshape(NX, TOK, TLA)
            acc[rows, :, TLA:] += jnp.dot(pg, t_b, preferred_element_type=F32).reshape(NX, TOK, D - TLA)

        def group(j):
            hop = (j + 1) // 2
            return mod(z + hop * (1 - 2 * lax.rem(j, 2)), NZ)

        def body(j, carry):
            @pl.when(j == 5)
            def _():
                with jax.named_scope("p_t5"):
                    t.step(5)

            with jax.named_scope("p_far"):
                t.far_at(j)
            now, last = group(j), group(j - 1)
            logits_of(now, 0, logit_a)
            elementwise(logit_b, pg_b, False)
            to_images(last, 0, pg_a)
            logits_of(now, 1, logit_b)
            elementwise(logit_a, pg_a, False)
            to_images(last, 1, pg_b)
            return carry

        t.far_at(1)
        first, final = mod(z + OFFSETS[1], NZ), mod(z + OFFSETS[7], NZ)
        logits_of(first, 0, logit_a)
        logits_of(first, 1, logit_b)
        elementwise(logit_a, pg_a, False)
        lax.fori_loop(2, NZ, body, 0)
        t.far_at(0)
        logits_of(z, 0, logit_a)
        elementwise(logit_b, pg_b, False)
        to_images(final, 0, pg_a)
        logits_of(z, 1, logit_b)
        elementwise(logit_a, pg_a, False)
        to_images(final, 1, pg_b)
        to_images(z, 0, pg_a)
    with jax.named_scope("red2"):
        red = reduce_rows(acc, give2, take2, share2, got2, p_s, p_r)
        next(red)
        elementwise(logit_b, pg_b, True)
        to_images(z, 1, pg_b)
        next(red)
        give_mg = share_rows(mg_out, i_s, i_r)
        for rows in hf_rows:
            ug = (scale * (1.0 / BATCH)) * next(red)
            un = unit[rows]
            mg = (ug - un * jnp.sum(un * ug, axis=1, keepdims=True)) / length[rows, 0:1]
            mg_out[me, rows] = mg.astype(BF16)
            next(give_mg)
        next(red)
    with jax.named_scope("mgshare"):
        next(give_mg)

    def exchange(give_ref, take_ref, base, value, kind):
        give_ref[...] = value
        slot = EXCHANGES.index(base)
        sizes = {"row": row_peers, "y": range(1, NY), "z": range(1, NZ)}[kind]
        for i, d in enumerate(sizes):
            if kind == "row":
                device = {"x": mod(x + d[0], NX), "c": lax.rem(c + d[1], NC)}
            else:
                device = {kind: mod((y if kind == "y" else z) + d, NY if kind == "y" else NZ)}
            send(give_ref, take_ref.at[i], st_s.at[slot], st_r.at[base + i], device)

    def collected(take_ref, base, value, kind):
        slot = EXCHANGES.index(base)
        sizes = {"row": row_peers, "y": range(1, NY), "z": range(1, NZ)}[kind]
        for i, d in enumerate(sizes):
            if kind == "row":
                device = {"x": mod(x - d[0], NX), "c": lax.rem(c + d[1], NC)}
            else:
                device = {kind: mod((y if kind == "y" else z) - d, NY if kind == "y" else NZ)}
            arrived(take_ref.at[i], st_s.at[slot], st_r.at[base + i], device)
            value = value + take_ref[i]
        all_sent(take_ref, st_s.at[slot], st_r.at[base], device)
        return value

    zi = lax.broadcasted_iota(jnp.int32, (NZ, EG, 384), 0)
    ji = lax.broadcasted_iota(jnp.int32, (NZ, EG, 384), 1)
    li = lax.broadcasted_iota(jnp.int32, (NZ, EG, 384), 2)

    def product(dy, h):
        yy = mod(y + dy, NY)
        at = pl.ds(h * NX, NX)
        mg = mg_out[at, :, pl.ds(pl.multiple_of(256 * yy, 128), 384)].reshape(NX * TOK, 384)
        mg_t = lax.dot_general(choose[dy], mg, (((1,), (1,)), ((), ())), preferred_element_type=F32).astype(BF16)
        rows = h_out[at].reshape(NX * TOK, KP)
        return jnp.dot(mg_t, rows, preferred_element_type=F32).reshape(NZ, EG, KP)

    def gradient_of(dy):
        yy = mod(y + dy, NY)
        if dy == 0:
            grad[yy] = product(dy, c)
        grad[yy] += product(dy, other)
        b_give[:, B_PLACE[dy]] = grad[yy, :, :, GLA:GLB].astype(BF16)
        tail[:, :, 32 * dy : 32 * dy + 32] = grad[yy, :, :, GLB : GLB + 32]

    with jax.named_scope("g_own"):
        for dy in (2, 1, 3, 0):
            mask = (ji < ED) & (li == 32 * mod(y + dy, NY) + ED * zi + ji)
            choose[dy] = jnp.where(mask, 1.0, 0.0).reshape(NZ * EG, 384).astype(BF16)
            if dy > 0:
                grad[mod(y + dy, NY)] = product(dy, c)
    with jax.named_scope("mgwait"):
        next(give_mg)
    z_order = (4, 3, 5, 2, 6, 1, 7)
    z_near = (1, 7, 2, 6, 3, 5, 4)
    b_parts = (pl.ds(0, 2), pl.ds(2, 3))

    def give_b(k):
        for dz in z_order:
            zz = mod(z + dz, NZ)
            send(
                b_give.at[zz, b_parts[k]], b_take.at[dz - 1, b_parts[k]],
                b_s.at[0], b_r.at[7 * k + dz - 1], {"z": zz},
            )

    with jax.named_scope("loss1"):
        loss_sum = jnp.sum(jnp.sum(loss_out[...], axis=0, keepdims=True), axis=1, keepdims=True)
        loss_sum = jnp.broadcast_to(loss_sum, (1, 128))
        exchange(l_give, l_take, 34, loss_sum, "row")
    with jax.named_scope("g_far"):
        half = NZ // 2
        y_far, y_up, y_down = mod(y + 2, NY), mod(y + 1, NY), mod(y - 1, NY)
        up, down = {"y": y_up}, {"y": y_down}
        gradient_of(2)
        far_p[...] = grad[y_far, :half, :, :GLA].astype(BF16)
        far_m[...] = grad[y_far, half:, :, :GLA].astype(BF16)
        send(far_p, r_far_p, g_s.at[0], g_r.at[0], up)
        send(far_m, r_far_m, g_s.at[1], g_r.at[1], down)
    with jax.named_scope("g_rest"):
        gradient_of(1)
        near_p[...] = grad[y_up, half:, :, :GLA].astype(BF16)
        send(near_p, r_near_p, g_s.at[2], g_r.at[2], up)
        give_b(0)
        gradient_of(3)
        near_m[...] = grad[y_down, :half, :, :GLA].astype(BF16)
        send(near_m, r_near_m, g_s.at[3], g_r.at[3], down)
        gradient_of(0)
        b_give[:, NY] = tail[...].astype(BF16)
        give_b(1)
    with jax.named_scope("g_relay"):
        arrived(r_far_p, g_s.at[0], g_r.at[0], down)
        relay_p[...] = (grad[y_up, :half, :, :GLA] + r_far_p[...].astype(F32)).astype(BF16)
        send(relay_p, r_relay_p, g_s.at[4], g_r.at[4], up)
        arrived(r_far_m, g_s.at[1], g_r.at[1], up)
        relay_m[...] = (grad[y_down, half:, :, :GLA] + r_far_m[...].astype(F32)).astype(BF16)
        send(relay_m, r_relay_m, g_s.at[5], g_r.at[5], down)
    with jax.named_scope("loss2"):
        loss_sum = collected(l_take, 34, loss_sum, "row")
        exchange(sy_give, sy_take, 24, loss_sum, "y")
    with jax.named_scope("g_ysum"):
        arrived(r_near_p, g_s.at[2], g_r.at[2], down)
        arrived(r_near_m, g_s.at[3], g_r.at[3], up)
        arrived(r_relay_p, g_s.at[4], g_r.at[4], down)
        arrived(r_relay_m, g_s.at[5], g_r.at[5], up)
        grad[y, :half, :, :GLA] += r_relay_p[...].astype(F32) + r_near_m[...].astype(F32)
        grad[y, half:, :, :GLA] += r_near_p[...].astype(F32) + r_relay_m[...].astype(F32)
        z_give[...] = grad[y, :, :, :GLA].astype(z_give.dtype)
        for dz in z_order:
            zz = mod(z + dz, NZ)
            send(z_give.at[zz], z_take.at[dz - 1], z_s.at[0], z_r.at[dz - 1], {"z": zz})
    with jax.named_scope("g_bz"):
        for dy in range(NY):
            yb_give[dy, 0] = grad[mod(y + dy, NY), pl.ds(z, 1), :, GLA:GLB].reshape(EG, GLB - GLA)
        last = tail[pl.ds(z, 1)].reshape(EG, 128)
        for dz in z_near:
            for k in range(2):
                arrived(b_take.at[dz - 1, b_parts[k]], b_s.at[0], b_r.at[7 * k + dz - 1], {"z": mod(z - dz, NZ)})
        for dz in z_near:
            for dy in range(NY):
                yb_give[dy, 0] += b_take[dz - 1, B_PLACE[dy]].astype(F32)
            last = last + b_take[dz - 1, NY].astype(F32)
        for dy in range(NY):
            yb_give[dy, 1] = last
        for dy in (2, 1, 3):
            yy = mod(y + dy, NY)
            send(yb_give.at[dy], yb_take.at[dy - 1], yb_s.at[0], yb_r.at[dy - 1], {"y": yy})
    with jax.named_scope("g_by"):
        right = yb_give[0, 0]
        last = last[:, 0:32]
        for dy in (1, 3, 2):
            arrived(yb_take.at[dy - 1], yb_s.at[0], yb_r.at[dy - 1], {"y": mod(y - dy, NY)})
            right = right + yb_take[dy - 1, 0]
            last = last + yb_take[dy - 1, 1][:, 32 * dy : 32 * dy + 32]
    with jax.named_scope("loss3"):
        loss_sum = collected(sy_take, 24, loss_sum, "y")
        exchange(sz_give, sz_take, 27, loss_sum, "z")
    with jax.named_scope("g_z"):
        left = grad[y, pl.ds(z, 1), :, :GLA].reshape(EG, GLA)
        for dz in z_near:
            arrived(z_take.at[dz - 1], z_s.at[0], z_r.at[dz - 1], {"z": mod(z - dz, NZ)})
            left = left + z_take[dz - 1].astype(F32)
        grad[y, pl.ds(z, 1), :, :GLA] = left.reshape(1, EG, GLA)
        grad[y, pl.ds(z, 1), :, GLA:GLB] = right.reshape(1, EG, GLB - GLA)
        grad[y, pl.ds(z, 1), :, GLB : GLB + 32] = last.reshape(1, EG, 32)

    g = grad[y, pl.ds(z, 1)].reshape(EG, KP)
    e_id = lax.broadcasted_iota(jnp.int32, (EG, KP), 0)
    k_id = lax.broadcasted_iota(jnp.int32, (EG, KP), 1)
    squared = jnp.where((e_id < ED) & (k_id < KD), g * g + FLOOR_VALUE, 0.0)

    with jax.named_scope("st_row"):
        e_col = e_id[:, 0:128]
        l_col = k_id[:, 0:128]
        rows = jnp.broadcast_to(jnp.sum(squared, axis=1, keepdims=True), (EG, 128))
        row_line = jnp.sum(jnp.where(e_col == l_col, rows, 0.0), axis=0, keepdims=True)
        exchange(row_give, row_take, 0, row_line, "row")
        cols = jnp.sum(squared, axis=0, keepdims=True)
        row_line = collected(row_take, 0, row_line, "row")[:, :ED]
        row_line = DECAY_RATE * row_moment[...].reshape(1, ED) + (1.0 - DECAY_RATE) * row_line / FF
        new_row = jnp.sum(
            jnp.where(
                e_id[:, :ED] == k_id[:, :ED], jnp.broadcast_to(row_line, (EG, ED)), 0.0
            ), axis=1, keepdims=True
        )
        new_row = jnp.where(e_col[:, 0:1] < ED, new_row, 1.0)
        ratio = jnp.sum(g * g / new_row, axis=0, keepdims=True)
    with jax.named_scope("st_col"):
        cols2 = jnp.concatenate([cols, ratio], axis=1)
        exchange(cy_give, cy_take, 7, cols2, "y")
        cols2 = collected(cy_take, 7, cols2, "y")
        exchange(cz_give, cz_take, 10, cols2, "z")
        cols2 = collected(cz_take, 10, cols2, "z")
    with jax.named_scope("st_tot"):
        cols, ratio = cols2[:, :KP], cols2[:, KP:]
        col_line = DECAY_RATE * col_moment[...].reshape(1, KD) + (1.0 - DECAY_RATE) * cols[:, :KD] / D
        raw_sum = jnp.sum(ratio[:, :KD] / col_line, axis=1, keepdims=True)
        exchange(s_give, s_take, 17, jnp.broadcast_to(raw_sum, (1, 128)), "row")
        raw = g[:ED, :KD] / jnp.sqrt(new_row[:ED] * col_line)
        loss_sum = collected(sz_take, 27, loss_sum, "z")
        small_out[...] = jnp.zeros_like(small_out)
        small_out[0:1, :KD] = col_line
        small_out[1:2, :ED] = row_line
        small_out[2:3, 0:128] = loss_sum * (1.0 / BATCH)
        both = collected(s_take, 17, jnp.broadcast_to(raw_sum, (1, 128)), "row")
    with jax.named_scope("upd"):
        rms = jnp.sqrt(both[:, 0:1] / (D * FF))
        update_out[...] = raw / jnp.maximum(1.0, rms / CLIP_LEVEL)
    with jax.named_scope("finish"):
        w.finish()
        t.finish()
        all_sent(h_out.at[pl.ds(0, 7)], h_s.at[0], h_r.at[0], {"c": other})
        for k, (ref, device) in enumerate(
            ((far_p, up), (far_m, down), (near_p, up), (near_m, down), (relay_p, up), (relay_m, down))
        ):
            all_sent(ref, g_s.at[k], g_r.at[k], device)
        all_sent(z_take, z_s.at[0], z_r.at[0], {"z": mod(z + 1, NZ)})
        all_sent(b_take, b_s.at[0], b_r.at[0], {"z": mod(z + 1, NZ)})
        all_sent(yb_take, yb_s.at[0], yb_r.at[0], up)


def step_kernel(hidden, weight, text, pooled, row_moment, col_moment, scale, bias):
    vmem = pl.BlockSpec(memory_space=pltpu.VMEM)
    smem = pl.BlockSpec(memory_space=pltpu.SMEM)
    n_row = NX * NC
    dma = pltpu.SemaphoreType.DMA
    return pl.pallas_call(
        whole_kernel,
        out_shape=(
            jax.ShapeDtypeStruct((ED, KD), F32),
            jax.ShapeDtypeStruct((8, KP), F32),
        ),
        in_specs=[pl.BlockSpec(memory_space=pl.ANY)] * 6 + [smem] * 2,
        out_specs=(vmem,) * 2,
        scratch_shapes=[
            pltpu.VMEM((TOK, FF), BF16),
            pltpu.VMEM((ED, KD), F32),
            pltpu.VMEM((TOK, D), BF16),
            pltpu.VMEM((TOK, D), BF16),
            pltpu.VMEM((ED,), F32),
            pltpu.VMEM((KD,), F32),
            dma((6,)),
            pltpu.VMEM((n_row, TOK, KP), BF16),
            pltpu.VMEM((EP, KP), BF16),
            pltpu.VMEM((NX * TOK, NY * TOK), F32),
            pltpu.VMEM((NX * TOK, NY * TOK), F32),
            pltpu.VMEM((NX * TOK, NY * TOK), BF16),
            pltpu.VMEM((NX * TOK, NY * TOK), BF16),
            pltpu.VMEM((n_row, TOK, KP), BF16),
            pltpu.VMEM((n_row, TOK, D), BF16),
            pltpu.VMEM((8, NY * TOK), F32),
            pltpu.VMEM((NZ * NY, EP, WLA), BF16),
            pltpu.VMEM((NY * NZ, EP, KP - WLA), BF16),
            pltpu.VMEM((D, KP), BF16),
            pltpu.VMEM((NZ * NY, TOK, TLA), BF16),
            pltpu.VMEM((NY * NZ, TOK, D - TLA), BF16),
            pltpu.VMEM((TOK, D), BF16),
            pltpu.VMEM((n_row, TOK, D), F32),
            pltpu.VMEM((NX, TOK, D), F32),
            pltpu.VMEM((NX, TOK, D), F32),
            pltpu.VMEM((NX - 1, TOK, D), BF16),
            pltpu.VMEM((NX - 1, TOK, D), BF16),
            pltpu.VMEM((n_row, TOK, D), BF16),
            pltpu.VMEM((TOK, D), F32),
            pltpu.VMEM((TOK, 128), F32),
            pltpu.VMEM((n_row, TOK, D), F32),
            pltpu.VMEM((NX, TOK, D), BF16),
            pltpu.VMEM((NX, TOK, D), BF16),
            pltpu.VMEM((NX - 1, TOK, D), BF16),
            pltpu.VMEM((NX - 1, TOK, D), BF16),
            pltpu.VMEM((NY, NZ, EG, KP), F32),
            *[pltpu.VMEM((NZ // 2, EG, GLA), BF16)] * 12,
            pltpu.VMEM((NZ, EG, GLA), BF16),
            pltpu.VMEM((NZ - 1, EG, GLA), BF16),
            pltpu.VMEM((NY, NZ * EG, 384), BF16),
            pltpu.VMEM((NZ, EG, 128), F32),
            pltpu.VMEM((NZ, NY + 1, EG, 128), BF16),
            pltpu.VMEM((NZ - 1, NY + 1, EG, 128), BF16),
            pltpu.VMEM((NY, 2, EG, 128), F32),
            pltpu.VMEM((NY - 1, 2, EG, 128), F32),
            pltpu.VMEM((1, 128), F32),
            pltpu.VMEM((n_row - 1, 1, 128), F32),
            pltpu.VMEM((1, 2 * KP), F32),
            pltpu.VMEM((NY - 1, 1, 2 * KP), F32),
            pltpu.VMEM((1, 2 * KP), F32),
            pltpu.VMEM((NZ - 1, 1, 2 * KP), F32),
            pltpu.VMEM((1, 128), F32),
            pltpu.VMEM((n_row - 1, 1, 128), F32),
            pltpu.VMEM((1, 128), F32),
            pltpu.VMEM((n_row - 1, 1, 128), F32),
            pltpu.VMEM((1, 128), F32),
            pltpu.VMEM((NY - 1, 1, 128), F32),
            pltpu.VMEM((1, 128), F32),
            pltpu.VMEM((NZ - 1, 1, 128), F32),
            dma((2,)), dma((N_MSG,)), dma((2,)), dma((N_MSG,)),
            dma((1,)), dma((7,)), dma((2,)), dma((10,)), dma((1,)), dma((16,)),
            dma((6,)), dma((6,)), dma((1,)), dma((7,)), dma((1,)), dma((14,)),
            dma((1,)), dma((3,)), dma((7,)), dma((41,)),
        ],
        compiler_params=pltpu.CompilerParams(
            collective_id=0, has_side_effects=True, vmem_limit_bytes=60 * 1024 * 1024
        ),
        name="step",
    )(hidden, weight, text, pooled, row_moment, col_moment, scale, bias)


def out_kernel(update_in, small, update, new_row, new_col, loss):
    update[...] = update_in[...]
    new_row[...] = small[1:2, :ED].reshape(ED)
    new_col[...] = small[0:1, :KD].reshape(KD)
    loss[0] = small[2, 0]


def per_device(pooled, hidden, text, weight, row_moment, col_moment, log_scale, bias):
    update, small = step_kernel(
        hidden, weight, text, pooled, row_moment, col_moment, log_scale.reshape(1), bias.reshape(1)
    )
    vmem = pl.BlockSpec(memory_space=pltpu.VMEM)
    update, new_row, new_col, loss = pl.pallas_call(
        out_kernel,
        out_shape=(
            jax.ShapeDtypeStruct((ED, KD), F32),
            jax.ShapeDtypeStruct((ED,), F32),
            jax.ShapeDtypeStruct((KD,), F32),
            jax.ShapeDtypeStruct((1,), F32),
        ),
        in_specs=[vmem] * 2,
        out_specs=(vmem, vmem, vmem, pl.BlockSpec(memory_space=pltpu.SMEM)),
        name="out",
    )(update, small)
    return (update, new_row, new_col, loss.reshape(()))


def solution(mesh):
    finer = Mesh(mesh.devices.reshape(NX, NC, NY, NZ), ALL)
    return jax.shard_map(
        per_device,
        mesh=finer,
        in_specs=(
            P(ALL, None), P(ALL, None), P(ALL, None), P(COL, ROW), P(COL), P(ROW), P(), P(),
        ),
        out_specs=(P(COL, ROW), P(COL), P(ROW), P()),
        check_vma=False,
    )
```
